128 devices in a mesh: own: 32 (over x, z, core), rep: 4 (over y).
Axes of the slice: x: 4, y: 4, z: 4, core: 2. Of those that a mesh axis runs over, the one named last changes fastest.
Arguments:
- block_pool: bfloat16 [8192, 64, 576], P(('own', 'rep')), may hold values from -16 to 16
- sel_index: int32 [4096], P(('own', 'rep')), may hold values from 0 to 63
- sel_layer: int32 [4096], P(('own', 'rep')), may hold values from 0 to 15, as said below
- counts: int32 [128], P(('own', 'rep')), may hold values from 8 to 32, as said below
Outputs:
- quant_codes: bfloat16 [32, 4, 32, 8, 18432], P('own', 'rep')
- quant_steps: float32 [32, 288], P('own')
- clip_error: float32 [32, 288], P('own')
The draws below stay inside these ranges and needn't reach their ends.
Inputs may be any that keep to these rules, and one draw needn't show every extreme that they name: `sel_layer`: among the 32 entries of one device, at most 8 name any one layer; the first 8 entries of every device all name one and the same layer. `counts`: some device has all 32 entries live.
All inputs are finite; a program needn't handle non-finite values.
Results may differ from the reference program's by a relative error of at most 0.001.
Values may be sent and summed in bfloat16 or wider, within the bound.
A program may use at most 128 MiB of HBM per device.

```python
import math
import jax
import jax.numpy as jnp
from jax import lax

LATENT = 576
TOKB = 64
SLICES = 2
CAP = 8
POOL_DEV = 64
SEL_DEV = 32
LAYERS = 16
HALF = 288
SEL_ALL = 4096
N_OWN = 32
N_REP = 4


def draw_block_pool(key, part):
    base_key = jax.random.fold_in(key, 11)
    key_chan, key_base, key_rows = jax.random.split(base_key, 3)
    shape = (N_OWN * N_REP * POOL_DEV, TOKB, LATENT)
    channel = jnp.exp(jax.random.uniform(key_chan, (LATENT,), jnp.float32, math.log(0.3), math.log(3.0)))
    base = jnp.clip(jax.random.normal(key_base, shape, jnp.float32), -5.0, 5.0)
    row_scale = jnp.ones((shape[0], 1, 1), jnp.float32)
    return (base * channel * row_scale).astype(jnp.bfloat16)


def draw_sel_layer(key, part):
    devices = N_OWN * N_REP
    base_key = jax.random.fold_in(key, 31)
    key_star, key_perm = jax.random.split(base_key, 2)
    star_layer = jax.random.randint(key_star, (), 0, LAYERS)
    items = jnp.arange((LAYERS - 1) * CAP, dtype=jnp.int32) // CAP
    device_keys = jax.random.split(key_perm, devices)

    def per_device(device_key):
        shuffled = jax.random.permutation(device_key, items)[:SEL_DEV - CAP]
        others = (star_layer + 1 + shuffled) % LAYERS
        front = jnp.full((CAP,), star_layer, jnp.int32)
        return jnp.concatenate([front, others.astype(jnp.int32)])
    return jax.vmap(per_device)(device_keys).reshape(-1).astype(jnp.int32)


def draw_counts(key, part):
    devices = N_OWN * N_REP
    base_key = jax.random.fold_in(key, 21)
    key_low, key_full, key_first = jax.random.split(base_key, 3)
    lower = jax.random.randint(key_low, (devices,), CAP, CAP + (SEL_DEV - CAP) // 3 + 1)
    full_mask = jax.random.randint(key_full, (devices,), 0, 8) == 0
    first_full = jax.random.randint(key_first, (), 0, devices)
    full_mask = full_mask | (jnp.arange(devices) == first_full)
    return jnp.where(full_mask, SEL_DEV, lower).astype(jnp.int32)


def touch_ends(drawn, stream_key, low, high):
    index_at = [jax.random.randint(jax.random.fold_in(stream_key, axis), (), 0, length) for axis, length in enumerate(drawn.shape)]
    main_axis = drawn.shape.index(max(drawn.shape))
    neighbour = index_at[:main_axis] + [(index_at[main_axis] + 1) % drawn.shape[main_axis]] + index_at[main_axis + 1:]
    return drawn.at[tuple(index_at)].set(low).at[tuple(neighbour)].set(high)


def setup_inputs(seed: int = 0) -> dict:
    seeds = jax.random.split(jax.random.key(seed), 5)
    return {
        "block_pool": draw_block_pool(jax.random.fold_in(seeds[4], 71), 0),
        "sel_index": touch_ends(jax.random.randint(seeds[1], (SEL_ALL,), 0, POOL_DEV), jax.random.fold_in(seeds[1], 1), 0, POOL_DEV - 1).astype(jnp.int32),
        "sel_layer": draw_sel_layer(jax.random.fold_in(seeds[4], 71), 0),
        "counts": draw_counts(jax.random.fold_in(seeds[4], 71), 0),
    }


headroom = 0.5


def slot_table(index_row, layer_row, live_count, group_layer, capacity):
    n_select = index_row.shape[0]
    is_live = jnp.arange(n_select) < live_count
    matches = (layer_row[None, :] == group_layer[:, None]) & is_live[None, :]
    ranking = jnp.cumsum(matches.astype(jnp.int32), axis=1) - 1
    slot_hit = matches[:, None, :] & (ranking[:, None, :] == jnp.arange(capacity)[None, :, None])
    chosen = jnp.sum(jnp.where(slot_hit, index_row[None, None, :], 0), axis=2).astype(jnp.int32)
    filled = jnp.any(slot_hit, axis=2)
    return chosen, filled


def reference(block_pool, sel_index, sel_layer, counts):
    devices = N_OWN * N_REP
    group_layer = (jnp.arange(N_OWN) // SLICES).astype(jnp.int32)
    index_rows = sel_index.reshape(devices, SEL_DEV)
    layer_rows = sel_layer.reshape(devices, SEL_DEV)
    chosen, filled = jax.vmap(lambda a, b, c: slot_table(a, b, c, group_layer, CAP))(index_rows, layer_rows, counts)
    pools = block_pool.reshape(devices, POOL_DEV, TOKB, SLICES, HALF)
    device_ids = jnp.arange(devices)[:, None]
    denominator = float(N_OWN * N_REP * CAP * TOKB)

    def one_group(group):
        slice_of = group % SLICES
        picked = jnp.take(chosen, group, axis=1)
        keep_mask = jnp.take(filled, group, axis=1)
        blocks = pools[device_ids, picked, :, slice_of]
        blocks = jnp.where(keep_mask[:, :, None, None], blocks, jnp.zeros((), blocks.dtype))
        values = blocks.astype(jnp.float32)
        peak_abs = jnp.max(jnp.abs(values), axis=(0, 1, 2))
        step_size = headroom * jnp.maximum(peak_abs, 1.0) / 127.0
        encoded = jnp.clip(values / step_size, -127.0, 127.0).astype(jnp.bfloat16)
        encoded = lax.optimization_barrier(encoded)
        decoded = encoded.astype(jnp.float32) * step_size
        sq_error = jnp.sum((values - decoded) ** 2, axis=(0, 1, 2))
        error_out = sq_error / (step_size * step_size * denominator)
        codes_out = encoded.reshape(N_OWN, N_REP, CAP, TOKB * HALF).transpose(1, 0, 2, 3)
        return codes_out, step_size, error_out

    quant_codes, quant_steps, clip_error = lax.map(one_group, jnp.arange(N_OWN))
    return quant_codes, quant_steps, clip_error
```

```python
import functools

import jax
import jax.numpy as jnp
from jax import lax
from jax.experimental import pallas as pl
from jax.experimental.pallas import tpu as pltpu
from jax.sharding import PartitionSpec as P

SLICES = 2
HEADROOM = 0.5
MESH = pl.DeviceIdType.MESH


def part_kernel(layers, capacity, half, idx_ref, lay_ref, cnt_ref, pool_ref, out_ref,
                blocks, wide, stage, zeros, slot_of, in_sem, out_sem, zero_sem):
    n_select = idx_ref.shape[0]
    tokens = blocks.shape[1]
    latent = blocks.shape[2]
    for j in range(n_select):
        pltpu.make_async_copy(pool_ref.at[idx_ref[j]], blocks.at[j], in_sem).start()
    live = cnt_ref[0]

    def clear(i, _):
        slot_of[i] = -1
        return 0

    lax.fori_loop(0, layers * capacity + layers, clear, 0)

    def place(j, _):
        layer = lay_ref[j]

        @pl.when(j < live)
        def _():
            rank = slot_of[layers * capacity + layer] + 1
            slot_of[layers * capacity + layer] = rank
            slot_of[layer * capacity + rank] = j
        return 0

    lax.fori_loop(0, n_select, place, 0)
    zeros[...] = jnp.zeros_like(zeros)
    pltpu.make_async_copy(pool_ref.at[pl.ds(0, n_select)], blocks, in_sem).wait()

    def one_layer(layer, used):
        some = slot_of[layers * capacity + layer] >= 0

        @pl.when(jnp.logical_not(some))
        def _():
            cp = pltpu.make_async_copy(zeros, out_ref.at[pl.ds(layer * SLICES, SLICES)], zero_sem)
            cp.start()
            cp.wait()

        @pl.when(some)
        def _():
            @pl.when(used > 0)
            def _():
                pltpu.make_async_copy(stage.at[0], out_ref.at[pl.ds(0, SLICES)], out_sem).wait()
            for c in range(capacity):
                j = slot_of[layer * capacity + c]

                @pl.when(j >= 0)
                def _():
                    for k in range(wide.shape[0]):
                        cols = min(128, latent - k * 128)
                        wide[k, pl.ds(c * tokens, tokens), :cols] = blocks[j, :, k * 128:k * 128 + cols].astype(jnp.float32)

                @pl.when(j < 0)
                def _():
                    wide[:, pl.ds(c * tokens, tokens), :] = jnp.zeros((wide.shape[0], tokens, 128), jnp.float32)

            def four(q, _):
                rows = [jnp.concatenate([wide[k, pl.ds(4 * q + m, capacity, stride=tokens), :]
                                         for k in range(wide.shape[0])], axis=1) for m in range(4)]
                for h in range(SLICES):
                    flat = jnp.concatenate([r[:, h * half:(h + 1) * half] for r in rows], axis=1)
                    stage[0, h, :, pl.ds(pl.multiple_of(q * 4 * half, 128), 4 * half)] = flat.astype(jnp.bfloat16)
                return 0

            lax.fori_loop(0, tokens // 4, four, 0)
            pltpu.make_async_copy(stage.at[0], out_ref.at[pl.ds(layer * SLICES, SLICES)], out_sem).start()
        return used + some.astype(jnp.int32)

    used = lax.fori_loop(0, layers, one_layer, 0)

    @pl.when(used > 0)
    def _():
        pltpu.make_async_copy(stage.at[0], out_ref.at[pl.ds(0, SLICES)], out_sem).wait()


def part(block_pool, sel_index, sel_layer, counts, layers, capacity):
    rows, tokens, latent = block_pool.shape
    half = latent // SLICES
    n_select = sel_index.shape[0]
    groups = layers * SLICES
    smem = pl.BlockSpec(memory_space=pltpu.SMEM)
    return pl.pallas_call(
        functools.partial(part_kernel, layers, capacity, half),
        out_shape=jax.ShapeDtypeStruct((groups, capacity, tokens * half), jnp.bfloat16),
        in_specs=[smem, smem, smem, pl.BlockSpec(memory_space=pltpu.HBM)],
        out_specs=pl.BlockSpec(memory_space=pltpu.HBM),
        scratch_shapes=[
            pltpu.VMEM((n_select, tokens, latent), jnp.bfloat16),
            pltpu.VMEM((-(-latent // 128), capacity * tokens, 128), jnp.float32),
            pltpu.VMEM((1, SLICES, capacity, tokens * half), jnp.bfloat16),
            pltpu.VMEM((SLICES, capacity, tokens * half), jnp.bfloat16),
            pltpu.SMEM((layers * capacity + layers,), jnp.int32),
            pltpu.SemaphoreType.DMA,
            pltpu.SemaphoreType.DMA,
            pltpu.SemaphoreType.DMA,
        ],
    )(sel_index, sel_layer, counts, block_pool)


def rep_peers():
    me = lax.axis_index("rep")
    count = lax.axis_size("rep")
    return [lax.rem(me + d, count) for d in range(1, count)]


def greet():
    barrier = pltpu.get_barrier_semaphore()
    for peer in rep_peers():
        pl.semaphore_signal(barrier, inc=1, device_id={"rep": peer}, device_id_type=MESH)


def share(mine, theirs, send_sem, recv_sem):
    pl.semaphore_wait(pltpu.get_barrier_semaphore(), len(rep_peers()))
    copies = []
    for i, peer in enumerate(rep_peers()):
        cp = pltpu.make_async_remote_copy(
            src_ref=mine, dst_ref=theirs.at[i], send_sem=send_sem.at[i], recv_sem=recv_sem.at[i],
            device_id={"rep": peer}, device_id_type=MESH)
        cp.start()
        copies.append(cp)
    for cp in copies:
        cp.wait()


def peak_kernel(steps, period, x_ref, out_ref, acc, mine, theirs, send_sem, recv_sem):
    i = pl.program_id(0)

    @pl.when(i == 0)
    def _():
        greet()
        acc[...] = jnp.zeros_like(acc)

    def fold(g, top):
        chunk = x_ref[:, :, pl.ds(pl.multiple_of(g * period, 128), period)].astype(jnp.float32)
        return jnp.maximum(top, jnp.max(jnp.abs(chunk), axis=0))

    acc[...] = lax.fori_loop(0, x_ref.shape[2] // period, fold, acc[...])

    @pl.when(i == steps - 1)
    def _():
        mine[...] = jnp.broadcast_to(jnp.max(acc[...], axis=0, keepdims=True), mine.shape)
        share(mine, theirs, send_sem, recv_sem)
        out_ref[...] = jnp.maximum(jnp.max(theirs[...], axis=0), mine[...])


def peaks(arrived, period, per_step=4):
    sources, capacity, flat = arrived.shape
    steps = sources // per_step
    peers = lax.axis_size("rep") - 1
    return pl.pallas_call(
        functools.partial(peak_kernel, steps, period),
        grid=(steps,),
        out_shape=jax.ShapeDtypeStruct((8, period), jnp.float32),
        in_specs=[pl.BlockSpec((per_step, capacity, flat), lambda i: (i, 0, 0))],
        out_specs=pl.BlockSpec((8, period), lambda i: (0, 0)),
        scratch_shapes=[
            pltpu.VMEM((capacity, period), jnp.float32),
            pltpu.VMEM((8, period), jnp.float32),
            pltpu.VMEM((peers, 8, period), jnp.float32),
            pltpu.SemaphoreType.DMA((peers,)),
            pltpu.SemaphoreType.DMA((peers,)),
        ],
        compiler_params=pltpu.CompilerParams(collective_id=0, has_side_effects=True),
    )(arrived)


def code_kernel(period, x_ref, step_ref, out_ref, err_ref):
    @pl.when(pl.program_id(0) == 0)
    def _():
        err_ref[...] = jnp.zeros_like(err_ref)

    step = jnp.broadcast_to(step_ref[...], err_ref.shape)
    inverse = 1.0 / step

    def fold(g, total):
        at = pl.ds(pl.multiple_of(g * period, 128), period)
        for s in range(x_ref.shape[0]):
            values = x_ref[s, :, at].astype(jnp.float32)
            codes = jnp.clip(values * inverse, -127.0, 127.0).astype(jnp.bfloat16)
            out_ref[s, :, at] = codes
            miss = values - codes.astype(jnp.float32) * step
            total = total + miss * miss
        return total

    err_ref[...] = lax.fori_loop(0, x_ref.shape[2] // period, fold, err_ref[...])


def encode(arrived, step_row, period, per_step=4):
    sources, capacity, flat = arrived.shape
    return pl.pallas_call(
        functools.partial(code_kernel, period),
        grid=(sources // per_step,),
        out_shape=(jax.ShapeDtypeStruct(arrived.shape, jnp.bfloat16),
                   jax.ShapeDtypeStruct((capacity, period), jnp.float32)),
        in_specs=[pl.BlockSpec((per_step, capacity, flat), lambda i: (i, 0, 0)),
                  pl.BlockSpec((1, period), lambda i: (0, 0))],
        out_specs=(pl.BlockSpec((per_step, capacity, flat), lambda i: (i, 0, 0)),
                   pl.BlockSpec((capacity, period), lambda i: (0, 0))),
    )(arrived, step_row)


def total_kernel(err_ref, out_ref, mine, theirs, send_sem, recv_sem):
    greet()
    mine[...] = jnp.broadcast_to(jnp.sum(err_ref[...], axis=0, keepdims=True), mine.shape)
    share(mine, theirs, send_sem, recv_sem)
    out_ref[...] = jnp.sum(theirs[...], axis=0) + mine[...]


def totals(err):
    period = err.shape[1]
    peers = lax.axis_size("rep") - 1
    vmem = pl.BlockSpec(memory_space=pltpu.VMEM)
    return pl.pallas_call(
        total_kernel,
        out_shape=jax.ShapeDtypeStruct((8, period), jnp.float32),
        in_specs=[vmem],
        out_specs=vmem,
        scratch_shapes=[
            pltpu.VMEM((8, period), jnp.float32),
            pltpu.VMEM((peers, 8, period), jnp.float32),
            pltpu.SemaphoreType.DMA((peers,)),
            pltpu.SemaphoreType.DMA((peers,)),
        ],
        compiler_params=pltpu.CompilerParams(collective_id=1, has_side_effects=True),
    )(err)


def body(block_pool, sel_index, sel_layer, counts):
    own_count = lax.axis_size("own")
    rep_count = lax.axis_size("rep")
    capacity = sel_index.shape[0] // 4
    tokens = block_pool.shape[1]
    half = block_pool.shape[2] // SLICES
    period = 4 * half
    parted = part(block_pool, sel_index, sel_layer, counts, own_count // SLICES, capacity)
    denominator = float(own_count * rep_count * capacity * tokens)
    arrived = lax.all_to_all(parted, "own", split_axis=0, concat_axis=0, tiled=True)
    top = jnp.max(peaks(arrived, period)[0].reshape(4, half), axis=0)
    step = HEADROOM * jnp.maximum(top, 1.0) / 127.0
    codes, err = encode(arrived, jnp.tile(step, 4)[None, :], period)
    error = jnp.sum(totals(err)[0].reshape(4, half), axis=0)
    return codes[None, None], step[None, :], (error / (step * step * denominator))[None, :]


def solution(mesh):
    return jax.shard_map(
        body,
        mesh=mesh,
        in_specs=(
            P(("own", "rep"), None, None),
            P(("own", "rep")),
            P(("own", "rep")),
            P(("own", "rep")),
        ),
        out_specs=(P("own", "rep", None, None, None), P("own", None), P("own", None)),
        check_vma=False,
    )
```

```python
import functools

import jax
import jax.numpy as jnp
from jax import lax
from jax.experimental import pallas as pl
from jax.experimental.pallas import tpu as pltpu
from jax.sharding import PartitionSpec as P

SLICES = 2
HEADROOM = 0.5
MESH = pl.DeviceIdType.MESH


def part_kernel(layers, capacity, half, idx_ref, lay_ref, cnt_ref, pool_ref, out_ref,
                blocks, wide, stage, zeros, slot_of, in_sem, out_sem, zero_sem):
    n_select = idx_ref.shape[0]
    tokens = blocks.shape[1]
    latent = blocks.shape[2]
    for j in range(n_select):
        pltpu.make_async_copy(pool_ref.at[idx_ref[j]], blocks.at[j], in_sem).start()
    live = cnt_ref[0]

    def clear(i, _):
        slot_of[i] = -1
        return 0

    lax.fori_loop(0, layers * capacity + layers, clear, 0)

    def place(j, _):
        layer = lay_ref[j]

        @pl.when(j < live)
        def _():
            rank = slot_of[layers * capacity + layer] + 1
            slot_of[layers * capacity + layer] = rank
            slot_of[layer * capacity + rank] = j
        return 0

    lax.fori_loop(0, n_select, place, 0)
    zeros[...] = jnp.zeros_like(zeros)
    pltpu.make_async_copy(pool_ref.at[pl.ds(0, n_select)], blocks, in_sem).wait()

    def one_layer(layer, used):
        some = slot_of[layers * capacity + layer] >= 0

        @pl.when(jnp.logical_not(some))
        def _():
            cp = pltpu.make_async_copy(zeros, out_ref.at[pl.ds(layer * SLICES, SLICES)], zero_sem)
            cp.start()
            cp.wait()

        @pl.when(some)
        def _():
            @pl.when(used > 0)
            def _():
                pltpu.make_async_copy(stage.at[0], out_ref.at[pl.ds(0, SLICES)], out_sem).wait()
            for c in range(capacity):
                j = slot_of[layer * capacity + c]

                @pl.when(j >= 0)
                def _():
                    for k in range(wide.shape[0]):
                        cols = min(128, latent - k * 128)
                        wide[k, pl.ds(c * tokens, tokens), :cols] = blocks[j, :, k * 128:k * 128 + cols].astype(jnp.float32)

                @pl.when(j < 0)
                def _():
                    wide[:, pl.ds(c * tokens, tokens), :] = jnp.zeros((wide.shape[0], tokens, 128), jnp.float32)

            def four(q, _):
                rows = [jnp.concatenate([wide[k, pl.ds(4 * q + m, capacity, stride=tokens), :]
                                         for k in range(wide.shape[0])], axis=1) for m in range(4)]
                for h in range(SLICES):
                    flat = jnp.concatenate([r[:, h * half:(h + 1) * half] for r in rows], axis=1)
                    stage[0, h, :, pl.ds(pl.multiple_of(q * 4 * half, 128), 4 * half)] = flat.astype(jnp.bfloat16)
                return 0

            lax.fori_loop(0, tokens // 4, four, 0)
            pltpu.make_async_copy(stage.at[0], out_ref.at[pl.ds(layer * SLICES, SLICES)], out_sem).start()
        return used + some.astype(jnp.int32)

    used = lax.fori_loop(0, layers, one_layer, 0)

    @pl.when(used > 0)
    def _():
        pltpu.make_async_copy(stage.at[0], out_ref.at[pl.ds(0, SLICES)], out_sem).wait()


def part(block_pool, sel_index, sel_layer, counts, layers, capacity):
    rows, tokens, latent = block_pool.shape
    half = latent // SLICES
    n_select = sel_index.shape[0]
    groups = layers * SLICES
    smem = pl.BlockSpec(memory_space=pltpu.SMEM)
    return pl.pallas_call(
        functools.partial(part_kernel, layers, capacity, half),
        out_shape=jax.ShapeDtypeStruct((groups, capacity, tokens * half), jnp.bfloat16),
        in_specs=[smem, smem, smem, pl.BlockSpec(memory_space=pltpu.HBM)],
        out_specs=pl.BlockSpec(memory_space=pltpu.HBM),
        scratch_shapes=[
            pltpu.VMEM((n_select, tokens, latent), jnp.bfloat16),
            pltpu.VMEM((-(-latent // 128), capacity * tokens, 128), jnp.float32),
            pltpu.VMEM((1, SLICES, capacity, tokens * half), jnp.bfloat16),
            pltpu.VMEM((SLICES, capacity, tokens * half), jnp.bfloat16),
            pltpu.SMEM((layers * capacity + layers,), jnp.int32),
            pltpu.SemaphoreType.DMA,
            pltpu.SemaphoreType.DMA,
            pltpu.SemaphoreType.DMA,
        ],
    )(sel_index, sel_layer, counts, block_pool)


def rep_peers():
    me = lax.axis_index("rep")
    count = lax.axis_size("rep")
    return [lax.rem(me + d, count) for d in range(1, count)]


def greet():
    barrier = pltpu.get_barrier_semaphore()
    for peer in rep_peers():
        pl.semaphore_signal(barrier, inc=1, device_id={"rep": peer}, device_id_type=MESH)


def share(mine, theirs, send_sem, recv_sem):
    pl.semaphore_wait(pltpu.get_barrier_semaphore(), len(rep_peers()))
    copies = []
    for i, peer in enumerate(rep_peers()):
        cp = pltpu.make_async_remote_copy(
            src_ref=mine, dst_ref=theirs.at[i], send_sem=send_sem.at[i], recv_sem=recv_sem.at[i],
            device_id={"rep": peer}, device_id_type=MESH)
        cp.start()
        copies.append(cp)
    for cp in copies:
        cp.wait()


def peak_kernel(steps, period, x_ref, out_ref, acc, mine, theirs, send_sem, recv_sem):
    i = pl.program_id(0)

    @pl.when(i == 0)
    def _():
        greet()
        acc[...] = jnp.zeros_like(acc)

    def fold(g, top):
        chunk = x_ref[:, :, pl.ds(pl.multiple_of(g * period, 128), period)].astype(jnp.float32)
        return jnp.maximum(top, jnp.max(jnp.abs(chunk), axis=0))

    acc[...] = lax.fori_loop(0, x_ref.shape[2] // period, fold, acc[...])

    @pl.when(i == steps - 1)
    def _():
        mine[...] = jnp.broadcast_to(jnp.max(acc[...], axis=0, keepdims=True), mine.shape)
        share(mine, theirs, send_sem, recv_sem)
        out_ref[...] = jnp.maximum(jnp.max(theirs[...], axis=0), mine[...])


def peaks(arrived, period, per_step=4):
    sources, capacity, flat = arrived.shape
    steps = sources // per_step
    peers = lax.axis_size("rep") - 1
    return pl.pallas_call(
        functools.partial(peak_kernel, steps, period),
        grid=(steps,),
        out_shape=jax.ShapeDtypeStruct((8, period), jnp.float32),
        in_specs=[pl.BlockSpec((per_step, capacity, flat), lambda i: (i, 0, 0))],
        out_specs=pl.BlockSpec((8, period), lambda i: (0, 0)),
        scratch_shapes=[
            pltpu.VMEM((capacity, period), jnp.float32),
            pltpu.VMEM((8, period), jnp.float32),
            pltpu.VMEM((peers, 8, period), jnp.float32),
            pltpu.SemaphoreType.DMA((peers,)),
            pltpu.SemaphoreType.DMA((peers,)),
        ],
        compiler_params=pltpu.CompilerParams(collective_id=0, has_side_effects=True),
    )(arrived)


def code_kernel(period, x_ref, step_ref, out_ref, err_ref):
    @pl.when(pl.program_id(0) == 0)
    def _():
        err_ref[...] = jnp.zeros_like(err_ref)

    step = jnp.broadcast_to(step_ref[...], err_ref.shape)
    inverse = 1.0 / step

    def fold(g, total):
        at = pl.ds(pl.multiple_of(g * period, 128), period)
        for s in range(x_ref.shape[0]):
            values = x_ref[s, :, at].astype(jnp.float32)
            codes = jnp.clip(values * inverse, -127.0, 127.0).astype(jnp.bfloat16)
            out_ref[s, :, at] = codes
            miss = values - codes.astype(jnp.float32) * step
            total = total + miss * miss
        return total

    err_ref[...] = lax.fori_loop(0, x_ref.shape[2] // period, fold, err_ref[...])


def encode(arrived, step_row, period, per_step=4):
    sources, capacity, flat = arrived.shape
    return pl.pallas_call(
        functools.partial(code_kernel, period),
        grid=(sources // per_step,),
        out_shape=(jax.ShapeDtypeStruct(arrived.shape, jnp.bfloat16),
                   jax.ShapeDtypeStruct((capacity, period), jnp.float32)),
        in_specs=[pl.BlockSpec((per_step, capacity, flat), lambda i: (i, 0, 0)),
                  pl.BlockSpec((1, period), lambda i: (0, 0))],
        out_specs=(pl.BlockSpec((per_step, capacity, flat), lambda i: (i, 0, 0)),
                   pl.BlockSpec((capacity, period), lambda i: (0, 0))),
    )(arrived, step_row)


def total_kernel(err_ref, out_ref, mine, theirs, send_sem, recv_sem):
    greet()
    mine[...] = jnp.broadcast_to(jnp.sum(err_ref[...], axis=0, keepdims=True), mine.shape)
    share(mine, theirs, send_sem, recv_sem)
    out_ref[...] = jnp.sum(theirs[...], axis=0) + mine[...]


def totals(err):
    period = err.shape[1]
    peers = lax.axis_size("rep") - 1
    vmem = pl.BlockSpec(memory_space=pltpu.VMEM)
    return pl.pallas_call(
        total_kernel,
        out_shape=jax.ShapeDtypeStruct((8, period), jnp.float32),
        in_specs=[vmem],
        out_specs=vmem,
        scratch_shapes=[
            pltpu.VMEM((8, period), jnp.float32),
            pltpu.VMEM((peers, 8, period), jnp.float32),
            pltpu.SemaphoreType.DMA((peers,)),
            pltpu.SemaphoreType.DMA((peers,)),
        ],
        compiler_params=pltpu.CompilerParams(collective_id=1, has_side_effects=True),
    )(err)


def split_kernel(half, idx_ref, cnt_ref, pool_ref, hot_ref, cold_ref, blocks, wide, flat, in_sem):
    n_select = idx_ref.shape[0]
    tokens, latent = blocks.shape[1], blocks.shape[2]
    capacity = hot_ref.shape[1]
    tiles = wide.shape[0]
    for j in range(n_select):
        pltpu.make_async_copy(pool_ref.at[idx_ref[j]], blocks.at[j], in_sem).start()
    pltpu.make_async_copy(pool_ref.at[pl.ds(0, n_select)], blocks, in_sem).wait()

    def widen(j, row):
        for k in range(tiles):
            cols = min(128, latent - k * 128)
            wide[k, pl.ds(row, tokens), :cols] = blocks[j, :, k * 128:k * 128 + cols].astype(jnp.float32)

    def strided(row, count, stride):
        return jnp.concatenate([wide[k, pl.ds(row, count, stride=stride), :] for k in range(tiles)], axis=1)

    for c in range(capacity):
        widen(c, c * tokens)

    def four(q, _):
        rows = [strided(4 * q + m, capacity, tokens) for m in range(4)]
        for h in range(SLICES):
            line = jnp.concatenate([r[:, h * half:(h + 1) * half] for r in rows], axis=1)
            hot_ref[h, :, pl.ds(pl.multiple_of(q * 4 * half, 128), 4 * half)] = line.astype(jnp.bfloat16)
        return 0

    lax.fori_loop(0, tokens // 4, four, 0)
    quads = tokens // 4
    lines = 4 * half // 128

    def one(j, _):
        widen(j, 0)
        rows = [strided(m, quads, 4) for m in range(4)]
        for h in range(SLICES):
            line = jnp.concatenate([r[:, h * half:(h + 1) * half] for r in rows], axis=1)
            for i in range(lines):
                flat[h, pl.ds(i, quads, stride=lines), :] = line[:, i * 128:(i + 1) * 128]
        for h in range(SLICES):
            cold_ref[h, j - capacity] = flat[h].astype(jnp.bfloat16)
        return 0

    lax.fori_loop(capacity, cnt_ref[0], one, 0)


def split(block_pool, sel_index, counts, capacity):
    _, tokens, latent = block_pool.shape
    half = latent // SLICES
    n_select = sel_index.shape[0]
    lines = tokens * half // 128
    smem = pl.BlockSpec(memory_space=pltpu.SMEM)
    vmem = pl.BlockSpec(memory_space=pltpu.VMEM)
    return pl.pallas_call(
        functools.partial(split_kernel, half),
        out_shape=(jax.ShapeDtypeStruct((SLICES, capacity, tokens * half), jnp.bfloat16),
                   jax.ShapeDtypeStruct((SLICES, n_select - capacity, lines, 128), jnp.bfloat16)),
        in_specs=[smem, smem, pl.BlockSpec(memory_space=pltpu.HBM)],
        out_specs=(vmem, vmem),
        scratch_shapes=[
            pltpu.VMEM((n_select, tokens, latent), jnp.bfloat16),
            pltpu.VMEM((-(-latent // 128), capacity * tokens, 128), jnp.float32),
            pltpu.VMEM((SLICES, lines, 128), jnp.float32),
            pltpu.SemaphoreType.DMA,
        ],
    )(sel_index, counts, block_pool)


def tables_kernel(row_ref, out_ref, own_send, own_recv, send_sem, recv_sem):
    me, mine = lax.axis_index("own"), lax.axis_index("rep")
    owners = lax.axis_size("own")
    barrier = pltpu.get_barrier_semaphore()

    def hello(i, _):
        pl.semaphore_signal(barrier, inc=1, device_id={"own": lax.rem(me + i, owners)}, device_id_type=MESH)
        return 0

    lax.fori_loop(1, owners, hello, 0)
    greet()
    out_ref[mine, me] = row_ref[...]
    pl.semaphore_wait(barrier, owners - 1 + len(rep_peers()))

    def push(i, _):
        pltpu.make_async_remote_copy(
            src_ref=row_ref, dst_ref=out_ref.at[mine, me], send_sem=own_send, recv_sem=own_recv,
            device_id={"own": lax.rem(me + i, owners)}, device_id_type=MESH).start()
        return 0

    lax.fori_loop(1, owners, push, 0)
    rest = out_ref.at[mine, pl.ds(0, owners - 1)]
    pltpu.make_async_copy(rest, rest, own_recv).wait()
    pltpu.make_async_copy(rest, rest, own_send).wait()
    copies = []
    for i, peer in enumerate(rep_peers()):
        cp = pltpu.make_async_remote_copy(
            src_ref=out_ref.at[mine], dst_ref=out_ref.at[mine], send_sem=send_sem.at[i], recv_sem=recv_sem.at[i],
            device_id={"rep": peer}, device_id_type=MESH)
        cp.start()
        copies.append(cp)
    for cp in copies:
        cp.wait()


def tables(row):
    owners, reps = lax.axis_size("own"), lax.axis_size("rep")
    vmem = pl.BlockSpec(memory_space=pltpu.VMEM)
    return pl.pallas_call(
        tables_kernel,
        out_shape=jax.ShapeDtypeStruct((reps, owners, 1, 128), jnp.int32),
        in_specs=[vmem],
        out_specs=vmem,
        scratch_shapes=[
            pltpu.SemaphoreType.DMA,
            pltpu.SemaphoreType.DMA,
            pltpu.SemaphoreType.DMA((reps - 1,)),
            pltpu.SemaphoreType.DMA((reps - 1,)),
        ],
        compiler_params=pltpu.CompilerParams(collective_id=2, has_side_effects=True),
    )(row)


SIDE = 4
CAP_ONE = 20
CAP_TWO = 16


def place():
    me = lax.axis_index("own")
    core = lax.rem(me, 2)
    x, z = me // (2 * SIDE), lax.rem(me // 2, SIDE)
    return core, jnp.where(core == 0, x, z), jnp.where(core == 0, z, x)


def index_of(core, a, b, slot):
    return jnp.where(core == 0, a * SIDE + b, b * SIDE + a) * 2 + slot


def plan(table, capacity):
    reps, owners = table.shape[0], table.shape[1]
    core, a, b = place()
    cold = table[:, :, 0, capacity:4 * capacity]
    n_cold = cold.shape[-1]
    layers = owners // 2
    hits = (cold[..., None] == jnp.arange(layers)).astype(jnp.int32)
    count = hits.reshape(reps, SIDE, SIDE, 2 * n_cold, SIDE, SIDE).sum(axis=3)
    top_one = jnp.maximum(count.sum(axis=4).max(), count.sum(axis=3).max())
    top_two = jnp.maximum(count.sum(axis=1).max(), count.sum(axis=2).max())
    fits = (top_one <= CAP_ONE) & (top_two <= CAP_TWO)

    mine = lax.dynamic_index_in_dim(cold, lax.axis_index("rep"), 0, keepdims=False)
    grid = mine.reshape(SIDE, SIDE, 2 * n_cold)
    grid = jnp.where(core == 0, grid, grid.transpose(1, 0, 2))
    live = grid >= 0
    to_a = jnp.where(live, jnp.where(core == 0, grid // SIDE, grid % SIDE), -1)
    to_b = jnp.where(live, jnp.where(core == 0, grid % SIDE, grid // SIDE), -1)

    column_a = lax.dynamic_index_in_dim(to_a, b, 1, keepdims=False)
    column_b = lax.dynamic_index_in_dim(to_b, b, 1, keepdims=False)
    n = 2 * n_cold
    before = jnp.arange(n)[None, :] < jnp.arange(n)[:, None]
    rank_one = jnp.sum((column_a[:, :, None] == column_a[:, None, :]) & before, axis=2)
    own_a = lax.dynamic_index_in_dim(column_a, a, 0, keepdims=False)
    own_rank = lax.dynamic_index_in_dim(rank_one, a, 0, keepdims=False)
    wanted = ((own_a[None, None, :] == jnp.arange(SIDE)[:, None, None])
              & (own_rank[None, None, :] == jnp.arange(CAP_ONE)[None, :, None]))
    pack_one = jnp.sum(jnp.where(wanted, jnp.arange(n), 0), axis=2)

    relay_b = jnp.where(column_a == a, column_b, -1).reshape(SIDE * n)
    held_at = (jnp.arange(SIDE)[:, None] * CAP_ONE + rank_one).reshape(SIDE * n)
    m = SIDE * n
    before = jnp.arange(m)[None, :] < jnp.arange(m)[:, None]
    rank_two = jnp.sum((relay_b[:, None] == relay_b[None, :]) & before, axis=1)
    wanted = ((relay_b[None, None, :] == jnp.arange(SIDE)[:, None, None])
              & (rank_two[None, None, :] == jnp.arange(CAP_TWO)[None, :, None]))
    pack_two = jnp.sum(jnp.where(wanted, held_at, 0), axis=2)

    final = ((to_a == a) & (to_b == b)).transpose(1, 0, 2)
    rows = final.reshape(SIDE, m)
    rank_end = jnp.sum(rows[:, None, :] & before[None], axis=2)
    number = rows.sum(axis=1)
    per_device = final.reshape(SIDE, SIDE, 2, n_cold)
    slot_before = jnp.arange(n_cold)[None, :] < jnp.arange(n_cold)[:, None]
    slot = jnp.sum(per_device[..., None, :] & slot_before, axis=-1)
    b_from = jnp.arange(SIDE)[:, None, None]
    a_from = jnp.arange(SIDE)[None, :, None]
    source = index_of(core, a_from, b_from, jnp.arange(2)[None, None, :])
    target = (source[..., None] * capacity + slot).reshape(SIDE * m)
    target = jnp.where(rows.reshape(SIDE * m), target, -1)
    position = (jnp.arange(SIDE)[:, None] * CAP_TWO + rank_end).reshape(SIDE * m)
    found = target[None, :] == jnp.arange(owners * capacity)[:, None]
    where_held = jnp.sum(jnp.where(found, position + 1, 0), axis=1) - 1
    return fits, pack_one.reshape(-1), pack_two.reshape(-1), number, where_held


def chip_peer(core, a, b, slot):
    return {"own": index_of(core, lax.rem(a, SIDE), lax.rem(b, SIDE), slot)}


def cold_kernel(one_ref, two_ref, cold_ref, out_ref, held, first, passed, second, sems_s, sems_r, local):
    core, a, b = place()
    n_cold = cold_ref.shape[1]
    barrier = pltpu.get_barrier_semaphore()
    partner = chip_peer(core, a, b, 1 - core)
    pl.semaphore_signal(barrier, inc=1, device_id=partner, device_id_type=MESH)
    for d in range(1, SIDE):
        pl.semaphore_signal(barrier, inc=1, device_id=chip_peer(core, a + d, b, core), device_id_type=MESH)
        pl.semaphore_signal(barrier, inc=1, device_id=chip_peer(core, a, b + d, core), device_id_type=MESH)
    pl.semaphore_wait(barrier, 2 * SIDE - 1)

    swap = pltpu.make_async_remote_copy(
        src_ref=cold_ref.at[1 - core], dst_ref=held.at[pl.ds(core * n_cold, n_cold)],
        send_sem=sems_s.at[0], recv_sem=sems_r.at[0], device_id=partner, device_id_type=MESH)
    swap.start()
    keep = pltpu.make_async_copy(cold_ref.at[core], held.at[pl.ds(core * n_cold, n_cold)], local)
    keep.start()
    keep.wait()
    swap.wait()

    copies = []
    for d in (2, 1, 3, 0):
        to = lax.rem(a + d, SIDE)

        def pack(k, _):
            block = held[one_ref[to * CAP_ONE + k]]
            if d == 0:
                passed[a * CAP_ONE + k] = block
            else:
                first[d - 1, k] = block
            return 0

        lax.fori_loop(0, CAP_ONE, pack, 0)
        if d:
            cp = pltpu.make_async_remote_copy(
                src_ref=first.at[d - 1], dst_ref=passed.at[pl.ds(a * CAP_ONE, CAP_ONE)],
                send_sem=sems_s.at[d], recv_sem=sems_r.at[d],
                device_id=chip_peer(core, a + d, b, core), device_id_type=MESH)
            cp.start()
            copies.append(cp)
    for cp in copies:
        cp.wait()

    copies = []
    for d in (2, 1, 3, 0):
        to = lax.rem(b + d, SIDE)

        def pack(k, _):
            block = passed[two_ref[to * CAP_TWO + k]]
            if d == 0:
                out_ref[b * CAP_TWO + k] = block
            else:
                second[d - 1, k] = block
            return 0

        lax.fori_loop(0, CAP_TWO, pack, 0)
        if d:
            cp = pltpu.make_async_remote_copy(
                src_ref=second.at[d - 1], dst_ref=out_ref.at[pl.ds(b * CAP_TWO, CAP_TWO)],
                send_sem=sems_s.at[SIDE - 1 + d], recv_sem=sems_r.at[SIDE - 1 + d],
                device_id=chip_peer(core, a, b + d, core), device_id_type=MESH)
            cp.start()
            copies.append(cp)
    for cp in copies:
        cp.wait()


def route_cold(pack_one, pack_two, cold):
    _, n_cold, lines, width = cold.shape
    smem = pl.BlockSpec(memory_space=pltpu.SMEM)
    vmem = pl.BlockSpec(memory_space=pltpu.VMEM)
    block = (lines, width)
    return pl.pallas_call(
        cold_kernel,
        out_shape=jax.ShapeDtypeStruct((SIDE * CAP_TWO, *block), cold.dtype),
        in_specs=[smem, smem, pl.BlockSpec(memory_space=pl.ANY)],
        out_specs=vmem,
        scratch_shapes=[
            pltpu.VMEM((2 * n_cold, *block), cold.dtype),
            pltpu.VMEM((SIDE - 1, CAP_ONE, *block), cold.dtype),
            pltpu.VMEM((SIDE * CAP_ONE, *block), cold.dtype),
            pltpu.VMEM((SIDE - 1, CAP_TWO, *block), cold.dtype),
            pltpu.SemaphoreType.DMA((2 * SIDE - 1,)),
            pltpu.SemaphoreType.DMA((2 * SIDE - 1,)),
            pltpu.SemaphoreType.DMA,
        ],
        compiler_params=pltpu.CompilerParams(collective_id=3, has_side_effects=True),
    )(pack_one, pack_two, cold)


def hot_kernel(layer, number_ref, hot_ref, cold_ref, out_ref, step_ref, held, between, relay, onward, final,
               acc, flat, mine, theirs, sem_s, sem_h, sem_b, sem_r, sem_o, sem_f, sem_out, send_sem, recv_sem):
    core, a, b = place()
    star_x, star_z = layer // SIDE, layer % SIDE
    star_a = jnp.where(core == 0, star_x, star_z)
    star_b = jnp.where(core == 0, star_z, star_x)
    da = lax.rem(a + SIDE - star_a, SIDE)
    db = lax.rem(b + SIDE - star_b, SIDE)
    barrier = pltpu.get_barrier_semaphore()
    partner = chip_peer(core, a, b, 1 - core)
    pl.semaphore_signal(barrier, inc=1, device_id=partner, device_id_type=MESH)
    for d in (1, SIDE - 1):
        pl.semaphore_signal(barrier, inc=1, device_id=chip_peer(core, a + d, b, core), device_id_type=MESH)
        pl.semaphore_signal(barrier, inc=1, device_id=chip_peer(core, a, b + d, core), device_id_type=MESH)
    greet()
    pl.semaphore_wait(barrier, 5 + len(rep_peers()))

    def send(src, dst, send_at, recv_at, to):
        return pltpu.make_async_remote_copy(
            src_ref=src, dst_ref=dst, send_sem=send_at, recv_sem=recv_at, device_id=to, device_id_type=MESH)

    def got(ref, sem):
        pltpu.make_async_copy(ref, ref, sem).wait()

    swap = send(hot_ref.at[1 - core], held.at[core], sem_s.at[0], sem_h, partner)
    swap.start()
    keep = pltpu.make_async_copy(hot_ref.at[core], held.at[core], sem_out.at[0])
    keep.start()
    keep.wait()
    other = 1 - core

    def home(da_from, db_from, slot):
        return index_of(core, lax.rem(star_a + da_from, SIDE), lax.rem(star_b + db_from, SIDE), slot)

    def toward(da_from, db_to, slot, src, n, to):
        cps = []
        for at_star in (True, False):
            @pl.when(db == 0 if at_star else db != 0)
            def _(at_star=at_star):
                s = home(da_from, 0, slot)
                if at_star:
                    send(src, final.at[s], sem_s.at[n], sem_f.at[s], to).start()
                else:
                    i = (da_from - 1) * 2 + slot
                    send(src, relay.at[i], sem_s.at[n], sem_r.at[i], to).start()

    for d, step_to, slot_mid in ((1, SIDE - 1, 1), (SIDE - 1, 1, 0)):
        @pl.when(da == d)
        def _(d=d, step_to=step_to, slot_mid=slot_mid):
            to = chip_peer(core, a + step_to, b, core)
            toward(d, db, core, held.at[core], 1, to)
            got(held.at[other], sem_h)
            toward(d, db, other, held.at[other], 2, to)
            got(between, sem_b)
            toward(2, db, slot_mid, between, 3, to)
            for n in range(1, 4):
                got(between, sem_s.at[n])

    @pl.when(da == 2)
    def _():
        for slot, step_to in ((0, 1), (1, SIDE - 1)):
            @pl.when(other == slot)
            def _():
                got(held.at[other], sem_h)
            send(held.at[slot], between, sem_s.at[1 + slot], sem_b, chip_peer(core, a + step_to, b, core)).start()
            @pl.when(core == slot)
            def _():
                pass
        for n in (1, 2):
            got(between, sem_s.at[n])

    def own_and_row(slots):
        order = []
        for da_from in (0, 1, 3, 2):
            for slot in slots:
                order.append((da_from, slot))
        return order

    def ready(da_from, slot):
        if da_from == 0:
            @pl.when(other == slot)
            def _():
                got(held.at[other], sem_h)
            return held.at[slot]
        i = (da_from - 1) * 2 + slot
        got(relay.at[i], sem_r.at[i])
        return relay.at[i]

    @pl.when((da == 0) & (db == 2))
    def _():
        n = 1
        for da_from, slot in own_and_row((0, 1)):
            src = ready(da_from, slot)
            step_to = 1 if slot == 0 else SIDE - 1
            i = {0: 0, 1: 1, 3: 2, 2: 3}[da_from]
            send(src, onward.at[i], sem_s.at[n], sem_o.at[i], chip_peer(core, a, b + step_to, core)).start()
            n += 1
        for k in range(1, n):
            got(between, sem_s.at[k])

    for d, step_to, slot_mid in ((1, SIDE - 1, 1), (SIDE - 1, 1, 0)):
        @pl.when((da == 0) & (db == d))
        def _(d=d, step_to=step_to, slot_mid=slot_mid):
            to = chip_peer(core, a, b + step_to, core)
            n = 1
            for da_from, slot in own_and_row((0, 1)):
                src = ready(da_from, slot)
                s = home(da_from, d, slot)
                send(src, final.at[s], sem_s.at[n], sem_f.at[s], to).start()
                n += 1
            for i, da_from in enumerate((0, 1, 3, 2)):
                got(onward.at[i], sem_o.at[i])
                s = home(da_from, 2, slot_mid)
                send(onward.at[i], final.at[s], sem_s.at[n], sem_f.at[s], to).start()
                n += 1
            for k in range(1, n):
                got(between, sem_s.at[k])

    period = acc.shape[1]
    lines = period // 128

    per = out_blocks = cold_ref.shape[0] // SIDE
    flat[...] = jnp.zeros_like(flat)
    for q in range(SIDE):
        def cold_fold(k, _):
            block = jnp.abs(cold_ref[q * per + k].astype(jnp.float32))
            flat[...] = jnp.maximum(flat[...], jnp.where(k < number_ref[q], block, 0.0))
            return 0
        lax.fori_loop(0, per, cold_fold, 0)
    quads = flat.shape[0] // lines
    row = jnp.concatenate([jnp.max(flat[pl.ds(i, quads, stride=lines), :], axis=0, keepdims=True)
                           for i in range(lines)], axis=1)
    acc[...] = jnp.broadcast_to(row, acc.shape)

    @pl.when((da == 0) & (db == 0))
    def _():
        def take(ref, s, n):
            pltpu.make_async_copy(ref, out_ref.at[s], sem_out.at[n]).start()

            def fold(g, top):
                chunk = ref[:, pl.ds(pl.multiple_of(g * period, 128), period)].astype(jnp.float32)
                return jnp.maximum(top, jnp.abs(chunk))

            acc[...] = lax.fori_loop(0, ref.shape[1] // period, fold, acc[...])

        take(held.at[core], home(0, 0, core), 0)
        got(held.at[other], sem_h)
        take(held.at[other], home(0, 0, other), 1)

        def arrive(s, n):
            got(final.at[s], sem_f.at[s])
            take(final.at[s], s, n)

        def near_and_row(i, _):
            p, slot = i // 2, lax.rem(i, 2)
            da_from = jnp.where(p < 2, p, 5 - p)

            @pl.when(i < 6)
            def _():
                arrive(home(jnp.where(i < 4, 1 + 2 * slot, 2), 0, jnp.where(i < 4, p, slot)), 2 + i)

            def both(side, _):
                arrive(home(da_from, 1 + 2 * side, slot), 8 + 2 * i + side)
                return 0

            lax.fori_loop(0, 2, both, 0)
            return 0

        lax.fori_loop(0, 8, near_and_row, 0)

        def far(i, _):
            p, slot = i // 2, lax.rem(i, 2)
            arrive(home(jnp.where(p < 2, p, 5 - p), 2, slot), 24 + i)
            return 0

        lax.fori_loop(0, 8, far, 0)

        def written(k, _):
            got(between, sem_out.at[k])
            return 0

        lax.fori_loop(0, 32, written, 0)

    swap.wait_send()
    half = period // 4
    top = jnp.max(acc[...], axis=0, keepdims=True)
    parts = [top[:, m * half:(m + 1) * half] for m in range(4)]
    peak = jnp.maximum(jnp.maximum(parts[0], parts[1]), jnp.maximum(parts[2], parts[3]))
    mine[...] = jnp.broadcast_to(peak, mine.shape)
    copies = []
    for i, peer in enumerate(rep_peers()):
        cp = pltpu.make_async_remote_copy(
            src_ref=mine, dst_ref=theirs.at[i], send_sem=send_sem.at[i], recv_sem=recv_sem.at[i],
            device_id={"rep": peer}, device_id_type=MESH)
        cp.start()
        copies.append(cp)
    for cp in copies:
        cp.wait()
    peak = jnp.maximum(jnp.max(theirs[...], axis=0), mine[...])
    step_ref[...] = HEADROOM * jnp.maximum(peak, 1.0) / 127.0


def route_hot(layer, number, hot, cold):
    _, capacity, flat = hot.shape
    owners = lax.axis_size("own")
    peers = lax.axis_size("rep") - 1
    lines, width = cold.shape[1:]
    period = flat // 16
    half = period // 4
    vmem = pl.BlockSpec(memory_space=pltpu.VMEM)
    block = (capacity, flat)
    return pl.pallas_call(
        functools.partial(hot_kernel, layer),
        out_shape=(jax.ShapeDtypeStruct((owners, *block), hot.dtype),
                   jax.ShapeDtypeStruct((8, half), jnp.float32)),
        in_specs=[pl.BlockSpec(memory_space=pltpu.SMEM), pl.BlockSpec(memory_space=pl.ANY), vmem],
        out_specs=(pl.BlockSpec(memory_space=pltpu.HBM), vmem),
        scratch_shapes=[
            pltpu.VMEM((2, *block), hot.dtype),
            pltpu.VMEM(block, hot.dtype),
            pltpu.VMEM((6, *block), hot.dtype),
            pltpu.VMEM((4, *block), hot.dtype),
            pltpu.VMEM((owners, *block), hot.dtype),
            pltpu.VMEM((capacity, period), jnp.float32),
            pltpu.VMEM((lines, width), jnp.float32),
            pltpu.VMEM((8, half), jnp.float32),
            pltpu.VMEM((peers, 8, half), jnp.float32),
            pltpu.SemaphoreType.DMA((13,)),
            pltpu.SemaphoreType.DMA,
            pltpu.SemaphoreType.DMA,
            pltpu.SemaphoreType.DMA((6,)),
            pltpu.SemaphoreType.DMA((4,)),
            pltpu.SemaphoreType.DMA((owners,)),
            pltpu.SemaphoreType.DMA((owners,)),
            pltpu.SemaphoreType.DMA((peers,)),
            pltpu.SemaphoreType.DMA((peers,)),
        ],
        compiler_params=pltpu.CompilerParams(collective_id=4 + layer, has_side_effects=True,
                                             vmem_limit_bytes=50 * 1024 * 1024),
    )(number, hot, cold)


def finish_kernel(period, flag_ref, where_ref, x_ref, cold_ref, step_ref, out_ref, err_ref, wide, flat_step, flat_err):
    i = pl.program_id(0)
    sources, capacity, width = x_ref.shape
    lines = period // 128
    rows = width // 128
    quads = rows // lines
    star = flag_ref[0] == 1
    step_row = step_ref[...]

    @pl.when(i == 0)
    def _():
        err_ref[...] = jnp.zeros_like(err_ref)
        flat_err[...] = jnp.zeros_like(flat_err)
        for k in range(lines):
            flat_step[pl.ds(k, quads, stride=lines), :] = jnp.broadcast_to(
                step_row[:, k * 128:(k + 1) * 128], (quads, 128))

    @pl.when(star)
    def _():
        step = jnp.broadcast_to(step_row, err_ref.shape)
        inverse = 1.0 / step

        def fold(g, total):
            at = pl.ds(pl.multiple_of(g * period, 128), period)
            for s in range(sources):
                values = x_ref[s, :, at].astype(jnp.float32)
                codes = jnp.clip(values * inverse, -127.0, 127.0).astype(jnp.bfloat16)
                out_ref[s, :, at] = codes
                miss = values - codes.astype(jnp.float32) * step
                total = total + miss * miss
            return total

        err_ref[...] = lax.fori_loop(0, width // period, fold, err_ref[...])

    @pl.when(jnp.logical_not(star))
    def _():
        for s in range(sources):
            base = (i * sources + s) * capacity
            first = where_ref[base]

            @pl.when(first < 0)
            def _():
                out_ref[s] = jnp.zeros((capacity, width), jnp.bfloat16)

            @pl.when(first >= 0)
            def _():
                wide[...] = jnp.zeros_like(wide)

                def one(c, _):
                    at = where_ref[base + c]

                    @pl.when(at >= 0)
                    def _():
                        values = cold_ref[at].astype(jnp.float32)
                        codes = jnp.clip(values / flat_step[...], -127.0, 127.0).astype(jnp.bfloat16)
                        codes = codes.astype(jnp.float32)
                        miss = values - codes * flat_step[...]
                        flat_err[...] += miss * miss
                        wide[pl.ds(c, rows, stride=capacity), :] = codes
                    return 0

                lax.fori_loop(0, capacity, one, 0)
                for r in range(rows):
                    out_ref[s, :, r * 128:(r + 1) * 128] = wide[r * capacity:(r + 1) * capacity, :].astype(jnp.bfloat16)

        @pl.when(i == pl.num_programs(0) - 1)
        def _():
            for k in range(lines):
                err_ref[0:1, k * 128:(k + 1) * 128] = jnp.sum(
                    flat_err[pl.ds(k, quads, stride=lines), :], axis=0, keepdims=True)


def finish(flag, where_held, arrived, cold, step_row, period, per_step=4):
    sources, capacity, width = arrived.shape
    rows = width // 128
    smem = pl.BlockSpec(memory_space=pltpu.SMEM)
    return pl.pallas_call(
        functools.partial(finish_kernel, period),
        grid=(sources // per_step,),
        out_shape=(jax.ShapeDtypeStruct(arrived.shape, jnp.bfloat16),
                   jax.ShapeDtypeStruct((capacity, period), jnp.float32)),
        in_specs=[smem, smem,
                  pl.BlockSpec((per_step, capacity, width), lambda i: (i, 0, 0)),
                  pl.BlockSpec(cold.shape, lambda i: (0, 0, 0)),
                  pl.BlockSpec((1, period), lambda i: (0, 0))],
        out_specs=(pl.BlockSpec((per_step, capacity, width), lambda i: (i, 0, 0)),
                   pl.BlockSpec((capacity, period), lambda i: (0, 0))),
        scratch_shapes=[
            pltpu.VMEM((rows * capacity, 128), jnp.float32),
            pltpu.VMEM((rows, 128), jnp.float32),
            pltpu.VMEM((rows, 128), jnp.float32),
        ],
    )(flag, where_held, arrived, cold, step_row)


def body(block_pool, sel_index, sel_layer, counts):
    own_count = lax.axis_size("own")
    rep_count = lax.axis_size("rep")
    layers = own_count // SLICES
    n_select = sel_index.shape[0]
    capacity = n_select // 4
    tokens = block_pool.shape[1]
    half = block_pool.shape[2] // SLICES
    period = 4 * half
    denominator = float(own_count * rep_count * capacity * tokens)
    live = jnp.where(jnp.arange(n_select) < counts[0], sel_layer, -1)
    table = tables(jnp.pad(live, (0, 128 - n_select), constant_values=-1)[None, :])
    fits, pack_one, pack_two, number, where_held = plan(table, capacity)
    star = sel_layer[0]

    def sparse():
        hot, cold = split(block_pool, sel_index, counts, capacity)
        cold = route_cold(pack_one, pack_two, cold)
        arrived, step = lax.switch(
            star, [functools.partial(route_hot, layer) for layer in range(layers)], number, hot, cold)
        step = step[0]
        flag = (lax.axis_index("own") // SLICES == star).astype(jnp.int32)[None]
        codes, err = finish(flag, where_held, arrived, cold, jnp.tile(step, 4)[None, :], period)
        return codes, step, err

    def dense():
        parted = part(block_pool, sel_index, sel_layer, counts, layers, capacity)
        arrived = lax.all_to_all(parted, "own", split_axis=0, concat_axis=0, tiled=True)
        top = jnp.max(peaks(arrived, period)[0].reshape(4, half), axis=0)
        step = HEADROOM * jnp.maximum(top, 1.0) / 127.0
        codes, err = encode(arrived, jnp.tile(step, 4)[None, :], period)
        return codes, step, err

    codes, step, err = lax.cond(fits, sparse, dense)
    error = jnp.sum(totals(err)[0].reshape(4, half), axis=0)
    return codes[None, None], step[None, :], (error / (step * step * denominator))[None, :]


def solution(mesh):
    return jax.shard_map(
        body,
        mesh=mesh,
        in_specs=(
            P(("own", "rep"), None, None),
            P(("own", "rep")),
            P(("own", "rep")),
            P(("own", "rep")),
        ),
        out_specs=(P("own", "rep", None, None, None), P("own", None), P("own", None)),
        check_vma=False,
    )
```

```python
import functools

import jax
import jax.numpy as jnp
from jax import lax
from jax.experimental import pallas as pl
from jax.experimental.pallas import tpu as pltpu
from jax.sharding import PartitionSpec as P

SLICES = 2
HEADROOM = 0.5
MESH = pl.DeviceIdType.MESH


def part_kernel(layers, capacity, half, idx_ref, lay_ref, cnt_ref, pool_ref, out_ref,
                blocks, wide, stage, zeros, slot_of, in_sem, out_sem, zero_sem):
    n_select = idx_ref.shape[0]
    tokens = blocks.shape[1]
    latent = blocks.shape[2]
    for j in range(n_select):
        pltpu.make_async_copy(pool_ref.at[idx_ref[j]], blocks.at[j], in_sem).start()
    live = cnt_ref[0]

    def clear(i, _):
        slot_of[i] = -1
        return 0

    lax.fori_loop(0, layers * capacity + layers, clear, 0)

    def place(j, _):
        layer = lay_ref[j]

        @pl.when(j < live)
        def _():
            rank = slot_of[layers * capacity + layer] + 1
            slot_of[layers * capacity + layer] = rank
            slot_of[layer * capacity + rank] = j
        return 0

    lax.fori_loop(0, n_select, place, 0)
    zeros[...] = jnp.zeros_like(zeros)
    pltpu.make_async_copy(pool_ref.at[pl.ds(0, n_select)], blocks, in_sem).wait()

    def one_layer(layer, used):
        some = slot_of[layers * capacity + layer] >= 0

        @pl.when(jnp.logical_not(some))
        def _():
            cp = pltpu.make_async_copy(zeros, out_ref.at[pl.ds(layer * SLICES, SLICES)], zero_sem)
            cp.start()
            cp.wait()

        @pl.when(some)
        def _():
            @pl.when(used > 0)
            def _():
                pltpu.make_async_copy(stage.at[0], out_ref.at[pl.ds(0, SLICES)], out_sem).wait()
            for c in range(capacity):
                j = slot_of[layer * capacity + c]

                @pl.when(j >= 0)
                def _():
                    for k in range(wide.shape[0]):
                        cols = min(128, latent - k * 128)
                        wide[k, pl.ds(c * tokens, tokens), :cols] = blocks[j, :, k * 128:k * 128 + cols].astype(jnp.float32)

                @pl.when(j < 0)
                def _():
                    wide[:, pl.ds(c * tokens, tokens), :] = jnp.zeros((wide.shape[0], tokens, 128), jnp.float32)

            def four(q, _):
                rows = [jnp.concatenate([wide[k, pl.ds(4 * q + m, capacity, stride=tokens), :]
                                         for k in range(wide.shape[0])], axis=1) for m in range(4)]
                for h in range(SLICES):
                    flat = jnp.concatenate([r[:, h * half:(h + 1) * half] for r in rows], axis=1)
                    stage[0, h, :, pl.ds(pl.multiple_of(q * 4 * half, 128), 4 * half)] = flat.astype(jnp.bfloat16)
                return 0

            lax.fori_loop(0, tokens // 4, four, 0)
            pltpu.make_async_copy(stage.at[0], out_ref.at[pl.ds(layer * SLICES, SLICES)], out_sem).start()
        return used + some.astype(jnp.int32)

    used = lax.fori_loop(0, layers, one_layer, 0)

    @pl.when(used > 0)
    def _():
        pltpu.make_async_copy(stage.at[0], out_ref.at[pl.ds(0, SLICES)], out_sem).wait()


def part(block_pool, sel_index, sel_layer, counts, layers, capacity):
    rows, tokens, latent = block_pool.shape
    half = latent // SLICES
    n_select = sel_index.shape[0]
    groups = layers * SLICES
    smem = pl.BlockSpec(memory_space=pltpu.SMEM)
    return pl.pallas_call(
        functools.partial(part_kernel, layers, capacity, half),
        out_shape=jax.ShapeDtypeStruct((groups, capacity, tokens * half), jnp.bfloat16),
        in_specs=[smem, smem, smem, pl.BlockSpec(memory_space=pltpu.HBM)],
        out_specs=pl.BlockSpec(memory_space=pltpu.HBM),
        scratch_shapes=[
            pltpu.VMEM((n_select, tokens, latent), jnp.bfloat16),
            pltpu.VMEM((-(-latent // 128), capacity * tokens, 128), jnp.float32),
            pltpu.VMEM((1, SLICES, capacity, tokens * half), jnp.bfloat16),
            pltpu.VMEM((SLICES, capacity, tokens * half), jnp.bfloat16),
            pltpu.SMEM((layers * capacity + layers,), jnp.int32),
            pltpu.SemaphoreType.DMA,
            pltpu.SemaphoreType.DMA,
            pltpu.SemaphoreType.DMA,
        ],
    )(sel_index, sel_layer, counts, block_pool)


def rep_peers():
    me = lax.axis_index("rep")
    count = lax.axis_size("rep")
    return [lax.rem(me + d, count) for d in range(1, count)]


def greet():
    barrier = pltpu.get_barrier_semaphore()
    for peer in rep_peers():
        pl.semaphore_signal(barrier, inc=1, device_id={"rep": peer}, device_id_type=MESH)


def share(mine, theirs, send_sem, recv_sem):
    pl.semaphore_wait(pltpu.get_barrier_semaphore(), len(rep_peers()))
    copies = []
    for i, peer in enumerate(rep_peers()):
        cp = pltpu.make_async_remote_copy(
            src_ref=mine, dst_ref=theirs.at[i], send_sem=send_sem.at[i], recv_sem=recv_sem.at[i],
            device_id={"rep": peer}, device_id_type=MESH)
        cp.start()
        copies.append(cp)
    for cp in copies:
        cp.wait()


def peak_kernel(steps, period, x_ref, out_ref, acc, mine, theirs, send_sem, recv_sem):
    i = pl.program_id(0)

    @pl.when(i == 0)
    def _():
        greet()
        acc[...] = jnp.zeros_like(acc)

    def fold(g, top):
        chunk = x_ref[:, :, pl.ds(pl.multiple_of(g * period, 128), period)].astype(jnp.float32)
        return jnp.maximum(top, jnp.max(jnp.abs(chunk), axis=0))

    acc[...] = lax.fori_loop(0, x_ref.shape[2] // period, fold, acc[...])

    @pl.when(i == steps - 1)
    def _():
        mine[...] = jnp.broadcast_to(jnp.max(acc[...], axis=0, keepdims=True), mine.shape)
        share(mine, theirs, send_sem, recv_sem)
        out_ref[...] = jnp.maximum(jnp.max(theirs[...], axis=0), mine[...])


def peaks(arrived, period, per_step=4):
    sources, capacity, flat = arrived.shape
    steps = sources // per_step
    peers = lax.axis_size("rep") - 1
    return pl.pallas_call(
        functools.partial(peak_kernel, steps, period),
        grid=(steps,),
        out_shape=jax.ShapeDtypeStruct((8, period), jnp.float32),
        in_specs=[pl.BlockSpec((per_step, capacity, flat), lambda i: (i, 0, 0))],
        out_specs=pl.BlockSpec((8, period), lambda i: (0, 0)),
        scratch_shapes=[
            pltpu.VMEM((capacity, period), jnp.float32),
            pltpu.VMEM((8, period), jnp.float32),
            pltpu.VMEM((peers, 8, period), jnp.float32),
            pltpu.SemaphoreType.DMA((peers,)),
            pltpu.SemaphoreType.DMA((peers,)),
        ],
        compiler_params=pltpu.CompilerParams(collective_id=0, has_side_effects=True),
    )(arrived)


def code_kernel(period, x_ref, step_ref, out_ref, err_ref):
    @pl.when(pl.program_id(0) == 0)
    def _():
        err_ref[...] = jnp.zeros_like(err_ref)

    step = jnp.broadcast_to(step_ref[...], err_ref.shape)
    inverse = 1.0 / step

    def fold(g, total):
        at = pl.ds(pl.multiple_of(g * period, 128), period)
        for s in range(x_ref.shape[0]):
            values = x_ref[s, :, at].astype(jnp.float32)
            codes = jnp.clip(values * inverse, -127.0, 127.0).astype(jnp.bfloat16)
            out_ref[s, :, at] = codes
            miss = values - codes.astype(jnp.float32) * step
            total = total + miss * miss
        return total

    err_ref[...] = lax.fori_loop(0, x_ref.shape[2] // period, fold, err_ref[...])


def encode(arrived, step_row, period, per_step=4):
    sources, capacity, flat = arrived.shape
    return pl.pallas_call(
        functools.partial(code_kernel, period),
        grid=(sources // per_step,),
        out_shape=(jax.ShapeDtypeStruct(arrived.shape, jnp.bfloat16),
                   jax.ShapeDtypeStruct((capacity, period), jnp.float32)),
        in_specs=[pl.BlockSpec((per_step, capacity, flat), lambda i: (i, 0, 0)),
                  pl.BlockSpec((1, period), lambda i: (0, 0))],
        out_specs=(pl.BlockSpec((per_step, capacity, flat), lambda i: (i, 0, 0)),
                   pl.BlockSpec((capacity, period), lambda i: (0, 0))),
    )(arrived, step_row)


def total_kernel(denominator, err_ref, step_ref, out_ref, mine, theirs, send_sem, recv_sem):
    greet()
    half = step_ref.shape[1]
    row = jnp.sum(err_ref[...], axis=0, keepdims=True)
    parts = [row[:, m * half:(m + 1) * half] for m in range(4)]
    mine[...] = jnp.broadcast_to((parts[0] + parts[1]) + (parts[2] + parts[3]), mine.shape)
    share(mine, theirs, send_sem, recv_sem)
    total = (jnp.sum(theirs[...], axis=0) + mine[...])[0:1]
    step = step_ref[...]
    out_ref[...] = total / (step * step * denominator)


def totals(err, step, denominator):
    half = step.shape[1]
    peers = lax.axis_size("rep") - 1
    vmem = pl.BlockSpec(memory_space=pltpu.VMEM)
    return pl.pallas_call(
        functools.partial(total_kernel, denominator),
        out_shape=jax.ShapeDtypeStruct((1, half), jnp.float32),
        in_specs=[vmem, vmem],
        out_specs=vmem,
        scratch_shapes=[
            pltpu.VMEM((8, half), jnp.float32),
            pltpu.VMEM((peers, 8, half), jnp.float32),
            pltpu.SemaphoreType.DMA((peers,)),
            pltpu.SemaphoreType.DMA((peers,)),
        ],
        compiler_params=pltpu.CompilerParams(collective_id=1, has_side_effects=True),
    )(err, step)


SIDE = 4
CAP_ONE = 20
CAP_TWO = 16
BY_LAYER, BY_SIDE, LIVE = 32, 48, 56


def open_kernel(half, idx_ref, lay_ref, cnt_ref, pool_ref, hot_ref, cold_ref, table_ref,
                pool, wide, flat, row_ref, pool_sem, own_send, own_recv, send_sem, recv_sem):
    n_select = idx_ref.shape[0]
    tokens, latent = pool.shape[1], pool.shape[2]
    capacity = hot_ref.shape[1]
    tiles = wide.shape[0]
    fetch = pltpu.make_async_copy(pool_ref, pool, pool_sem)
    fetch.start()
    me, mine = lax.axis_index("own"), lax.axis_index("rep")
    owners = lax.axis_size("own")
    barrier = pltpu.get_barrier_semaphore()

    def hello(i, _):
        pl.semaphore_signal(barrier, inc=1, device_id={"own": lax.rem(me + i, owners)}, device_id_type=MESH)
        return 0

    lax.fori_loop(1, owners, hello, 0)
    greet()

    lane = lax.broadcasted_iota(jnp.int32, (1, 128), 1)
    live = cnt_ref[0]
    row = jnp.where(lane == LIVE, live, jnp.where(lane < BY_LAYER, -1, 0))
    for j in range(n_select):
        layer = lay_ref[j]
        is_live = jnp.where(j < live, 1, 0)
        row = jnp.where(lane == j, jnp.where(j < live, layer, -1), row)
        if j >= capacity:
            spot = ((lane == BY_LAYER + layer) | (lane == BY_SIDE + lax.shift_right_logical(layer, 2))
                    | (lane == BY_SIDE + SIDE + (layer & (SIDE - 1))))
            row = row + jnp.where(spot, is_live, 0)
    row_ref[...] = row
    table_ref[mine, me] = row
    pl.semaphore_wait(barrier, owners - 1 + len(rep_peers()))

    def push(i, _):
        pltpu.make_async_remote_copy(
            src_ref=row_ref, dst_ref=table_ref.at[mine, me], send_sem=own_send, recv_sem=own_recv,
            device_id={"own": lax.rem(me + i, owners)}, device_id_type=MESH).start()
        return 0

    lax.fori_loop(1, owners, push, 0)
    fetch.wait()

    def widen(j, to):
        at = idx_ref[j]
        for k in range(tiles):
            cols = min(128, latent - k * 128)
            wide[k, pl.ds(to, tokens), :cols] = pool[at, :, k * 128:k * 128 + cols].astype(jnp.float32)

    def strided(start, count, stride):
        return jnp.concatenate([wide[k, pl.ds(start, count, stride=stride), :] for k in range(tiles)], axis=1)

    for c in range(capacity):
        widen(c, c * tokens)

    def four(q, _):
        rows = [strided(4 * q + m, capacity, tokens) for m in range(4)]
        for h in range(SLICES):
            line = jnp.concatenate([r[:, h * half:(h + 1) * half] for r in rows], axis=1)
            hot_ref[h, :, pl.ds(pl.multiple_of(q * 4 * half, 128), 4 * half)] = line.astype(jnp.bfloat16)
        return 0

    lax.fori_loop(0, tokens // 4, four, 0)

    rest = table_ref.at[mine, pl.ds(0, owners - 1)]
    pltpu.make_async_copy(rest, rest, own_recv).wait()
    pltpu.make_async_copy(rest, rest, own_send).wait()
    copies = []
    for i, peer in enumerate(rep_peers()):
        cp = pltpu.make_async_remote_copy(
            src_ref=table_ref.at[mine], dst_ref=table_ref.at[mine], send_sem=send_sem.at[i], recv_sem=recv_sem.at[i],
            device_id={"rep": peer}, device_id_type=MESH)
        cp.start()
        copies.append(cp)

    quads = tokens // 4
    lines = 4 * half // 128

    def one(j, _):
        widen(j, 0)
        rows = [strided(m, quads, 4) for m in range(4)]
        for h in range(SLICES):
            line = jnp.concatenate([r[:, h * half:(h + 1) * half] for r in rows], axis=1)
            for i in range(lines):
                flat[h, pl.ds(i, quads, stride=lines), :] = line[:, i * 128:(i + 1) * 128]
        for h in range(SLICES):
            cold_ref[h, j - capacity] = flat[h].astype(jnp.bfloat16)
        return 0

    lax.fori_loop(capacity, n_select, one, 0)
    for cp in copies:
        cp.wait()


def open_exchange(block_pool, sel_index, sel_layer, counts, capacity):
    _, tokens, latent = block_pool.shape
    half = latent // SLICES
    n_select = sel_index.shape[0]
    lines = tokens * half // 128
    owners, reps = lax.axis_size("own"), lax.axis_size("rep")
    smem = pl.BlockSpec(memory_space=pltpu.SMEM)
    vmem = pl.BlockSpec(memory_space=pltpu.VMEM)
    return pl.pallas_call(
        functools.partial(open_kernel, half),
        out_shape=(jax.ShapeDtypeStruct((SLICES, capacity, tokens * half), jnp.bfloat16),
                   jax.ShapeDtypeStruct((SLICES, n_select - capacity, lines, 128), jnp.bfloat16),
                   jax.ShapeDtypeStruct((reps, owners, 1, 128), jnp.int32)),
        in_specs=[smem, smem, smem, pl.BlockSpec(memory_space=pltpu.HBM)],
        out_specs=(vmem, vmem, vmem),
        scratch_shapes=[
            pltpu.VMEM(block_pool.shape, jnp.bfloat16),
            pltpu.VMEM((-(-latent // 128), capacity * tokens, 128), jnp.float32),
            pltpu.VMEM((SLICES, lines, 128), jnp.float32),
            pltpu.VMEM((1, 128), jnp.int32),
            pltpu.SemaphoreType.DMA,
            pltpu.SemaphoreType.DMA,
            pltpu.SemaphoreType.DMA,
            pltpu.SemaphoreType.DMA((reps - 1,)),
            pltpu.SemaphoreType.DMA((reps - 1,)),
        ],
        compiler_params=pltpu.CompilerParams(collective_id=2, has_side_effects=True),
    )(sel_index, sel_layer, counts, block_pool)


def place():
    me = lax.axis_index("own")
    core = lax.rem(me, 2)
    x, z = me // (2 * SIDE), lax.rem(me // 2, SIDE)
    return core, jnp.where(core == 0, x, z), jnp.where(core == 0, z, x)


def index_of(core, a, b, slot):
    return jnp.where(core == 0, a * SIDE + b, b * SIDE + a) * 2 + slot


def chip_peer(core, a, b, slot):
    return {"own": index_of(core, lax.rem(a, SIDE), lax.rem(b, SIDE), slot)}


def plan_kernel(capacity, n_cold, table_ref, rows_ref, fits_ref, one_ref, two_ref, number_ref, where_ref, flag_ref,
                near, rank_one, rank_two, sem):
    core, a, b = place()
    me = lax.axis_index("own")
    cp = pltpu.make_async_copy(rows_ref.at[lax.axis_index("rep")], near, sem)
    cp.start()
    reps, owners = table_ref.shape[0], table_ref.shape[1]
    lane = lax.broadcasted_iota(jnp.int32, (1, 128), 1)
    one, two = jnp.zeros((1, 128), jnp.int32), jnp.zeros((1, 128), jnp.int32)
    for r in range(reps):
        chips = [table_ref[r, 2 * c] + table_ref[r, 2 * c + 1] for c in range(SIDE * SIDE)]
        for c in chips:
            one = jnp.maximum(one, c)
        for i in range(SIDE):
            for picked in (chips[i::SIDE], chips[SIDE * i:SIDE * i + SIDE]):
                two = jnp.maximum(two, (picked[0] + picked[1]) + (picked[2] + picked[3]))
    one = jnp.where((lane >= BY_SIDE) & (lane < LIVE), one, 0).astype(jnp.float32)
    two = jnp.where((lane >= BY_LAYER) & (lane < BY_SIDE), two, 0).astype(jnp.float32)
    fits_ref[0] = jnp.where(jnp.logical_and(jnp.max(one) <= CAP_ONE, jnp.max(two) <= CAP_TWO), 1, 0)

    def clear(ref, value):
        def put(i, _):
            ref[i] = value
            return 0
        lax.fori_loop(0, ref.shape[0], put, 0, unroll=8 if ref.shape[0] % 8 == 0 else 1)

    clear(one_ref, 0)
    clear(two_ref, 0)
    clear(number_ref, 0)
    clear(where_ref, -1)
    clear(rank_two, 0)
    cp.wait()
    layer_here = me // 2
    flag_ref[0] = jnp.where(near[0, 0, 0] == layer_here, 1, 0)

    def column(a_from, _):
        clear(rank_one, 0)
        for slot in range(2):
            device = index_of(core, a_from, b, slot)

            def entry(j, _):
                layer = near[device, 0, j]
                high, low = lax.shift_right_logical(layer, 2), layer & (SIDE - 1)
                to_a = jnp.where(core == 0, high, low)
                to_b = jnp.where(core == 0, low, high)
                first = rank_one[to_a]
                rank_one[to_a] = first + 1
                first = jnp.minimum(first, CAP_ONE - 1)

                @pl.when(a_from == a)
                def _():
                    one_ref[to_a * CAP_ONE + first] = slot * n_cold + j - capacity

                @pl.when(to_a == a)
                def _():
                    second = rank_two[to_b]
                    rank_two[to_b] = second + 1
                    two_ref[to_b * CAP_TWO + jnp.minimum(second, CAP_TWO - 1)] = a_from * CAP_ONE + first
                return 0

            lax.fori_loop(capacity, near[device, 0, LIVE], entry, 0)
        return 0

    lax.fori_loop(0, SIDE, column, 0)

    def arriving(n, _):
        b_from, a_from, slot = n // (2 * SIDE), lax.rem(n // 2, SIDE), lax.rem(n, 2)
        device = index_of(core, a_from, b_from, slot)

        @pl.when(near[device, 0, BY_LAYER + layer_here] > 0)
        def _():
            def entry(j, held):
                hit = near[device, 0, j] == layer_here

                @pl.when(hit)
                def _():
                    count = number_ref[b_from]
                    number_ref[b_from] = count + 1
                    where_ref[device * capacity + held] = b_from * CAP_TWO + count
                return held + jnp.where(hit, 1, 0)

            lax.fori_loop(capacity, near[device, 0, LIVE], entry, 0)
        return 0

    lax.fori_loop(0, owners, arriving, 0)


def plan(table, capacity, n_cold):
    reps, owners = table.shape[0], table.shape[1]
    smem = pl.BlockSpec(memory_space=pltpu.SMEM)
    sizes = (1, SIDE * CAP_ONE, SIDE * CAP_TWO, SIDE, owners * capacity, 1)
    return pl.pallas_call(
        functools.partial(plan_kernel, capacity, n_cold),
        out_shape=tuple(jax.ShapeDtypeStruct((n,), jnp.int32) for n in sizes),
        in_specs=[pl.BlockSpec(memory_space=pltpu.VMEM), pl.BlockSpec(memory_space=pl.ANY)],
        out_specs=tuple(smem for _ in sizes),
        scratch_shapes=[
            pltpu.SMEM((owners, 1, 128), jnp.int32),
            pltpu.SMEM((SIDE,), jnp.int32),
            pltpu.SMEM((SIDE,), jnp.int32),
            pltpu.SemaphoreType.DMA,
        ],
    )(table, table)


def route_kernel(layer, one_ref, two_ref, number_ref, hot_ref, cold_ref, out_ref, landed, row_ref,
                 final, held, first, passed, second, acc, flat, mine, theirs,
                 sem_send, sem_block, sem_out, sems_s, sems_r, local, send_sem, recv_sem):
    core, a, b = place()
    me = lax.axis_index("own")
    other = 1 - core
    beside = index_of(core, a, b, other)
    n_cold = cold_ref.shape[1]
    star_x, star_z = layer // SIDE, layer % SIDE
    star_a = jnp.where(core == 0, star_x, star_z)
    star_b = jnp.where(core == 0, star_z, star_x)
    da = lax.rem(a + SIDE - star_a, SIDE)
    db = lax.rem(b + SIDE - star_b, SIDE)
    relay = jnp.logical_and(da == 0, db != 0)
    star = jnp.logical_and(da == 0, db == 0)
    barrier = pltpu.get_barrier_semaphore()
    partner = chip_peer(core, a, b, other)
    pl.semaphore_signal(barrier, inc=1, device_id=partner, device_id_type=MESH)
    for d in range(1, SIDE):
        pl.semaphore_signal(barrier, inc=1, device_id=chip_peer(core, a + d, b, core), device_id_type=MESH)
        pl.semaphore_signal(barrier, inc=1, device_id=chip_peer(core, a, b + d, core), device_id_type=MESH)
    greet()
    keep_hot = pltpu.make_async_copy(hot_ref.at[core], final.at[me], local.at[0])
    keep_hot.start()
    keep_cold = pltpu.make_async_copy(cold_ref.at[core], held.at[pl.ds(core * n_cold, n_cold)], local.at[1])
    keep_cold.start()
    pl.semaphore_wait(barrier, 2 * SIDE - 1 + len(rep_peers()))

    def send(src, dst, send_at, recv_at, to):
        return pltpu.make_async_remote_copy(
            src_ref=src, dst_ref=dst, send_sem=send_at, recv_sem=recv_at, device_id=to, device_id_type=MESH)

    swap_cold = send(cold_ref.at[other], held.at[pl.ds(core * n_cold, n_cold)], sems_s.at[0], sems_r.at[0], partner)
    swap_cold.start()
    swap_hot = send(hot_ref.at[other], final.at[me], sem_send.at[0], sem_block.at[me], partner)
    swap_hot.start()
    keep_hot.wait()

    dist = jnp.where(da != 0, da, db)

    def onward(slot):
        step = jnp.where(dist == 2, jnp.where(slot == 0, 1, SIDE - 1), SIDE - dist)
        return chip_peer(core, a + jnp.where(da != 0, step, 0), b + jnp.where(da != 0, 0, step), core)

    def forward(s, n, slot):
        send(final.at[s], final.at[s], sem_send.at[n], sem_block.at[s], onward(slot)).start()

    def got(s):
        pltpu.make_async_copy(final.at[s], final.at[s], sem_block.at[s]).wait()

    @pl.when(jnp.logical_not(star))
    def _():
        forward(me, 1, core)
        got(beside)
        forward(beside, 2, other)

    keep_cold.wait()
    swap_cold.wait()

    def pack(src, table, at, dst, start, count):
        def body(k, _):
            dst[start + k] = src[table[at + k]]
            return 0
        lax.fori_loop(0, count, body, 0)

    copies = []
    for d in (2, 1, 3):
        pack(held, one_ref, lax.rem(a + d, SIDE) * CAP_ONE, first, (d - 1) * CAP_ONE, CAP_ONE)
        cp = send(first.at[pl.ds((d - 1) * CAP_ONE, CAP_ONE)], passed.at[pl.ds(a * CAP_ONE, CAP_ONE)],
                  sems_s.at[d], sems_r.at[d], chip_peer(core, a + d, b, core))
        cp.start()
        copies.append(cp)
    pack(held, one_ref, a * CAP_ONE, passed, a * CAP_ONE, CAP_ONE)

    @pl.when(jnp.logical_or(da == 1, da == 3))
    def _():
        slot = jnp.where(da == 1, 1, 0)
        s = index_of(core, lax.rem(star_a + 2, SIDE), b, slot)
        got(s)
        forward(s, 3, slot)

    for cp in copies:
        cp.wait()
    copies = []
    for d in (2, 1, 3):
        pack(passed, two_ref, lax.rem(b + d, SIDE) * CAP_TWO, second, (d - 1) * CAP_TWO, CAP_TWO)
        cp = send(second.at[pl.ds((d - 1) * CAP_TWO, CAP_TWO)], landed.at[pl.ds(b * CAP_TWO, CAP_TWO)],
                  sems_s.at[SIDE - 1 + d], sems_r.at[SIDE - 1 + d], chip_peer(core, a, b + d, core))
        cp.start()
        copies.append(cp)
    pack(passed, two_ref, b * CAP_TWO, landed, b * CAP_TWO, CAP_TWO)

    def of(a_from, b_from, slot):
        return index_of(core, lax.rem(star_a + a_from, SIDE), lax.rem(star_b + b_from, SIDE), slot)

    def row_order(p):
        return jnp.where(p < 2, p, 5 - p)

    @pl.when(relay)
    def _():
        def row_block(i, _):
            slot = lax.rem(i, 2)
            s = of(row_order(i // 2), db, slot)
            got(s)
            forward(s, 1 + i, slot)
            return 0

        lax.fori_loop(2, 2 * SIDE, row_block, 0)

        @pl.when(db != 2)
        def _():
            slot = jnp.where(db == 1, 1, 0)

            def far_block(p, _):
                s = of(row_order(p), 2, slot)
                got(s)
                forward(s, 2 * SIDE + 1 + p, slot)
                return 0

            lax.fori_loop(0, SIDE, far_block, 0)

    period = acc.shape[1]
    lines = period // 128

    @pl.when(star)
    def _():
        acc[...] = jnp.zeros_like(acc)

        def take(s, n):
            pltpu.make_async_copy(final.at[s], out_ref.at[s], sem_out.at[n]).start()

            def fold(g, top):
                chunk = final[s, :, pl.ds(pl.multiple_of(g * period, 128), period)].astype(jnp.float32)
                return jnp.maximum(top, jnp.abs(chunk))

            acc[...] = lax.fori_loop(0, final.shape[2] // period, fold, acc[...])

        take(me, 0)

        def arrive(n, _):
            i = n - 2
            step, which = i // 3, lax.rem(i, 3)
            early = i < 18
            row_a = jnp.where(step < 4, 1 + 2 * lax.rem(step, 2), 2)
            row_slot = jnp.where(step < 4, step // 2, step - 4)
            near_step = jnp.where(early, step, 6 + (i - 18) // 2)
            near_b = jnp.where(early, which * 2 - 1, 1 + 2 * lax.rem(i - 18, 2))
            far_step = i - 22
            is_row = jnp.logical_and(early, which == 0)
            is_far = i >= 22
            block_step = jnp.where(is_far, far_step, near_step)
            from_a = jnp.where(is_row, row_a, row_order(block_step // 2))
            from_b = jnp.where(is_row, 0, jnp.where(is_far, 2, near_b))
            slot = jnp.where(is_row, row_slot, lax.rem(block_step, 2))
            s = jnp.where(n == 1, beside, of(from_a, from_b, slot))
            got(s)
            take(s, n)
            return 0

        lax.fori_loop(1, 32, arrive, 0)

    for cp in copies:
        cp.wait()

    @pl.when(jnp.logical_not(star))
    def _():
        flat[...] = jnp.zeros_like(flat)
        for q in range(SIDE):
            def cold_fold(k, _):
                block = jnp.abs(landed[q * CAP_TWO + k].astype(jnp.float32))
                flat[...] = jnp.maximum(flat[...], jnp.where(k < number_ref[q], block, 0.0))
                return 0
            lax.fori_loop(0, CAP_TWO, cold_fold, 0)
        quads = flat.shape[0] // lines
        row = jnp.concatenate([jnp.max(flat[pl.ds(i, quads, stride=lines), :], axis=0, keepdims=True)
                               for i in range(lines)], axis=1)
        acc[...] = jnp.broadcast_to(row, acc.shape)

    half = period // 4
    top = jnp.max(acc[...], axis=0, keepdims=True)
    parts = [top[:, m * half:(m + 1) * half] for m in range(4)]
    peak = jnp.maximum(jnp.maximum(parts[0], parts[1]), jnp.maximum(parts[2], parts[3]))
    mine[...] = jnp.broadcast_to(peak, mine.shape)
    swap_hot.wait_send()

    def drained(n, _):
        pltpu.make_async_copy(final.at[0], final.at[0], sem_send.at[n]).wait()
        return 0

    sent = jnp.where(da != 0, jnp.where(da == 2, 2, 3), jnp.where(db == 0, 0, jnp.where(db == 2, 8, 12)))
    lax.fori_loop(1, sent + 1, drained, 0)
    copies = []
    for i, peer in enumerate(rep_peers()):
        cp = send(mine, theirs.at[i], send_sem.at[i], recv_sem.at[i], {"rep": peer})
        cp.start()
        copies.append(cp)

    @pl.when(star)
    def _():
        def written(n, _):
            pltpu.make_async_copy(final.at[0], final.at[0], sem_out.at[n]).wait()
            return 0

        lax.fori_loop(0, 32, written, 0)

    for cp in copies:
        cp.wait()
    peak = jnp.maximum(jnp.max(theirs[...], axis=0), mine[...])
    step = HEADROOM * jnp.maximum(peak, 1.0) / 127.0
    row_ref[...] = jnp.concatenate([step] * 4, axis=1)


def route(layer, one, two, number, hot, cold):
    _, capacity, flat = hot.shape
    owners = lax.axis_size("own")
    peers = lax.axis_size("rep") - 1
    _, n_cold, lines, width = cold.shape
    period = flat // 16
    half = period // 4
    smem = pl.BlockSpec(memory_space=pltpu.SMEM)
    vmem = pl.BlockSpec(memory_space=pltpu.VMEM)
    block, small = (capacity, flat), (lines, width)
    return pl.pallas_call(
        functools.partial(route_kernel, layer),
        out_shape=(jax.ShapeDtypeStruct((owners, *block), hot.dtype),
                   jax.ShapeDtypeStruct((SIDE * CAP_TWO, *small), cold.dtype),
                   jax.ShapeDtypeStruct((8, period), jnp.float32)),
        in_specs=[smem, smem, smem, pl.BlockSpec(memory_space=pl.ANY), pl.BlockSpec(memory_space=pl.ANY)],
        out_specs=(pl.BlockSpec(memory_space=pltpu.HBM), vmem, vmem),
        scratch_shapes=[
            pltpu.VMEM((owners, *block), hot.dtype),
            pltpu.VMEM((2 * n_cold, *small), cold.dtype),
            pltpu.VMEM(((SIDE - 1) * CAP_ONE, *small), cold.dtype),
            pltpu.VMEM((SIDE * CAP_ONE, *small), cold.dtype),
            pltpu.VMEM(((SIDE - 1) * CAP_TWO, *small), cold.dtype),
            pltpu.VMEM((capacity, period), jnp.float32),
            pltpu.VMEM((lines, width), jnp.float32),
            pltpu.VMEM((8, half), jnp.float32),
            pltpu.VMEM((peers, 8, half), jnp.float32),
            pltpu.SemaphoreType.DMA((13,)),
            pltpu.SemaphoreType.DMA((owners,)),
            pltpu.SemaphoreType.DMA((owners,)),
            pltpu.SemaphoreType.DMA((2 * SIDE - 1,)),
            pltpu.SemaphoreType.DMA((2 * SIDE - 1,)),
            pltpu.SemaphoreType.DMA((2,)),
            pltpu.SemaphoreType.DMA((peers,)),
            pltpu.SemaphoreType.DMA((peers,)),
        ],
        compiler_params=pltpu.CompilerParams(collective_id=4 + layer, has_side_effects=True,
                                             vmem_limit_bytes=50 * 1024 * 1024),
    )(one, two, number, hot, cold)


def finish_kernel(period, flag_ref, where_ref, x_ref, cold_ref, step_ref, out_ref, err_ref, step_out, wide, flat_step, flat_err):
    i = pl.program_id(0)
    sources, capacity, width = x_ref.shape
    lines = period // 128
    rows = width // 128
    quads = rows // lines
    star = flag_ref[0] == 1
    step_row = step_ref[0:1]

    @pl.when(i == 0)
    def _():
        step_out[...] = step_row[:, :step_out.shape[1]]
        err_ref[...] = jnp.zeros_like(err_ref)
        flat_err[...] = jnp.zeros_like(flat_err)
        for k in range(lines):
            flat_step[pl.ds(k, quads, stride=lines), :] = jnp.broadcast_to(
                step_row[:, k * 128:(k + 1) * 128], (quads, 128))

    @pl.when(star)
    def _():
        step = jnp.broadcast_to(step_row, err_ref.shape)
        inverse = 1.0 / step

        def fold(g, total):
            at = pl.ds(pl.multiple_of(g * period, 128), period)
            for s in range(sources):
                values = x_ref[s, :, at].astype(jnp.float32)
                codes = jnp.clip(values * inverse, -127.0, 127.0).astype(jnp.bfloat16)
                out_ref[s, :, at] = codes
                miss = values - codes.astype(jnp.float32) * step
                total = total + miss * miss
            return total

        err_ref[...] = lax.fori_loop(0, width // period, fold, err_ref[...])

    @pl.when(jnp.logical_not(star))
    def _():
        for s in range(sources):
            base = (i * sources + s) * capacity
            first = where_ref[base]

            @pl.when(first < 0)
            def _():
                out_ref[s] = jnp.zeros((capacity, width), jnp.bfloat16)

            @pl.when(first >= 0)
            def _():
                wide[...] = jnp.zeros_like(wide)

                def one(c, _):
                    at = where_ref[base + c]

                    @pl.when(at >= 0)
                    def _():
                        values = cold_ref[at].astype(jnp.float32)
                        codes = jnp.clip(values / flat_step[...], -127.0, 127.0).astype(jnp.bfloat16)
                        codes = codes.astype(jnp.float32)
                        miss = values - codes * flat_step[...]
                        flat_err[...] += miss * miss
                        wide[pl.ds(c, rows, stride=capacity), :] = codes
                    return 0

                lax.fori_loop(0, capacity, one, 0)
                for r in range(rows):
                    out_ref[s, :, r * 128:(r + 1) * 128] = wide[r * capacity:(r + 1) * capacity, :].astype(jnp.bfloat16)

        @pl.when(i == pl.num_programs(0) - 1)
        def _():
            for k in range(lines):
                err_ref[0:1, k * 128:(k + 1) * 128] = jnp.sum(
                    flat_err[pl.ds(k, quads, stride=lines), :], axis=0, keepdims=True)


def finish(flag, where_held, arrived, cold, step_row, period, per_step=4):
    sources, capacity, width = arrived.shape
    rows = width // 128
    smem = pl.BlockSpec(memory_space=pltpu.SMEM)
    return pl.pallas_call(
        functools.partial(finish_kernel, period),
        grid=(sources // per_step,),
        out_shape=(jax.ShapeDtypeStruct(arrived.shape, jnp.bfloat16),
                   jax.ShapeDtypeStruct((capacity, period), jnp.float32),
                   jax.ShapeDtypeStruct((1, period // 4), jnp.float32)),
        in_specs=[smem, smem,
                  pl.BlockSpec((per_step, capacity, width), lambda i: (i, 0, 0)),
                  pl.BlockSpec(cold.shape, lambda i: (0, 0, 0)),
                  pl.BlockSpec((8, period), lambda i: (0, 0))],
        out_specs=(pl.BlockSpec((per_step, capacity, width), lambda i: (i, 0, 0)),
                   pl.BlockSpec((capacity, period), lambda i: (0, 0)),
                   pl.BlockSpec((1, period // 4), lambda i: (0, 0))),
        scratch_shapes=[
            pltpu.VMEM((rows * capacity, 128), jnp.float32),
            pltpu.VMEM((rows, 128), jnp.float32),
            pltpu.VMEM((rows, 128), jnp.float32),
        ],
    )(flag, where_held, arrived, cold, step_row)


def body(block_pool, sel_index, sel_layer, counts):
    own_count = lax.axis_size("own")
    rep_count = lax.axis_size("rep")
    layers = own_count // SLICES
    n_select = sel_index.shape[0]
    capacity = n_select // 4
    tokens = block_pool.shape[1]
    half = block_pool.shape[2] // SLICES
    period = 4 * half
    denominator = float(own_count * rep_count * capacity * tokens)
    hot, cold, table = open_exchange(block_pool, sel_index, sel_layer, counts, capacity)
    fits, one, two, number, where_held, flag = plan(table, capacity, n_select - capacity)

    def sparse():
        arrived, landed, step_row = lax.switch(
            sel_layer[0], [functools.partial(route, layer) for layer in range(layers)], one, two, number, hot, cold)
        return finish(flag, where_held, arrived, landed, step_row, period)

    def dense():
        parted = part(block_pool, sel_index, sel_layer, counts, layers, capacity)
        arrived = lax.all_to_all(parted, "own", split_axis=0, concat_axis=0, tiled=True)
        top = jnp.max(peaks(arrived, period)[0].reshape(4, half), axis=0)
        step = HEADROOM * jnp.maximum(top, 1.0) / 127.0
        codes, err = encode(arrived, jnp.tile(step, 4)[None, :], period)
        return codes, err, step[None, :]

    codes, err, step = lax.cond(fits[0] == 1, sparse, dense)
    return codes[None, None], step, totals(err, step, denominator)


def solution(mesh):
    return jax.shard_map(
        body,
        mesh=mesh,
        in_specs=(
            P(("own", "rep"), None, None),
            P(("own", "rep")),
            P(("own", "rep")),
            P(("own", "rep")),
        ),
        out_specs=(P("own", "rep", None, None, None), P("own", None), P("own", None)),
        check_vma=False,
    )
```

```python
import functools

import jax
import jax.numpy as jnp
from jax import lax
from jax.experimental import pallas as pl
from jax.experimental.pallas import tpu as pltpu
from jax.sharding import PartitionSpec as P

SLICES = 2
HEADROOM = 0.5
MESH = pl.DeviceIdType.MESH


def part_kernel(layers, capacity, half, idx_ref, lay_ref, cnt_ref, pool_ref, out_ref,
                blocks, wide, stage, zeros, slot_of, in_sem, out_sem, zero_sem):
    n_select = idx_ref.shape[0]
    tokens = blocks.shape[1]
    latent = blocks.shape[2]
    for j in range(n_select):
        pltpu.make_async_copy(pool_ref.at[idx_ref[j]], blocks.at[j], in_sem).start()
    live = cnt_ref[0]

    def clear(i, _):
        slot_of[i] = -1
        return 0

    lax.fori_loop(0, layers * capacity + layers, clear, 0)

    def place(j, _):
        layer = lay_ref[j]

        @pl.when(j < live)
        def _():
            rank = slot_of[layers * capacity + layer] + 1
            slot_of[layers * capacity + layer] = rank
            slot_of[layer * capacity + rank] = j
        return 0

    lax.fori_loop(0, n_select, place, 0)
    zeros[...] = jnp.zeros_like(zeros)
    pltpu.make_async_copy(pool_ref.at[pl.ds(0, n_select)], blocks, in_sem).wait()

    def one_layer(layer, used):
        some = slot_of[layers * capacity + layer] >= 0

        @pl.when(jnp.logical_not(some))
        def _():
            cp = pltpu.make_async_copy(zeros, out_ref.at[pl.ds(layer * SLICES, SLICES)], zero_sem)
            cp.start()
            cp.wait()

        @pl.when(some)
        def _():
            @pl.when(used > 0)
            def _():
                pltpu.make_async_copy(stage.at[0], out_ref.at[pl.ds(0, SLICES)], out_sem).wait()
            for c in range(capacity):
                j = slot_of[layer * capacity + c]

                @pl.when(j >= 0)
                def _():
                    for k in range(wide.shape[0]):
                        cols = min(128, latent - k * 128)
                        wide[k, pl.ds(c * tokens, tokens), :cols] = blocks[j, :, k * 128:k * 128 + cols].astype(jnp.float32)

                @pl.when(j < 0)
                def _():
                    wide[:, pl.ds(c * tokens, tokens), :] = jnp.zeros((wide.shape[0], tokens, 128), jnp.float32)

            def four(q, _):
                rows = [jnp.concatenate([wide[k, pl.ds(4 * q + m, capacity, stride=tokens), :]
                                         for k in range(wide.shape[0])], axis=1) for m in range(4)]
                for h in range(SLICES):
                    flat = jnp.concatenate([r[:, h * half:(h + 1) * half] for r in rows], axis=1)
                    stage[0, h, :, pl.ds(pl.multiple_of(q * 4 * half, 128), 4 * half)] = flat.astype(jnp.bfloat16)
                return 0

            lax.fori_loop(0, tokens // 4, four, 0)
            pltpu.make_async_copy(stage.at[0], out_ref.at[pl.ds(layer * SLICES, SLICES)], out_sem).start()
        return used + some.astype(jnp.int32)

    used = lax.fori_loop(0, layers, one_layer, 0)

    @pl.when(used > 0)
    def _():
        pltpu.make_async_copy(stage.at[0], out_ref.at[pl.ds(0, SLICES)], out_sem).wait()


def part(block_pool, sel_index, sel_layer, counts, layers, capacity):
    rows, tokens, latent = block_pool.shape
    half = latent // SLICES
    n_select = sel_index.shape[0]
    groups = layers * SLICES
    smem = pl.BlockSpec(memory_space=pltpu.SMEM)
    return pl.pallas_call(
        functools.partial(part_kernel, layers, capacity, half),
        out_shape=jax.ShapeDtypeStruct((groups, capacity, tokens * half), jnp.bfloat16),
        in_specs=[smem, smem, smem, pl.BlockSpec(memory_space=pltpu.HBM)],
        out_specs=pl.BlockSpec(memory_space=pltpu.HBM),
        scratch_shapes=[
            pltpu.VMEM((n_select, tokens, latent), jnp.bfloat16),
            pltpu.VMEM((-(-latent // 128), capacity * tokens, 128), jnp.float32),
            pltpu.VMEM((1, SLICES, capacity, tokens * half), jnp.bfloat16),
            pltpu.VMEM((SLICES, capacity, tokens * half), jnp.bfloat16),
            pltpu.SMEM((layers * capacity + layers,), jnp.int32),
            pltpu.SemaphoreType.DMA,
            pltpu.SemaphoreType.DMA,
            pltpu.SemaphoreType.DMA,
        ],
    )(sel_index, sel_layer, counts, block_pool)


def rep_peers():
    me = lax.axis_index("rep")
    count = lax.axis_size("rep")
    return [lax.rem(me + d, count) for d in range(1, count)]


def greet():
    barrier = pltpu.get_barrier_semaphore()
    for peer in rep_peers():
        pl.semaphore_signal(barrier, inc=1, device_id={"rep": peer}, device_id_type=MESH)


def share(mine, theirs, send_sem, recv_sem):
    pl.semaphore_wait(pltpu.get_barrier_semaphore(), len(rep_peers()))
    copies = []
    for i, peer in enumerate(rep_peers()):
        cp = pltpu.make_async_remote_copy(
            src_ref=mine, dst_ref=theirs.at[i], send_sem=send_sem.at[i], recv_sem=recv_sem.at[i],
            device_id={"rep": peer}, device_id_type=MESH)
        cp.start()
        copies.append(cp)
    for cp in copies:
        cp.wait()


def peak_kernel(steps, period, x_ref, out_ref, acc, mine, theirs, send_sem, recv_sem):
    i = pl.program_id(0)

    @pl.when(i == 0)
    def _():
        greet()
        acc[...] = jnp.zeros_like(acc)

    def fold(g, top):
        chunk = x_ref[:, :, pl.ds(pl.multiple_of(g * period, 128), period)].astype(jnp.float32)
        return jnp.maximum(top, jnp.max(jnp.abs(chunk), axis=0))

    acc[...] = lax.fori_loop(0, x_ref.shape[2] // period, fold, acc[...])

    @pl.when(i == steps - 1)
    def _():
        mine[...] = jnp.broadcast_to(jnp.max(acc[...], axis=0, keepdims=True), mine.shape)
        share(mine, theirs, send_sem, recv_sem)
        out_ref[...] = jnp.maximum(jnp.max(theirs[...], axis=0), mine[...])


def peaks(arrived, period, per_step=4):
    sources, capacity, flat = arrived.shape
    steps = sources // per_step
    peers = lax.axis_size("rep") - 1
    return pl.pallas_call(
        functools.partial(peak_kernel, steps, period),
        grid=(steps,),
        out_shape=jax.ShapeDtypeStruct((8, period), jnp.float32),
        in_specs=[pl.BlockSpec((per_step, capacity, flat), lambda i: (i, 0, 0))],
        out_specs=pl.BlockSpec((8, period), lambda i: (0, 0)),
        scratch_shapes=[
            pltpu.VMEM((capacity, period), jnp.float32),
            pltpu.VMEM((8, period), jnp.float32),
            pltpu.VMEM((peers, 8, period), jnp.float32),
            pltpu.SemaphoreType.DMA((peers,)),
            pltpu.SemaphoreType.DMA((peers,)),
        ],
        compiler_params=pltpu.CompilerParams(collective_id=0, has_side_effects=True),
    )(arrived)


def code_kernel(period, x_ref, step_ref, out_ref, err_ref):
    @pl.when(pl.program_id(0) == 0)
    def _():
        err_ref[...] = jnp.zeros_like(err_ref)

    step = jnp.broadcast_to(step_ref[...], err_ref.shape)
    inverse = 1.0 / step

    def fold(g, total):
        at = pl.ds(pl.multiple_of(g * period, 128), period)
        for s in range(x_ref.shape[0]):
            values = x_ref[s, :, at].astype(jnp.float32)
            codes = jnp.clip(values * inverse, -127.0, 127.0).astype(jnp.bfloat16)
            out_ref[s, :, at] = codes
            miss = values - codes.astype(jnp.float32) * step
            total = total + miss * miss
        return total

    err_ref[...] = lax.fori_loop(0, x_ref.shape[2] // period, fold, err_ref[...])


def encode(arrived, step_row, period, per_step=4):
    sources, capacity, flat = arrived.shape
    return pl.pallas_call(
        functools.partial(code_kernel, period),
        grid=(sources // per_step,),
        out_shape=(jax.ShapeDtypeStruct(arrived.shape, jnp.bfloat16),
                   jax.ShapeDtypeStruct((capacity, period), jnp.float32)),
        in_specs=[pl.BlockSpec((per_step, capacity, flat), lambda i: (i, 0, 0)),
                  pl.BlockSpec((1, period), lambda i: (0, 0))],
        out_specs=(pl.BlockSpec((per_step, capacity, flat), lambda i: (i, 0, 0)),
                   pl.BlockSpec((capacity, period), lambda i: (0, 0))),
    )(arrived, step_row)


def total_kernel(denominator, err_ref, step_ref, out_ref, mine, theirs, send_sem, recv_sem):
    greet()
    half = step_ref.shape[1]
    row = jnp.sum(err_ref[...], axis=0, keepdims=True)
    parts = [row[:, m * half:(m + 1) * half] for m in range(4)]
    mine[...] = jnp.broadcast_to((parts[0] + parts[1]) + (parts[2] + parts[3]), mine.shape)
    share(mine, theirs, send_sem, recv_sem)
    total = (jnp.sum(theirs[...], axis=0) + mine[...])[0:1]
    step = step_ref[...]
    out_ref[...] = total / (step * step * denominator)


def totals(err, step, denominator):
    half = step.shape[1]
    peers = lax.axis_size("rep") - 1
    vmem = pl.BlockSpec(memory_space=pltpu.VMEM)
    return pl.pallas_call(
        functools.partial(total_kernel, denominator),
        out_shape=jax.ShapeDtypeStruct((1, half), jnp.float32),
        in_specs=[vmem, vmem],
        out_specs=vmem,
        scratch_shapes=[
            pltpu.VMEM((8, half), jnp.float32),
            pltpu.VMEM((peers, 8, half), jnp.float32),
            pltpu.SemaphoreType.DMA((peers,)),
            pltpu.SemaphoreType.DMA((peers,)),
        ],
        compiler_params=pltpu.CompilerParams(collective_id=1, has_side_effects=True),
    )(err, step)


SIDE = 4
CAP_ONE = 20
CAP_TWO = 16
BY_LAYER, BY_SIDE, LIVE = 32, 48, 56


def open_kernel(half, idx_ref, lay_ref, cnt_ref, pool_ref, hot_ref, cold_ref, table_ref, peaks_ref,
                pool, wide, flat, row_ref, pool_sem, own_send, own_recv, send_sem, recv_sem):
    n_select = idx_ref.shape[0]
    tokens, latent = pool.shape[1], pool.shape[2]
    capacity = hot_ref.shape[1]
    tiles = wide.shape[0]
    fetch = pltpu.make_async_copy(pool_ref, pool, pool_sem)
    fetch.start()
    me, mine = lax.axis_index("own"), lax.axis_index("rep")
    owners = lax.axis_size("own")
    barrier = pltpu.get_barrier_semaphore()

    def hello(i, _):
        pl.semaphore_signal(barrier, inc=1, device_id={"own": lax.rem(me + i, owners)}, device_id_type=MESH)
        return 0

    lax.fori_loop(1, owners, hello, 0)
    greet()

    lane = lax.broadcasted_iota(jnp.int32, (1, 128), 1)
    live = cnt_ref[0]
    row = jnp.where(lane == LIVE, live, jnp.where(lane < BY_LAYER, -1, 0))
    for j in range(n_select):
        layer = lay_ref[j]
        is_live = jnp.where(j < live, 1, 0)
        row = jnp.where(lane == j, jnp.where(j < live, layer, -1), row)
        if j >= capacity:
            spot = ((lane == BY_LAYER + layer) | (lane == BY_SIDE + lax.shift_right_logical(layer, 2))
                    | (lane == BY_SIDE + SIDE + (layer & (SIDE - 1))))
            row = row + jnp.where(spot, is_live, 0)
    row_ref[...] = row
    table_ref[mine, me] = row
    pl.semaphore_wait(barrier, owners - 1 + len(rep_peers()))

    def push(i, _):
        pltpu.make_async_remote_copy(
            src_ref=row_ref, dst_ref=table_ref.at[mine, me], send_sem=own_send, recv_sem=own_recv,
            device_id={"own": lax.rem(me + i, owners)}, device_id_type=MESH).start()
        return 0

    lax.fori_loop(1, owners, push, 0)
    fetch.wait()

    def widen(j, to):
        at = idx_ref[j]
        for k in range(tiles):
            cols = min(128, latent - k * 128)
            wide[k, pl.ds(to, tokens), :cols] = pool[at, :, k * 128:k * 128 + cols].astype(jnp.float32)

    def strided(start, count, stride):
        return jnp.concatenate([wide[k, pl.ds(start, count, stride=stride), :] for k in range(tiles)], axis=1)

    for c in range(capacity):
        widen(c, c * tokens)

    def four(q, top):
        rows = [strided(4 * q + m, capacity, tokens) for m in range(4)]
        for r in rows:
            top = jnp.maximum(top, jnp.abs(r))
        for h in range(SLICES):
            line = jnp.concatenate([r[:, h * half:(h + 1) * half] for r in rows], axis=1)
            hot_ref[h, :, pl.ds(pl.multiple_of(q * 4 * half, 128), 4 * half)] = line.astype(jnp.bfloat16)
        return top

    top = lax.fori_loop(0, tokens // 4, four, jnp.zeros((capacity, tiles * 128), jnp.float32))
    top = jnp.max(top, axis=0, keepdims=True)
    for h in range(SLICES):
        peaks_ref[h] = jnp.broadcast_to(top[:, h * half:(h + 1) * half], peaks_ref.shape[1:])

    rest = table_ref.at[mine, pl.ds(0, owners - 1)]
    pltpu.make_async_copy(rest, rest, own_recv).wait()
    pltpu.make_async_copy(rest, rest, own_send).wait()
    copies = []
    for i, peer in enumerate(rep_peers()):
        cp = pltpu.make_async_remote_copy(
            src_ref=table_ref.at[mine], dst_ref=table_ref.at[mine], send_sem=send_sem.at[i], recv_sem=recv_sem.at[i],
            device_id={"rep": peer}, device_id_type=MESH)
        cp.start()
        copies.append(cp)

    quads = tokens // 4
    lines = 4 * half // 128

    def one(j, _):
        widen(j, 0)
        rows = [strided(m, quads, 4) for m in range(4)]
        for h in range(SLICES):
            line = jnp.concatenate([r[:, h * half:(h + 1) * half] for r in rows], axis=1)
            for i in range(lines):
                flat[h, pl.ds(i, quads, stride=lines), :] = line[:, i * 128:(i + 1) * 128]
        for h in range(SLICES):
            cold_ref[h, j - capacity] = flat[h].astype(jnp.bfloat16)
        return 0

    lax.fori_loop(capacity, n_select, one, 0)
    for cp in copies:
        cp.wait()


def open_exchange(block_pool, sel_index, sel_layer, counts, capacity):
    _, tokens, latent = block_pool.shape
    half = latent // SLICES
    n_select = sel_index.shape[0]
    lines = tokens * half // 128
    owners, reps = lax.axis_size("own"), lax.axis_size("rep")
    smem = pl.BlockSpec(memory_space=pltpu.SMEM)
    vmem = pl.BlockSpec(memory_space=pltpu.VMEM)
    return pl.pallas_call(
        functools.partial(open_kernel, half),
        out_shape=(jax.ShapeDtypeStruct((SLICES, capacity, tokens * half), jnp.bfloat16),
                   jax.ShapeDtypeStruct((SLICES, n_select - capacity, lines, 128), jnp.bfloat16),
                   jax.ShapeDtypeStruct((reps, owners, 1, 128), jnp.int32),
                   jax.ShapeDtypeStruct((SLICES, 8, half), jnp.float32)),
        in_specs=[smem, smem, smem, pl.BlockSpec(memory_space=pltpu.HBM)],
        out_specs=(vmem, vmem, vmem, vmem),
        scratch_shapes=[
            pltpu.VMEM(block_pool.shape, jnp.bfloat16),
            pltpu.VMEM((-(-latent // 128), capacity * tokens, 128), jnp.float32),
            pltpu.VMEM((SLICES, lines, 128), jnp.float32),
            pltpu.VMEM((1, 128), jnp.int32),
            pltpu.SemaphoreType.DMA,
            pltpu.SemaphoreType.DMA,
            pltpu.SemaphoreType.DMA,
            pltpu.SemaphoreType.DMA((reps - 1,)),
            pltpu.SemaphoreType.DMA((reps - 1,)),
        ],
        compiler_params=pltpu.CompilerParams(collective_id=2, has_side_effects=True),
    )(sel_index, sel_layer, counts, block_pool)


def place():
    me = lax.axis_index("own")
    core = lax.rem(me, 2)
    x, z = me // (2 * SIDE), lax.rem(me // 2, SIDE)
    return core, jnp.where(core == 0, x, z), jnp.where(core == 0, z, x)


def index_of(core, a, b, slot):
    return jnp.where(core == 0, a * SIDE + b, b * SIDE + a) * 2 + slot


def chip_peer(core, a, b, slot):
    return {"own": index_of(core, lax.rem(a, SIDE), lax.rem(b, SIDE), slot)}


def plan_kernel(capacity, n_cold, table_ref, rows_ref, fits_ref, one_ref, two_ref, number_ref, where_ref,
                near, rank_one, rank_two, sem):
    core, a, b = place()
    me = lax.axis_index("own")
    cp = pltpu.make_async_copy(rows_ref.at[lax.axis_index("rep")], near, sem)
    cp.start()
    reps, owners = table_ref.shape[0], table_ref.shape[1]
    lane = lax.broadcasted_iota(jnp.int32, (1, 128), 1)
    one, two = jnp.zeros((1, 128), jnp.int32), jnp.zeros((1, 128), jnp.int32)
    for r in range(reps):
        chips = [table_ref[r, 2 * c] + table_ref[r, 2 * c + 1] for c in range(SIDE * SIDE)]
        for c in chips:
            one = jnp.maximum(one, c)
        for i in range(SIDE):
            for picked in (chips[i::SIDE], chips[SIDE * i:SIDE * i + SIDE]):
                two = jnp.maximum(two, (picked[0] + picked[1]) + (picked[2] + picked[3]))
    one = jnp.where((lane >= BY_SIDE) & (lane < LIVE), one, 0).astype(jnp.float32)
    two = jnp.where((lane >= BY_LAYER) & (lane < BY_SIDE), two, 0).astype(jnp.float32)
    fits_ref[0] = jnp.where(jnp.logical_and(jnp.max(one) <= CAP_ONE, jnp.max(two) <= CAP_TWO), 1, 0)

    def clear(ref, value):
        def put(i, _):
            ref[i] = value
            return 0
        lax.fori_loop(0, ref.shape[0], put, 0, unroll=8 if ref.shape[0] % 8 == 0 else 1)

    clear(one_ref, 0)
    clear(two_ref, 0)
    clear(number_ref, 0)
    clear(where_ref, -1)
    clear(rank_two, 0)
    cp.wait()
    layer_here = me // 2

    def column(a_from, _):
        clear(rank_one, 0)
        for slot in range(2):
            device = index_of(core, a_from, b, slot)

            def entry(j, _):
                layer = near[device, 0, j]
                high, low = lax.shift_right_logical(layer, 2), layer & (SIDE - 1)
                to_a = jnp.where(core == 0, high, low)
                to_b = jnp.where(core == 0, low, high)
                first = rank_one[to_a]
                rank_one[to_a] = first + 1
                first = jnp.minimum(first, CAP_ONE - 1)

                @pl.when(a_from == a)
                def _():
                    one_ref[to_a * CAP_ONE + first] = slot * n_cold + j - capacity

                @pl.when(to_a == a)
                def _():
                    second = rank_two[to_b]
                    rank_two[to_b] = second + 1
                    two_ref[to_b * CAP_TWO + jnp.minimum(second, CAP_TWO - 1)] = a_from * CAP_ONE + first
                return 0

            lax.fori_loop(capacity, near[device, 0, LIVE], entry, 0)
        return 0

    lax.fori_loop(0, SIDE, column, 0)

    def arriving(n, _):
        b_from, a_from, slot = n // (2 * SIDE), lax.rem(n // 2, SIDE), lax.rem(n, 2)
        device = index_of(core, a_from, b_from, slot)

        @pl.when(near[device, 0, BY_LAYER + layer_here] > 0)
        def _():
            def entry(j, held):
                hit = near[device, 0, j] == layer_here

                @pl.when(hit)
                def _():
                    count = number_ref[b_from]
                    number_ref[b_from] = count + 1
                    where_ref[device * capacity + held] = b_from * CAP_TWO + count
                return held + jnp.where(hit, 1, 0)

            lax.fori_loop(capacity, near[device, 0, LIVE], entry, 0)
        return 0

    lax.fori_loop(0, owners, arriving, 0)


def plan(table, capacity, n_cold):
    reps, owners = table.shape[0], table.shape[1]
    smem = pl.BlockSpec(memory_space=pltpu.SMEM)
    sizes = (1, SIDE * CAP_ONE, SIDE * CAP_TWO, SIDE, owners * capacity)
    return pl.pallas_call(
        functools.partial(plan_kernel, capacity, n_cold),
        out_shape=tuple(jax.ShapeDtypeStruct((n,), jnp.int32) for n in sizes),
        in_specs=[pl.BlockSpec(memory_space=pltpu.VMEM), pl.BlockSpec(memory_space=pl.ANY)],
        out_specs=tuple(smem for _ in sizes),
        scratch_shapes=[
            pltpu.SMEM((owners, 1, 128), jnp.int32),
            pltpu.SMEM((SIDE,), jnp.int32),
            pltpu.SMEM((SIDE,), jnp.int32),
            pltpu.SemaphoreType.DMA,
        ],
    )(table, table)


def route_kernel(layer, denominator, one_ref, two_ref, number_ref, hot_ref, cold_ref, peaks_ref,
                 final, landed, step_ref, error_ref,
                 held, first, passed, second, tops, wide_step, acc, flat, flat_step, mine, theirs, sums, their_sums,
                 sem_send, sem_block, sems_s, sems_r, local, top_send, top_recv, send_sem, recv_sem, sum_send, sum_recv):
    core, a, b = place()
    me = lax.axis_index("own")
    owners = final.shape[0]
    other = 1 - core
    beside = index_of(core, a, b, other)
    n_cold = cold_ref.shape[1]
    star_x, star_z = layer // SIDE, layer % SIDE
    star_a = jnp.where(core == 0, star_x, star_z)
    star_b = jnp.where(core == 0, star_z, star_x)
    da = lax.rem(a + SIDE - star_a, SIDE)
    db = lax.rem(b + SIDE - star_b, SIDE)
    relay = jnp.logical_and(da == 0, db != 0)
    star = jnp.logical_and(da == 0, db == 0)
    others = jnp.logical_not(star)
    barrier = pltpu.get_barrier_semaphore()
    partner = chip_peer(core, a, b, other)
    pl.semaphore_signal(barrier, inc=1, device_id=partner, device_id_type=MESH)
    for d in range(1, SIDE):
        pl.semaphore_signal(barrier, inc=1, device_id=chip_peer(core, a + d, b, core), device_id_type=MESH)
        pl.semaphore_signal(barrier, inc=1, device_id=chip_peer(core, a, b + d, core), device_id_type=MESH)
    greet()

    @pl.when(star)
    def _():
        def invite(i, _):
            pl.semaphore_signal(barrier, inc=1, device_id={"own": lax.rem(me + i, owners)}, device_id_type=MESH)
            return 0

        lax.fori_loop(1, owners, invite, 0)

    keep_hot = pltpu.make_async_copy(hot_ref.at[core], final.at[me], local.at[0])
    keep_hot.start()
    keep_cold = pltpu.make_async_copy(cold_ref.at[core], held.at[pl.ds(core * n_cold, n_cold)], local.at[1])
    keep_cold.start()
    pl.semaphore_wait(barrier, 2 * SIDE - 1 + len(rep_peers()) + jnp.where(star, 1, 2))

    def send(src, dst, send_at, recv_at, to):
        return pltpu.make_async_remote_copy(
            src_ref=src, dst_ref=dst, send_sem=send_at, recv_sem=recv_at, device_id=to, device_id_type=MESH)

    swap_hot = send(hot_ref.at[other], final.at[me], sem_send.at[0], sem_block.at[me], partner)
    swap_hot.start()
    swap_cold = send(cold_ref.at[other], held.at[pl.ds(core * n_cold, n_cold)], sems_s.at[0], sems_r.at[0], partner)
    swap_cold.start()
    report = [send(peaks_ref.at[h], tops.at[me], top_send.at[h], top_recv, {"own": SLICES * layer + h})
              for h in range(SLICES)]
    for h in range(SLICES):
        @pl.when(me != SLICES * layer + h)
        def _(h=h):
            report[h].start()
    keep_hot.wait()

    dist = jnp.where(da != 0, da, db)

    def onward(slot):
        step = jnp.where(dist == 2, jnp.where(slot == 0, 1, SIDE - 1), SIDE - dist)
        return chip_peer(core, a + jnp.where(da != 0, step, 0), b + jnp.where(da != 0, 0, step), core)

    def forward(s, n, slot):
        send(final.at[s], final.at[s], sem_send.at[n], sem_block.at[s], onward(slot)).start()

    def got(s):
        pltpu.make_async_copy(final.at[s], final.at[s], sem_block.at[s]).wait()

    @pl.when(others)
    def _():
        forward(me, 1, core)
        got(beside)
        forward(beside, 2, other)

    keep_cold.wait()
    swap_cold.wait()

    def pack(src, table, at, dst, start, count):
        def body(k, _):
            dst[start + k] = src[table[at + k]]
            return 0
        lax.fori_loop(0, count, body, 0)

    copies = []
    for d in (2, 1, 3):
        pack(held, one_ref, lax.rem(a + d, SIDE) * CAP_ONE, first, (d - 1) * CAP_ONE, CAP_ONE)
        cp = send(first.at[pl.ds((d - 1) * CAP_ONE, CAP_ONE)], passed.at[pl.ds(a * CAP_ONE, CAP_ONE)],
                  sems_s.at[d], sems_r.at[d], chip_peer(core, a + d, b, core))
        cp.start()
        copies.append(cp)
    pack(held, one_ref, a * CAP_ONE, passed, a * CAP_ONE, CAP_ONE)

    @pl.when(jnp.logical_or(da == 1, da == 3))
    def _():
        slot = jnp.where(da == 1, 1, 0)
        s = index_of(core, lax.rem(star_a + 2, SIDE), b, slot)
        got(s)
        forward(s, 3, slot)

    def of(a_from, b_from, slot):
        return index_of(core, lax.rem(star_a + a_from, SIDE), lax.rem(star_b + b_from, SIDE), slot)

    def row_order(p):
        return jnp.where(p < 2, p, 5 - p)

    def row_blocks(start, stop):
        def row_block(i, _):
            near = i < SIDE
            slot = jnp.where(near, i // 2, i - SIDE)
            s = of(jnp.where(near, 1 + 2 * lax.rem(i, 2), 2), db, slot)
            got(s)
            forward(s, 3 + i, slot)
            return 0

        lax.fori_loop(start, stop, row_block, 0)

    @pl.when(relay)
    def _():
        row_blocks(0, SIDE)

    period = acc.shape[1]
    lines = period // 128
    half = period // 4

    def trade(src, dst, send_at, recv_at):
        cps = []
        for i, peer in enumerate(rep_peers()):
            cp = send(src, dst.at[i], send_at.at[i], recv_at.at[i], {"rep": peer})
            cp.start()
            cps.append(cp)
        for cp in cps:
            cp.wait()

    def settle():
        trade(mine, theirs, send_sem, recv_sem)
        peak = jnp.maximum(jnp.max(theirs[...], axis=0), mine[...])
        step = HEADROOM * jnp.maximum(peak, 1.0) / 127.0
        step_ref[...] = step
        wide_step[...] = jnp.concatenate([step] * 4, axis=1)

    @pl.when(star)
    def _():
        own_top = pltpu.make_async_copy(peaks_ref.at[core], tops.at[me], local.at[0])
        own_top.start()
        own_top.wait()
        rest = tops.at[pl.ds(0, owners - 1)]
        pltpu.make_async_copy(rest, rest, top_recv).wait()
        mine[...] = jnp.max(tops[...], axis=0)
        settle()

    for cp in copies:
        cp.wait()
    copies = []
    for d in (2, 1, 3):
        pack(passed, two_ref, lax.rem(b + d, SIDE) * CAP_TWO, second, (d - 1) * CAP_TWO, CAP_TWO)
        cp = send(second.at[pl.ds((d - 1) * CAP_TWO, CAP_TWO)], landed.at[pl.ds(b * CAP_TWO, CAP_TWO)],
                  sems_s.at[SIDE - 1 + d], sems_r.at[SIDE - 1 + d], chip_peer(core, a, b + d, core))
        cp.start()
        copies.append(cp)
    pack(passed, two_ref, b * CAP_TWO, landed, b * CAP_TWO, CAP_TWO)

    @pl.when(relay)
    def _():
        row_blocks(SIDE, SIDE + 2)

        @pl.when(db != 2)
        def _():
            slot = jnp.where(db == 1, 1, 0)

            def far_block(p, _):
                s = of(row_order(p), 2, slot)
                got(s)
                forward(s, 2 * SIDE + 1 + p, slot)
                return 0

            lax.fori_loop(0, SIDE, far_block, 0)

    @pl.when(star)
    def _():
        acc[...] = jnp.zeros_like(acc)

        def encode_block(s):
            step = wide_step[...]
            inverse = 1.0 / step

            def fold(g, total):
                at = pl.ds(pl.multiple_of(g * period, 128), period)
                values = final[s, :, at].astype(jnp.float32)
                codes = jnp.clip(values * inverse, -127.0, 127.0).astype(jnp.bfloat16)
                final[s, :, at] = codes
                miss = values - codes.astype(jnp.float32) * step
                return total + miss * miss

            acc[...] = lax.fori_loop(0, final.shape[2] // period, fold, acc[...])

        swap_hot.wait_send()

        def arrive(n, _):
            i = n - 2
            step, which = i // 3, lax.rem(i, 3)
            early = i < 18
            row_a = jnp.where(step < 4, 1 + 2 * lax.rem(step, 2), 2)
            row_slot = jnp.where(step < 4, step // 2, step - 4)
            near_step = jnp.where(early, step, 6 + (i - 18) // 2)
            near_b = jnp.where(early, which * 2 - 1, 1 + 2 * lax.rem(i - 18, 2))
            is_row = jnp.logical_and(early, which == 0)
            is_far = i >= 22
            q = near_step - 2
            near_a = jnp.where(near_step < 2, 0, jnp.where(q < SIDE, 1 + 2 * lax.rem(q, 2), 2))
            near_slot = jnp.where(near_step < 2, near_step, jnp.where(q < SIDE, q // 2, q - SIDE))
            far_step = i - 22
            from_a = jnp.where(is_row, row_a, jnp.where(is_far, row_order(far_step // 2), near_a))
            from_b = jnp.where(is_row, 0, jnp.where(is_far, 2, near_b))
            slot = jnp.where(is_row, row_slot, jnp.where(is_far, lax.rem(far_step, 2), near_slot))
            s = jnp.where(n == 0, me, jnp.where(n == 1, beside, of(from_a, from_b, slot)))

            @pl.when(n > 0)
            def _():
                got(s)
            encode_block(s)
            return 0

        lax.fori_loop(0, owners, arrive, 0)
        row = jnp.sum(acc[...], axis=0, keepdims=True)
        parts = [row[:, m * half:(m + 1) * half] for m in range(4)]
        sums[...] = jnp.broadcast_to((parts[0] + parts[1]) + (parts[2] + parts[3]), sums.shape)

    for cp in copies:
        cp.wait()
    quads = flat.shape[0] // lines

    def gathered(op, join):
        row = [op(flat[pl.ds(i, quads, stride=lines), :], axis=0, keepdims=True) for i in range(lines)]
        row = jnp.concatenate(row, axis=1)
        parts = [row[:, m * half:(m + 1) * half] for m in range(4)]
        return join(join(parts[0], parts[1]), join(parts[2], parts[3]))

    @pl.when(others)
    def _():
        flat[...] = jnp.zeros_like(flat)
        for q in range(SIDE):
            def cold_top(k, _):
                block = jnp.abs(landed[q * CAP_TWO + k].astype(jnp.float32))
                flat[...] = jnp.maximum(flat[...], jnp.where(k < number_ref[q], block, 0.0))
                return 0
            lax.fori_loop(0, CAP_TWO, cold_top, 0)
        mine[...] = jnp.broadcast_to(gathered(jnp.max, jnp.maximum), mine.shape)
        settle()
        for i in range(lines):
            flat_step[pl.ds(i, quads, stride=lines), :] = jnp.broadcast_to(
                wide_step[0:1, i * 128:(i + 1) * 128], (quads, 128))
        flat[...] = jnp.zeros_like(flat)
        for q in range(SIDE):
            def cold_code(k, _):
                values = landed[q * CAP_TWO + k].astype(jnp.float32)
                codes = jnp.clip(values / flat_step[...], -127.0, 127.0).astype(jnp.bfloat16)
                landed[q * CAP_TWO + k] = codes
                miss = values - codes.astype(jnp.float32) * flat_step[...]
                flat[...] += jnp.where(k < number_ref[q], miss * miss, 0.0)
                return 0
            lax.fori_loop(0, CAP_TWO, cold_code, 0)
        sums[...] = jnp.broadcast_to(gathered(jnp.sum, jnp.add), sums.shape)
        swap_hot.wait_send()

        def drained(n, _):
            pltpu.make_async_copy(final.at[0], final.at[0], sem_send.at[n]).wait()
            return 0

        sent = jnp.where(da != 0, jnp.where(da == 2, 2, 3), jnp.where(db == 2, 8, 12))
        lax.fori_loop(1, sent + 1, drained, 0)

    for h in range(SLICES):
        @pl.when(me != SLICES * layer + h)
        def _(h=h):
            report[h].wait_send()
    trade(sums, their_sums, sum_send, sum_recv)
    step = step_ref[...]
    error_ref[...] = (jnp.sum(their_sums[...], axis=0) + sums[...]) / (step * step * denominator)


def route(layer, denominator, one, two, number, hot, cold, peaks):
    _, capacity, flat = hot.shape
    owners = lax.axis_size("own")
    peers = lax.axis_size("rep") - 1
    _, n_cold, lines, width = cold.shape
    period = flat // 16
    half = period // 4
    smem = pl.BlockSpec(memory_space=pltpu.SMEM)
    vmem = pl.BlockSpec(memory_space=pltpu.VMEM)
    anywhere = pl.BlockSpec(memory_space=pl.ANY)
    block, small = (capacity, flat), (lines, width)
    stat = (8, half)
    dma = pltpu.SemaphoreType.DMA
    return pl.pallas_call(
        functools.partial(route_kernel, layer, denominator),
        out_shape=(jax.ShapeDtypeStruct((owners, *block), hot.dtype),
                   jax.ShapeDtypeStruct((SIDE * CAP_TWO, *small), cold.dtype),
                   jax.ShapeDtypeStruct(stat, jnp.float32),
                   jax.ShapeDtypeStruct(stat, jnp.float32)),
        in_specs=[smem, smem, smem, anywhere, anywhere, anywhere],
        out_specs=(vmem, vmem, vmem, vmem),
        scratch_shapes=[
            pltpu.VMEM((2 * n_cold, *small), cold.dtype),
            pltpu.VMEM(((SIDE - 1) * CAP_ONE, *small), cold.dtype),
            pltpu.VMEM((SIDE * CAP_ONE, *small), cold.dtype),
            pltpu.VMEM(((SIDE - 1) * CAP_TWO, *small), cold.dtype),
            pltpu.VMEM((owners, *stat), jnp.float32),
            pltpu.VMEM((8, period), jnp.float32),
            pltpu.VMEM((capacity, period), jnp.float32),
            pltpu.VMEM(small, jnp.float32),
            pltpu.VMEM(small, jnp.float32),
            pltpu.VMEM(stat, jnp.float32),
            pltpu.VMEM((peers, *stat), jnp.float32),
            pltpu.VMEM(stat, jnp.float32),
            pltpu.VMEM((peers, *stat), jnp.float32),
            dma((13,)), dma((owners,)), dma((2 * SIDE - 1,)), dma((2 * SIDE - 1,)), dma((2,)),
            dma((SLICES,)), dma, dma((peers,)), dma((peers,)), dma((peers,)), dma((peers,)),
        ],
        compiler_params=pltpu.CompilerParams(collective_id=4 + layer, has_side_effects=True,
                                             vmem_limit_bytes=VMEM_ROUTE),
    )(one, two, number, hot, cold, peaks)


VMEM_ROUTE = 40 * 1024 * 1024
VMEM_FINISH = 20 * 1024 * 1024


def finish_kernel(layer, where_ref, final, landed, step_in, error_in, out_ref, step_ref, error_ref,
                  wide, stage, zeros, stage_sem, sem):
    owners, capacity, width = final.shape
    rows = width // 128
    step_ref[...] = step_in[0:1]
    error_ref[...] = error_in[0:1]
    star = lax.axis_index("own") // SLICES == layer
    batch = 4

    @pl.when(star)
    def _():
        copies = [pltpu.make_async_copy(final.at[pl.ds(i * batch, batch)], out_ref.at[pl.ds(i * batch, batch)], sem.at[i])
                  for i in range(owners // batch)]
        for cp in copies:
            cp.start()
        for cp in copies:
            cp.wait()

    @pl.when(jnp.logical_not(star))
    def _():
        zeros[...] = jnp.zeros_like(zeros)

        def empty(s, _):
            @pl.when(where_ref[s * capacity] < 0)
            def _():
                pltpu.make_async_copy(zeros, out_ref.at[s], sem.at[s]).start()
            return 0

        lax.fori_loop(0, owners, empty, 0)

        def fill(s, used):
            some = where_ref[s * capacity] >= 0
            slot = lax.rem(used, 2)

            @pl.when(some)
            def _():
                wide[...] = jnp.zeros_like(wide)

                def one(c, _):
                    at = where_ref[s * capacity + c]

                    @pl.when(at >= 0)
                    def _():
                        wide[pl.ds(c, rows, stride=capacity), :] = landed[at].astype(jnp.float32)
                    return 0

                lax.fori_loop(0, capacity, one, 0)

                @pl.when(used >= 2)
                def _():
                    pltpu.make_async_copy(stage.at[slot], out_ref.at[s], stage_sem.at[slot]).wait()
                for r in range(rows):
                    stage[slot, :, r * 128:(r + 1) * 128] = wide[r * capacity:(r + 1) * capacity, :].astype(jnp.bfloat16)
                pltpu.make_async_copy(stage.at[slot], out_ref.at[s], stage_sem.at[slot]).start()
            return used + some.astype(jnp.int32)

        used = lax.fori_loop(0, owners, fill, 0)
        for n in range(2):
            @pl.when(used > n)
            def _():
                pltpu.make_async_copy(stage.at[n], out_ref.at[n], stage_sem.at[n]).wait()

        def wait(s, _):
            @pl.when(where_ref[s * capacity] < 0)
            def _():
                pltpu.make_async_copy(zeros, out_ref.at[s], sem.at[s]).wait()
            return 0

        lax.fori_loop(0, owners, wait, 0)


def finish(layer, where_held, final, landed, step, error):
    owners, capacity, width = final.shape
    half = step.shape[1]
    vmem = pl.BlockSpec(memory_space=pltpu.VMEM)
    return pl.pallas_call(
        functools.partial(finish_kernel, layer),
        out_shape=(jax.ShapeDtypeStruct(final.shape, final.dtype),
                   jax.ShapeDtypeStruct((1, half), jnp.float32),
                   jax.ShapeDtypeStruct((1, half), jnp.float32)),
        in_specs=[pl.BlockSpec(memory_space=pltpu.SMEM), vmem, vmem, vmem, vmem],
        out_specs=(pl.BlockSpec(memory_space=pltpu.HBM), vmem, vmem),
        scratch_shapes=[
            pltpu.VMEM((width // 128 * capacity, 128), jnp.float32),
            pltpu.VMEM((2, capacity, width), final.dtype),
            pltpu.VMEM((capacity, width), final.dtype),
            pltpu.SemaphoreType.DMA((2,)),
            pltpu.SemaphoreType.DMA((owners,)),
        ],
        compiler_params=pltpu.CompilerParams(vmem_limit_bytes=VMEM_FINISH),
    )(where_held, final, landed, step, error)


def body(block_pool, sel_index, sel_layer, counts):
    own_count = lax.axis_size("own")
    rep_count = lax.axis_size("rep")
    layers = own_count // SLICES
    n_select = sel_index.shape[0]
    capacity = n_select // 4
    tokens = block_pool.shape[1]
    half = block_pool.shape[2] // SLICES
    period = 4 * half
    denominator = float(own_count * rep_count * capacity * tokens)
    hot, cold, table, tops = open_exchange(block_pool, sel_index, sel_layer, counts, capacity)
    fits, one, two, number, where_held = plan(table, capacity, n_select - capacity)

    def routed(layer):
        return finish(layer, where_held, *route(layer, denominator, one, two, number, hot, cold, tops))

    def sparse():
        return lax.switch(sel_layer[0], [functools.partial(routed, layer) for layer in range(layers)])

    def dense():
        parted = part(block_pool, sel_index, sel_layer, counts, layers, capacity)
        arrived = lax.all_to_all(parted, "own", split_axis=0, concat_axis=0, tiled=True)
        top = jnp.max(peaks(arrived, period)[0].reshape(4, half), axis=0)
        step = HEADROOM * jnp.maximum(top, 1.0) / 127.0
        codes, err = encode(arrived, jnp.tile(step, 4)[None, :], period)
        return codes, step[None, :], totals(err, step[None, :], denominator)

    codes, step, error = lax.cond(fits[0] == 1, sparse, dense)
    return codes[None, None], step, error


def solution(mesh):
    return jax.shard_map(
        body,
        mesh=mesh,
        in_specs=(
            P(("own", "rep"), None, None),
            P(("own", "rep")),
            P(("own", "rep")),
            P(("own", "rep")),
        ),
        out_specs=(P("own", "rep", None, None, None), P("own", None), P("own", None)),
        check_vma=False,
    )
```

```python
import functools

import jax
import jax.numpy as jnp
from jax import lax
from jax.experimental import pallas as pl
from jax.experimental.pallas import tpu as pltpu
from jax.sharding import PartitionSpec as P

SLICES = 2
HEADROOM = 0.5
MESH = pl.DeviceIdType.MESH


def part_kernel(layers, capacity, half, idx_ref, lay_ref, cnt_ref, pool_ref, out_ref,
                blocks, wide, stage, zeros, slot_of, in_sem, out_sem, zero_sem):
    n_select = idx_ref.shape[0]
    tokens = blocks.shape[1]
    latent = blocks.shape[2]
    for j in range(n_select):
        pltpu.make_async_copy(pool_ref.at[idx_ref[j]], blocks.at[j], in_sem).start()
    live = cnt_ref[0]

    def clear(i, _):
        slot_of[i] = -1
        return 0

    lax.fori_loop(0, layers * capacity + layers, clear, 0)

    def place(j, _):
        layer = lay_ref[j]

        @pl.when(j < live)
        def _():
            rank = slot_of[layers * capacity + layer] + 1
            slot_of[layers * capacity + layer] = rank
            slot_of[layer * capacity + rank] = j
        return 0

    lax.fori_loop(0, n_select, place, 0)
    zeros[...] = jnp.zeros_like(zeros)
    pltpu.make_async_copy(pool_ref.at[pl.ds(0, n_select)], blocks, in_sem).wait()

    def one_layer(layer, used):
        some = slot_of[layers * capacity + layer] >= 0

        @pl.when(jnp.logical_not(some))
        def _():
            cp = pltpu.make_async_copy(zeros, out_ref.at[pl.ds(layer * SLICES, SLICES)], zero_sem)
            cp.start()
            cp.wait()

        @pl.when(some)
        def _():
            @pl.when(used > 0)
            def _():
                pltpu.make_async_copy(stage.at[0], out_ref.at[pl.ds(0, SLICES)], out_sem).wait()
            for c in range(capacity):
                j = slot_of[layer * capacity + c]

                @pl.when(j >= 0)
                def _():
                    for k in range(wide.shape[0]):
                        cols = min(128, latent - k * 128)
                        wide[k, pl.ds(c * tokens, tokens), :cols] = blocks[j, :, k * 128:k * 128 + cols].astype(jnp.float32)

                @pl.when(j < 0)
                def _():
                    wide[:, pl.ds(c * tokens, tokens), :] = jnp.zeros((wide.shape[0], tokens, 128), jnp.float32)

            def four(q, _):
                rows = [jnp.concatenate([wide[k, pl.ds(4 * q + m, capacity, stride=tokens), :]
                                         for k in range(wide.shape[0])], axis=1) for m in range(4)]
                for h in range(SLICES):
                    flat = jnp.concatenate([r[:, h * half:(h + 1) * half] for r in rows], axis=1)
                    stage[0, h, :, pl.ds(pl.multiple_of(q * 4 * half, 128), 4 * half)] = flat.astype(jnp.bfloat16)
                return 0

            lax.fori_loop(0, tokens // 4, four, 0)
            pltpu.make_async_copy(stage.at[0], out_ref.at[pl.ds(layer * SLICES, SLICES)], out_sem).start()
        return used + some.astype(jnp.int32)

    used = lax.fori_loop(0, layers, one_layer, 0)

    @pl.when(used > 0)
    def _():
        pltpu.make_async_copy(stage.at[0], out_ref.at[pl.ds(0, SLICES)], out_sem).wait()


def part(block_pool, sel_index, sel_layer, counts, layers, capacity):
    rows, tokens, latent = block_pool.shape
    half = latent // SLICES
    n_select = sel_index.shape[0]
    groups = layers * SLICES
    smem = pl.BlockSpec(memory_space=pltpu.SMEM)
    return pl.pallas_call(
        functools.partial(part_kernel, layers, capacity, half),
        out_shape=jax.ShapeDtypeStruct((groups, capacity, tokens * half), jnp.bfloat16),
        in_specs=[smem, smem, smem, pl.BlockSpec(memory_space=pltpu.HBM)],
        out_specs=pl.BlockSpec(memory_space=pltpu.HBM),
        scratch_shapes=[
            pltpu.VMEM((n_select, tokens, latent), jnp.bfloat16),
            pltpu.VMEM((-(-latent // 128), capacity * tokens, 128), jnp.float32),
            pltpu.VMEM((1, SLICES, capacity, tokens * half), jnp.bfloat16),
            pltpu.VMEM((SLICES, capacity, tokens * half), jnp.bfloat16),
            pltpu.SMEM((layers * capacity + layers,), jnp.int32),
            pltpu.SemaphoreType.DMA,
            pltpu.SemaphoreType.DMA,
            pltpu.SemaphoreType.DMA,
        ],
    )(sel_index, sel_layer, counts, block_pool)


def rep_peers():
    me = lax.axis_index("rep")
    count = lax.axis_size("rep")
    return [lax.rem(me + d, count) for d in range(1, count)]


def greet():
    barrier = pltpu.get_barrier_semaphore()
    for peer in rep_peers():
        pl.semaphore_signal(barrier, inc=1, device_id={"rep": peer}, device_id_type=MESH)


def share(mine, theirs, send_sem, recv_sem):
    pl.semaphore_wait(pltpu.get_barrier_semaphore(), len(rep_peers()))
    copies = []
    for i, peer in enumerate(rep_peers()):
        cp = pltpu.make_async_remote_copy(
            src_ref=mine, dst_ref=theirs.at[i], send_sem=send_sem.at[i], recv_sem=recv_sem.at[i],
            device_id={"rep": peer}, device_id_type=MESH)
        cp.start()
        copies.append(cp)
    for cp in copies:
        cp.wait()


def peak_kernel(steps, period, x_ref, out_ref, acc, mine, theirs, send_sem, recv_sem):
    i = pl.program_id(0)

    @pl.when(i == 0)
    def _():
        greet()
        acc[...] = jnp.zeros_like(acc)

    def fold(g, top):
        chunk = x_ref[:, :, pl.ds(pl.multiple_of(g * period, 128), period)].astype(jnp.float32)
        return jnp.maximum(top, jnp.max(jnp.abs(chunk), axis=0))

    acc[...] = lax.fori_loop(0, x_ref.shape[2] // period, fold, acc[...])

    @pl.when(i == steps - 1)
    def _():
        mine[...] = jnp.broadcast_to(jnp.max(acc[...], axis=0, keepdims=True), mine.shape)
        share(mine, theirs, send_sem, recv_sem)
        out_ref[...] = jnp.maximum(jnp.max(theirs[...], axis=0), mine[...])


def peaks(arrived, period, per_step=4):
    sources, capacity, flat = arrived.shape
    steps = sources // per_step
    peers = lax.axis_size("rep") - 1
    return pl.pallas_call(
        functools.partial(peak_kernel, steps, period),
        grid=(steps,),
        out_shape=jax.ShapeDtypeStruct((8, period), jnp.float32),
        in_specs=[pl.BlockSpec((per_step, capacity, flat), lambda i: (i, 0, 0))],
        out_specs=pl.BlockSpec((8, period), lambda i: (0, 0)),
        scratch_shapes=[
            pltpu.VMEM((capacity, period), jnp.float32),
            pltpu.VMEM((8, period), jnp.float32),
            pltpu.VMEM((peers, 8, period), jnp.float32),
            pltpu.SemaphoreType.DMA((peers,)),
            pltpu.SemaphoreType.DMA((peers,)),
        ],
        compiler_params=pltpu.CompilerParams(collective_id=0, has_side_effects=True),
    )(arrived)


def code_kernel(period, x_ref, step_ref, out_ref, err_ref):
    @pl.when(pl.program_id(0) == 0)
    def _():
        err_ref[...] = jnp.zeros_like(err_ref)

    step = jnp.broadcast_to(step_ref[...], err_ref.shape)
    inverse = 1.0 / step

    def fold(g, total):
        at = pl.ds(pl.multiple_of(g * period, 128), period)
        for s in range(x_ref.shape[0]):
            values = x_ref[s, :, at].astype(jnp.float32)
            codes = jnp.clip(values * inverse, -127.0, 127.0).astype(jnp.bfloat16)
            out_ref[s, :, at] = codes
            miss = values - codes.astype(jnp.float32) * step
            total = total + miss * miss
        return total

    err_ref[...] = lax.fori_loop(0, x_ref.shape[2] // period, fold, err_ref[...])


def encode(arrived, step_row, period, per_step=4):
    sources, capacity, flat = arrived.shape
    return pl.pallas_call(
        functools.partial(code_kernel, period),
        grid=(sources // per_step,),
        out_shape=(jax.ShapeDtypeStruct(arrived.shape, jnp.bfloat16),
                   jax.ShapeDtypeStruct((capacity, period), jnp.float32)),
        in_specs=[pl.BlockSpec((per_step, capacity, flat), lambda i: (i, 0, 0)),
                  pl.BlockSpec((1, period), lambda i: (0, 0))],
        out_specs=(pl.BlockSpec((per_step, capacity, flat), lambda i: (i, 0, 0)),
                   pl.BlockSpec((capacity, period), lambda i: (0, 0))),
    )(arrived, step_row)


def total_kernel(denominator, err_ref, step_ref, out_ref, mine, theirs, send_sem, recv_sem):
    greet()
    half = step_ref.shape[1]
    row = jnp.sum(err_ref[...], axis=0, keepdims=True)
    parts = [row[:, m * half:(m + 1) * half] for m in range(4)]
    mine[...] = jnp.broadcast_to((parts[0] + parts[1]) + (parts[2] + parts[3]), mine.shape)
    share(mine, theirs, send_sem, recv_sem)
    total = (jnp.sum(theirs[...], axis=0) + mine[...])[0:1]
    step = step_ref[...]
    out_ref[...] = total / (step * step * denominator)


def totals(err, step, denominator):
    half = step.shape[1]
    peers = lax.axis_size("rep") - 1
    vmem = pl.BlockSpec(memory_space=pltpu.VMEM)
    return pl.pallas_call(
        functools.partial(total_kernel, denominator),
        out_shape=jax.ShapeDtypeStruct((1, half), jnp.float32),
        in_specs=[vmem, vmem],
        out_specs=vmem,
        scratch_shapes=[
            pltpu.VMEM((8, half), jnp.float32),
            pltpu.VMEM((peers, 8, half), jnp.float32),
            pltpu.SemaphoreType.DMA((peers,)),
            pltpu.SemaphoreType.DMA((peers,)),
        ],
        compiler_params=pltpu.CompilerParams(collective_id=1, has_side_effects=True),
    )(err, step)


SIDE = 4
CAP_ONE = 24
CAP_TWO = 20
CAP_SIDE = 8
BY_LAYER, BY_SIDE, LIVE = 32, 48, 56


def open_kernel(half, idx_ref, lay_ref, cnt_ref, pool_ref, hot_ref, cold_ref, table_ref, peaks_ref,
                pool, wide, flat, row_ref, pool_sem, own_send, own_recv, send_sem, recv_sem):
    n_select = idx_ref.shape[0]
    tokens, latent = pool.shape[1], pool.shape[2]
    capacity = hot_ref.shape[1]
    tiles = wide.shape[0]
    fetch = pltpu.make_async_copy(pool_ref, pool, pool_sem)
    fetch.start()
    me, mine = lax.axis_index("own"), lax.axis_index("rep")
    owners = lax.axis_size("own")
    barrier = pltpu.get_barrier_semaphore()

    def hello(i, _):
        pl.semaphore_signal(barrier, inc=1, device_id={"own": lax.rem(me + i, owners)}, device_id_type=MESH)
        return 0

    lax.fori_loop(1, owners, hello, 0)
    greet()

    lane = lax.broadcasted_iota(jnp.int32, (1, 128), 1)
    live = cnt_ref[0]
    row = jnp.where(lane == LIVE, live, jnp.where(lane < BY_LAYER, -1, 0))
    for j in range(n_select):
        layer = lay_ref[j]
        is_live = jnp.where(j < live, 1, 0)
        row = jnp.where(lane == j, jnp.where(j < live, layer, -1), row)
        if j >= capacity:
            spot = ((lane == BY_LAYER + layer) | (lane == BY_SIDE + lax.shift_right_logical(layer, 2))
                    | (lane == BY_SIDE + SIDE + (layer & (SIDE - 1))))
            row = row + jnp.where(spot, is_live, 0)
    row_ref[...] = row
    table_ref[mine, me] = row
    pl.semaphore_wait(barrier, owners - 1 + len(rep_peers()))

    def push(i, _):
        pltpu.make_async_remote_copy(
            src_ref=row_ref, dst_ref=table_ref.at[mine, me], send_sem=own_send, recv_sem=own_recv,
            device_id={"own": lax.rem(me + i, owners)}, device_id_type=MESH).start()
        return 0

    lax.fori_loop(1, owners, push, 0)
    fetch.wait()

    def widen(j, to):
        at = idx_ref[j]
        for k in range(tiles):
            cols = min(128, latent - k * 128)
            wide[k, pl.ds(to, tokens), :cols] = pool[at, :, k * 128:k * 128 + cols].astype(jnp.float32)

    def strided(start, count, stride):
        return jnp.concatenate([wide[k, pl.ds(start, count, stride=stride), :] for k in range(tiles)], axis=1)

    for c in range(capacity):
        widen(c, c * tokens)

    def four(q, top):
        rows = [strided(4 * q + m, capacity, tokens) for m in range(4)]
        for r in rows:
            top = jnp.maximum(top, jnp.abs(r))
        for h in range(SLICES):
            line = jnp.concatenate([r[:, h * half:(h + 1) * half] for r in rows], axis=1)
            hot_ref[h, :, pl.ds(pl.multiple_of(q * 4 * half, 128), 4 * half)] = line.astype(jnp.bfloat16)
        return top

    top = lax.fori_loop(0, tokens // 4, four, jnp.zeros((capacity, tiles * 128), jnp.float32))
    top = jnp.max(top, axis=0, keepdims=True)
    for h in range(SLICES):
        peaks_ref[h] = jnp.broadcast_to(top[:, h * half:(h + 1) * half], peaks_ref.shape[1:])

    rest = table_ref.at[mine, pl.ds(0, owners - 1)]
    pltpu.make_async_copy(rest, rest, own_recv).wait()
    pltpu.make_async_copy(rest, rest, own_send).wait()
    copies = []
    for i, peer in enumerate(rep_peers()):
        cp = pltpu.make_async_remote_copy(
            src_ref=table_ref.at[mine], dst_ref=table_ref.at[mine], send_sem=send_sem.at[i], recv_sem=recv_sem.at[i],
            device_id={"rep": peer}, device_id_type=MESH)
        cp.start()
        copies.append(cp)

    quads = tokens // 4
    lines = 4 * half // 128

    def one(j, _):
        widen(j, 0)
        rows = [strided(m, quads, 4) for m in range(4)]
        for h in range(SLICES):
            line = jnp.concatenate([r[:, h * half:(h + 1) * half] for r in rows], axis=1)
            for i in range(lines):
                flat[h, pl.ds(i, quads, stride=lines), :] = line[:, i * 128:(i + 1) * 128]
        for h in range(SLICES):
            cold_ref[h, j - capacity] = flat[h].astype(jnp.bfloat16)
        return 0

    lax.fori_loop(capacity, n_select, one, 0)
    for cp in copies:
        cp.wait()


def open_exchange(block_pool, sel_index, sel_layer, counts, capacity):
    _, tokens, latent = block_pool.shape
    half = latent // SLICES
    n_select = sel_index.shape[0]
    lines = tokens * half // 128
    owners, reps = lax.axis_size("own"), lax.axis_size("rep")
    smem = pl.BlockSpec(memory_space=pltpu.SMEM)
    vmem = pl.BlockSpec(memory_space=pltpu.VMEM)
    return pl.pallas_call(
        functools.partial(open_kernel, half),
        out_shape=(jax.ShapeDtypeStruct((SLICES, capacity, tokens * half), jnp.bfloat16),
                   jax.ShapeDtypeStruct((SLICES, n_select - capacity, lines, 128), jnp.bfloat16),
                   jax.ShapeDtypeStruct((reps, owners, 1, 128), jnp.int32),
                   jax.ShapeDtypeStruct((SLICES, 8, half), jnp.float32)),
        in_specs=[smem, smem, smem, pl.BlockSpec(memory_space=pltpu.HBM)],
        out_specs=(vmem, vmem, vmem, vmem),
        scratch_shapes=[
            pltpu.VMEM(block_pool.shape, jnp.bfloat16),
            pltpu.VMEM((-(-latent // 128), capacity * tokens, 128), jnp.float32),
            pltpu.VMEM((SLICES, lines, 128), jnp.float32),
            pltpu.VMEM((1, 128), jnp.int32),
            pltpu.SemaphoreType.DMA,
            pltpu.SemaphoreType.DMA,
            pltpu.SemaphoreType.DMA,
            pltpu.SemaphoreType.DMA((reps - 1,)),
            pltpu.SemaphoreType.DMA((reps - 1,)),
        ],
        compiler_params=pltpu.CompilerParams(collective_id=2, has_side_effects=True),
    )(sel_index, sel_layer, counts, block_pool)


def place():
    me = lax.axis_index("own")
    core = lax.rem(me, 2)
    x, z = me // (2 * SIDE), lax.rem(me // 2, SIDE)
    return core, jnp.where(core == 0, x, z), jnp.where(core == 0, z, x)


def index_of(core, a, b, slot):
    return jnp.where(core == 0, a * SIDE + b, b * SIDE + a) * 2 + slot


def chip_peer(core, a, b, slot):
    return {"own": index_of(core, lax.rem(a, SIDE), lax.rem(b, SIDE), slot)}


def plan_kernel(capacity, n_cold, lay_ref, table_ref, rows_ref, fits_ref, one_ref, two_ref, side_ref, number_ref, where_ref,
                near, rank_one, rank_two, rank_side, sem):
    core, a, b = place()
    me = lax.axis_index("own")
    cp = pltpu.make_async_copy(rows_ref.at[lax.axis_index("rep")], near, sem)
    cp.start()
    reps, owners = table_ref.shape[0], table_ref.shape[1]
    lane = lax.broadcasted_iota(jnp.int32, (1, 128), 1)
    one, two, side = (jnp.zeros((1, 128), jnp.int32) for _ in range(3))
    star_x, star_z = lax.shift_right_logical(lay_ref[0], 2), lay_ref[0] & (SIDE - 1)
    star_a, star_b = jnp.where(core == 0, star_x, star_z), jnp.where(core == 0, star_z, star_x)
    named = (lane >= BY_LAYER) & (lane < BY_SIDE)
    in_column = jnp.where(named & (lax.shift_right_logical(lane - BY_LAYER, 2) == star_x), 1, 0)
    in_row = jnp.where(named & (((lane - BY_LAYER) & (SIDE - 1)) == star_z), 1, 0)
    for r in range(reps):
        chips = [table_ref[r, 2 * c] + table_ref[r, 2 * c + 1] for c in range(SIDE * SIDE)]
        for c in chips:
            one = jnp.maximum(one, c)
        for i, c in enumerate(chips):
            x, z = i // SIDE, i % SIDE
            turns_x = jnp.where(jnp.logical_and(star_z == z, star_x != x), 1, 0)
            turns_z = jnp.where(jnp.logical_and(star_x == x, star_z != z), 1, 0)
            side = jnp.maximum(side, c * (in_column * turns_x + in_row * turns_z))
        for i in range(SIDE):
            for picked in (chips[i::SIDE], chips[SIDE * i:SIDE * i + SIDE]):
                two = jnp.maximum(two, (picked[0] + picked[1]) + (picked[2] + picked[3]))
    side = side.astype(jnp.float32)
    one = jnp.where((lane >= BY_SIDE) & (lane < LIVE), one, 0).astype(jnp.float32)
    two = jnp.where(named, two, 0).astype(jnp.float32)
    fits = jnp.logical_and(jnp.max(one) <= CAP_ONE, jnp.max(two) <= CAP_TWO)
    fits_ref[0] = jnp.where(jnp.logical_and(fits, jnp.max(side) <= CAP_SIDE), 1, 0)

    def clear(ref, value):
        def put(i, _):
            ref[i] = value
            return 0
        lax.fori_loop(0, ref.shape[0], put, 0, unroll=8 if ref.shape[0] % 8 == 0 else 1)

    clear(one_ref, 0)
    clear(two_ref, 0)
    clear(side_ref, 0)
    clear(number_ref, 0)
    clear(where_ref, -1)
    clear(rank_two, 0)
    clear(rank_side, 0)
    cp.wait()
    layer_here = me // 2

    def column(a_from, _):
        clear(rank_one, 0)
        turn = jnp.logical_and(b == star_b, a_from != star_a)
        for slot in range(2):
            device = index_of(core, a_from, b, slot)

            def entry(j, _):
                layer = near[device, 0, j]
                high, low = lax.shift_right_logical(layer, 2), layer & (SIDE - 1)
                to_a = jnp.where(core == 0, high, low)
                to_b = jnp.where(core == 0, low, high)
                aside = jnp.logical_and(turn, to_a == star_a)

                @pl.when(jnp.logical_and(aside, a_from == a))
                def _():
                    rank = rank_side[to_b]
                    rank_side[to_b] = rank + 1
                    side_ref[to_b * CAP_SIDE + jnp.minimum(rank, CAP_SIDE - 1)] = slot * n_cold + j - capacity

                @pl.when(jnp.logical_not(aside))
                def _():
                    first = rank_one[to_a]
                    rank_one[to_a] = first + 1
                    first = jnp.minimum(first, CAP_ONE - 1)

                    @pl.when(a_from == a)
                    def _():
                        one_ref[to_a * CAP_ONE + first] = slot * n_cold + j - capacity

                    @pl.when(to_a == a)
                    def _():
                        second = rank_two[to_b]
                        rank_two[to_b] = second + 1
                        two_ref[to_b * CAP_TWO + jnp.minimum(second, CAP_TWO - 1)] = a_from * CAP_ONE + first
                return 0

            lax.fori_loop(capacity, near[device, 0, LIVE], entry, 0)
        return 0

    lax.fori_loop(0, SIDE, column, 0)

    def arriving(n, _):
        b_from, a_from, slot = n // (2 * SIDE), lax.rem(n // 2, SIDE), lax.rem(n, 2)
        device = index_of(core, a_from, b_from, slot)
        aside = jnp.logical_and(jnp.logical_and(b_from == star_b, a == star_a), a_from != star_a)
        d = lax.rem(a + SIDE - a_from, SIDE) - 1
        bank = jnp.where(aside, SIDE + d, b_from)
        base = jnp.where(aside, SIDE * CAP_TWO + d * CAP_SIDE, b_from * CAP_TWO)

        @pl.when(near[device, 0, BY_LAYER + layer_here] > 0)
        def _():
            def entry(j, held):
                hit = near[device, 0, j] == layer_here

                @pl.when(hit)
                def _():
                    count = number_ref[bank]
                    number_ref[bank] = count + 1
                    where_ref[device * capacity + held] = base + count
                return held + jnp.where(hit, 1, 0)

            lax.fori_loop(capacity, near[device, 0, LIVE], entry, 0)
        return 0

    lax.fori_loop(0, owners, arriving, 0)


def plan(sel_layer, table, capacity, n_cold):
    reps, owners = table.shape[0], table.shape[1]
    smem = pl.BlockSpec(memory_space=pltpu.SMEM)
    sizes = (1, SIDE * CAP_ONE, SIDE * CAP_TWO, SIDE * CAP_SIDE, 2 * SIDE, owners * capacity)
    return pl.pallas_call(
        functools.partial(plan_kernel, capacity, n_cold),
        out_shape=tuple(jax.ShapeDtypeStruct((n,), jnp.int32) for n in sizes),
        in_specs=[smem, pl.BlockSpec(memory_space=pltpu.VMEM), pl.BlockSpec(memory_space=pl.ANY)],
        out_specs=tuple(smem for _ in sizes),
        scratch_shapes=[
            pltpu.SMEM((owners, 1, 128), jnp.int32),
            pltpu.SMEM((SIDE,), jnp.int32),
            pltpu.SMEM((SIDE,), jnp.int32),
            pltpu.SMEM((SIDE,), jnp.int32),
            pltpu.SemaphoreType.DMA,
        ],
    )(sel_layer, table, table)


def route_kernel(layer, denominator, one_ref, two_ref, side_ref, number_ref, hot_ref, cold_ref, peaks_ref,
                 final, landed, step_ref, error_ref,
                 held, first, passed, second, turned, turning, tops, wide_step, acc, flat, flat_step, mine, theirs, sums, their_sums,
                 sem_send, sem_block, sems_s, sems_r, side_s, side_r, side_f, local, top_send, top_recv, send_sem, recv_sem, sum_send, sum_recv):
    core, a, b = place()
    me = lax.axis_index("own")
    owners = final.shape[0]
    other = 1 - core
    beside = index_of(core, a, b, other)
    n_cold = cold_ref.shape[1]
    star_x, star_z = layer // SIDE, layer % SIDE
    star_a = jnp.where(core == 0, star_x, star_z)
    star_b = jnp.where(core == 0, star_z, star_x)
    da = lax.rem(a + SIDE - star_a, SIDE)
    db = lax.rem(b + SIDE - star_b, SIDE)
    relay = jnp.logical_and(da == 0, db != 0)
    star = jnp.logical_and(da == 0, db == 0)
    others = jnp.logical_not(star)
    beside_star = jnp.logical_and(da != 0, db == 0)
    corner = jnp.logical_and(da != 0, db != 0)
    barrier = pltpu.get_barrier_semaphore()
    partner = chip_peer(core, a, b, other)
    pl.semaphore_signal(barrier, inc=1, device_id=partner, device_id_type=MESH)
    for d in range(1, SIDE):
        pl.semaphore_signal(barrier, inc=1, device_id=chip_peer(core, a + d, b, core), device_id_type=MESH)
        pl.semaphore_signal(barrier, inc=1, device_id=chip_peer(core, a, b + d, core), device_id_type=MESH)
    greet()

    @pl.when(star)
    def _():
        def invite(i, _):
            pl.semaphore_signal(barrier, inc=1, device_id={"own": lax.rem(me + i, owners)}, device_id_type=MESH)
            return 0

        lax.fori_loop(1, owners, invite, 0)

    keep_hot = pltpu.make_async_copy(hot_ref.at[core], final.at[me], local.at[0])
    keep_hot.start()
    keep_cold = pltpu.make_async_copy(cold_ref.at[core], held.at[pl.ds(core * n_cold, n_cold)], local.at[1])
    keep_cold.start()
    pl.semaphore_wait(barrier, 2 * SIDE - 1 + len(rep_peers()) + jnp.where(star, 1, 2))

    def send(src, dst, send_at, recv_at, to):
        return pltpu.make_async_remote_copy(
            src_ref=src, dst_ref=dst, send_sem=send_at, recv_sem=recv_at, device_id=to, device_id_type=MESH)

    swap_hot = send(hot_ref.at[other], final.at[me], sem_send.at[0], sem_block.at[me], partner)
    swap_hot.start()
    swap_cold = send(cold_ref.at[other], held.at[pl.ds(core * n_cold, n_cold)], sems_s.at[0], sems_r.at[0], partner)
    swap_cold.start()
    report = [send(peaks_ref.at[h], tops.at[me], top_send.at[h], top_recv, {"own": SLICES * layer + h})
              for h in range(SLICES)]
    for h in range(SLICES):
        @pl.when(me != SLICES * layer + h)
        def _(h=h):
            report[h].start()
    keep_hot.wait()

    dist = jnp.where(da != 0, da, db)

    def onward(slot):
        step = jnp.where(dist == 2, jnp.where(slot == 0, 1, SIDE - 1), SIDE - dist)
        return chip_peer(core, a + jnp.where(da != 0, step, 0), b + jnp.where(da != 0, 0, step), core)

    def forward(s, n, slot):
        send(final.at[s], final.at[s], sem_send.at[n], sem_block.at[s], onward(slot)).start()

    def got(s):
        pltpu.make_async_copy(final.at[s], final.at[s], sem_block.at[s]).wait()

    @pl.when(others)
    def _():
        forward(me, 1, core)
        got(beside)
        forward(beside, 2, other)

    keep_cold.wait()
    swap_cold.wait()

    def pack(src, table, at, dst, start, count):
        def body(k, _):
            dst[start + k] = src[table[at + k]]
            return 0
        lax.fori_loop(0, count, body, 0)

    copies = []
    for d in (2, 1, 3):
        pack(held, one_ref, lax.rem(a + d, SIDE) * CAP_ONE, first, (d - 1) * CAP_ONE, CAP_ONE)
        cp = send(first.at[pl.ds((d - 1) * CAP_ONE, CAP_ONE)], passed.at[pl.ds(a * CAP_ONE, CAP_ONE)],
                  sems_s.at[d], sems_r.at[d], chip_peer(core, a + d, b, core))
        go = jnp.logical_not(jnp.logical_and(db == 0, da + d == SIDE))
        pl.when(go)(cp.start)
        copies.append((go, cp))

    for d in range(1, SIDE):
        @pl.when(beside_star)
        def _(d=d):
            at = (d - 1) * CAP_SIDE
            pack(held, side_ref, lax.rem(b + d, SIDE) * CAP_SIDE, turned, at, CAP_SIDE)
            send(turned.at[pl.ds(at, CAP_SIDE)], turning, side_s.at[d - 1], side_r, chip_peer(core, a, b + d, core)).start()
    pack(held, one_ref, a * CAP_ONE, passed, a * CAP_ONE, CAP_ONE)

    @pl.when(jnp.logical_or(da == 1, da == 3))
    def _():
        slot = jnp.where(da == 1, 1, 0)
        s = index_of(core, lax.rem(star_a + 2, SIDE), b, slot)
        got(s)
        forward(s, 3, slot)

    def of(a_from, b_from, slot):
        return index_of(core, lax.rem(star_a + a_from, SIDE), lax.rem(star_b + b_from, SIDE), slot)

    def row_order(p):
        return jnp.where(p < 2, p, 5 - p)

    def row_blocks(start, stop):
        def row_block(i, _):
            near = i < SIDE
            slot = jnp.where(near, i // 2, i - SIDE)
            s = of(jnp.where(near, 1 + 2 * lax.rem(i, 2), 2), db, slot)
            got(s)
            forward(s, 3 + i, slot)
            return 0

        lax.fori_loop(start, stop, row_block, 0)

    @pl.when(relay)
    def _():
        row_blocks(0, SIDE)

    period = acc.shape[1]
    lines = period // 128
    half = period // 4

    def trade(src, dst, send_at, recv_at):
        cps = []
        for i, peer in enumerate(rep_peers()):
            cp = send(src, dst.at[i], send_at.at[i], recv_at.at[i], {"rep": peer})
            cp.start()
            cps.append(cp)
        for cp in cps:
            cp.wait()

    def settle():
        trade(mine, theirs, send_sem, recv_sem)
        peak = jnp.maximum(jnp.max(theirs[...], axis=0), mine[...])
        step = HEADROOM * jnp.maximum(peak, 1.0) / 127.0
        step_ref[...] = step
        wide_step[...] = jnp.concatenate([step] * 4, axis=1)

    @pl.when(star)
    def _():
        own_top = pltpu.make_async_copy(peaks_ref.at[core], tops.at[me], local.at[0])
        own_top.start()
        own_top.wait()
        rest = tops.at[pl.ds(0, owners - 1)]
        pltpu.make_async_copy(rest, rest, top_recv).wait()
        mine[...] = jnp.max(tops[...], axis=0)
        settle()

    def settled(copies):
        for go, cp in copies:
            pl.when(go)(cp.wait_send)
            pl.when(others)(cp.wait_recv)

    settled(copies)
    copies = []
    for d in (2, 1, 3):
        pack(passed, two_ref, lax.rem(b + d, SIDE) * CAP_TWO, second, (d - 1) * CAP_TWO, CAP_TWO)
        cp = send(second.at[pl.ds((d - 1) * CAP_TWO, CAP_TWO)], landed.at[pl.ds(b * CAP_TWO, CAP_TWO)],
                  sems_s.at[SIDE - 1 + d], sems_r.at[SIDE - 1 + d], chip_peer(core, a, b + d, core))
        go = jnp.logical_not(jnp.logical_and(da == 0, db + d == SIDE))
        pl.when(go)(cp.start)
        copies.append((go, cp))
    pack(passed, two_ref, b * CAP_TWO, landed, b * CAP_TWO, CAP_TWO)

    def side_slot(d):
        return landed.at[pl.ds(SIDE * CAP_TWO + d * CAP_SIDE, CAP_SIDE)]

    @pl.when(corner)
    def _():
        pltpu.make_async_copy(turning, turning, side_r).wait()
        d = SIDE - 1 - da
        cp = send(turning, side_slot(d), side_s.at[SIDE - 1], side_f.at[d], chip_peer(core, a + SIDE - da, b, core))
        cp.start()
        cp.wait_send()

    @pl.when(beside_star)
    def _():
        for d in range(SIDE - 1):
            pltpu.make_async_copy(turning, turning, side_s.at[d]).wait()

    @pl.when(relay)
    def _():
        row_blocks(SIDE, SIDE + 2)

        @pl.when(db != 2)
        def _():
            slot = jnp.where(db == 1, 1, 0)

            def far_block(p, _):
                s = of(row_order(p), 2, slot)
                got(s)
                forward(s, 2 * SIDE + 1 + p, slot)
                return 0

            lax.fori_loop(0, SIDE, far_block, 0)

    @pl.when(star)
    def _():
        acc[...] = jnp.zeros_like(acc)

        def encode_block(s):
            step = wide_step[...]
            inverse = 1.0 / step

            def fold(g, total):
                at = pl.ds(pl.multiple_of(g * period, 128), period)
                values = final[s, :, at].astype(jnp.float32)
                codes = jnp.clip(values * inverse, -127.0, 127.0).astype(jnp.bfloat16)
                final[s, :, at] = codes
                miss = values - codes.astype(jnp.float32) * step
                return total + miss * miss

            acc[...] = lax.fori_loop(0, final.shape[2] // period, fold, acc[...])

        swap_hot.wait_send()

        def arrive(n, _):
            i = n - 2
            step, which = i // 3, lax.rem(i, 3)
            early = i < 18
            row_a = jnp.where(step < 4, 1 + 2 * lax.rem(step, 2), 2)
            row_slot = jnp.where(step < 4, step // 2, step - 4)
            near_step = jnp.where(early, step, 6 + (i - 18) // 2)
            near_b = jnp.where(early, which * 2 - 1, 1 + 2 * lax.rem(i - 18, 2))
            is_row = jnp.logical_and(early, which == 0)
            is_far = i >= 22
            q = near_step - 2
            near_a = jnp.where(near_step < 2, 0, jnp.where(q < SIDE, 1 + 2 * lax.rem(q, 2), 2))
            near_slot = jnp.where(near_step < 2, near_step, jnp.where(q < SIDE, q // 2, q - SIDE))
            far_step = i - 22
            from_a = jnp.where(is_row, row_a, jnp.where(is_far, row_order(far_step // 2), near_a))
            from_b = jnp.where(is_row, 0, jnp.where(is_far, 2, near_b))
            slot = jnp.where(is_row, row_slot, jnp.where(is_far, lax.rem(far_step, 2), near_slot))
            s = jnp.where(n == 0, me, jnp.where(n == 1, beside, of(from_a, from_b, slot)))

            @pl.when(n > 0)
            def _():
                got(s)
            encode_block(s)
            return 0

        lax.fori_loop(0, owners, arrive, 0)
        row = jnp.sum(acc[...], axis=0, keepdims=True)
        parts = [row[:, m * half:(m + 1) * half] for m in range(4)]
        sums[...] = jnp.broadcast_to((parts[0] + parts[1]) + (parts[2] + parts[3]), sums.shape)

    settled(copies)

    @pl.when(relay)
    def _():
        for d in range(SIDE - 1):
            pltpu.make_async_copy(side_slot(d), side_slot(d), side_f.at[d]).wait()
    quads = flat.shape[0] // lines

    def gathered(op, join):
        row = [op(flat[pl.ds(i, quads, stride=lines), :], axis=0, keepdims=True) for i in range(lines)]
        row = jnp.concatenate(row, axis=1)
        parts = [row[:, m * half:(m + 1) * half] for m in range(4)]
        return join(join(parts[0], parts[1]), join(parts[2], parts[3]))

    @pl.when(others)
    def _():
        banks = [(q * CAP_TWO, CAP_TWO) for q in range(SIDE)]
        banks += [(SIDE * CAP_TWO + d * CAP_SIDE, CAP_SIDE) for d in range(SIDE - 1)]
        flat[...] = jnp.zeros_like(flat)
        for q, (start, size) in enumerate(banks):
            def cold_top(k, _):
                block = jnp.abs(landed[start + k].astype(jnp.float32))
                flat[...] = jnp.maximum(flat[...], jnp.where(k < number_ref[q], block, 0.0))
                return 0
            lax.fori_loop(0, size, cold_top, 0)
        mine[...] = jnp.broadcast_to(gathered(jnp.max, jnp.maximum), mine.shape)
        settle()
        for i in range(lines):
            flat_step[pl.ds(i, quads, stride=lines), :] = jnp.broadcast_to(
                wide_step[0:1, i * 128:(i + 1) * 128], (quads, 128))
        flat[...] = jnp.zeros_like(flat)
        for q, (start, size) in enumerate(banks):
            def cold_code(k, _):
                values = landed[start + k].astype(jnp.float32)
                codes = jnp.clip(values / flat_step[...], -127.0, 127.0).astype(jnp.bfloat16)
                landed[start + k] = codes
                miss = values - codes.astype(jnp.float32) * flat_step[...]
                flat[...] += jnp.where(k < number_ref[q], miss * miss, 0.0)
                return 0
            lax.fori_loop(0, size, cold_code, 0)
        sums[...] = jnp.broadcast_to(gathered(jnp.sum, jnp.add), sums.shape)
        swap_hot.wait_send()

        def drained(n, _):
            pltpu.make_async_copy(final.at[0], final.at[0], sem_send.at[n]).wait()
            return 0

        sent = jnp.where(da != 0, jnp.where(da == 2, 2, 3), jnp.where(db == 2, 8, 12))
        lax.fori_loop(1, sent + 1, drained, 0)

    for h in range(SLICES):
        @pl.when(me != SLICES * layer + h)
        def _(h=h):
            report[h].wait_send()
    trade(sums, their_sums, sum_send, sum_recv)
    step = step_ref[...]
    error_ref[...] = (jnp.sum(their_sums[...], axis=0) + sums[...]) / (step * step * denominator)


def route(layer, denominator, one, two, side, number, hot, cold, peaks):
    _, capacity, flat = hot.shape
    owners = lax.axis_size("own")
    peers = lax.axis_size("rep") - 1
    _, n_cold, lines, width = cold.shape
    period = flat // 16
    half = period // 4
    smem = pl.BlockSpec(memory_space=pltpu.SMEM)
    vmem = pl.BlockSpec(memory_space=pltpu.VMEM)
    anywhere = pl.BlockSpec(memory_space=pl.ANY)
    block, small = (capacity, flat), (lines, width)
    stat = (8, half)
    dma = pltpu.SemaphoreType.DMA
    return pl.pallas_call(
        functools.partial(route_kernel, layer, denominator),
        out_shape=(jax.ShapeDtypeStruct((owners, *block), hot.dtype),
                   jax.ShapeDtypeStruct((SIDE * CAP_TWO + (SIDE - 1) * CAP_SIDE, *small), cold.dtype),
                   jax.ShapeDtypeStruct(stat, jnp.float32),
                   jax.ShapeDtypeStruct(stat, jnp.float32)),
        in_specs=[smem, smem, smem, smem, anywhere, anywhere, anywhere],
        out_specs=(vmem, vmem, vmem, vmem),
        scratch_shapes=[
            pltpu.VMEM((2 * n_cold, *small), cold.dtype),
            pltpu.VMEM(((SIDE - 1) * CAP_ONE, *small), cold.dtype),
            pltpu.VMEM((SIDE * CAP_ONE, *small), cold.dtype),
            pltpu.VMEM(((SIDE - 1) * CAP_TWO, *small), cold.dtype),
            pltpu.VMEM(((SIDE - 1) * CAP_SIDE, *small), cold.dtype),
            pltpu.VMEM((CAP_SIDE, *small), cold.dtype),
            pltpu.VMEM((owners, *stat), jnp.float32),
            pltpu.VMEM((8, period), jnp.float32),
            pltpu.VMEM((capacity, period), jnp.float32),
            pltpu.VMEM(small, jnp.float32),
            pltpu.VMEM(small, jnp.float32),
            pltpu.VMEM(stat, jnp.float32),
            pltpu.VMEM((peers, *stat), jnp.float32),
            pltpu.VMEM(stat, jnp.float32),
            pltpu.VMEM((peers, *stat), jnp.float32),
            dma((13,)), dma((owners,)), dma((2 * SIDE - 1,)), dma((2 * SIDE - 1,)),
            dma((SIDE,)), dma, dma((SIDE - 1,)), dma((2,)),
            dma((SLICES,)), dma, dma((peers,)), dma((peers,)), dma((peers,)), dma((peers,)),
        ],
        compiler_params=pltpu.CompilerParams(collective_id=4 + layer, has_side_effects=True,
                                             vmem_limit_bytes=VMEM_ROUTE),
    )(one, two, side, number, hot, cold, peaks)


VMEM_ROUTE = 40 * 1024 * 1024
VMEM_FINISH = 20 * 1024 * 1024


def finish_kernel(layer, where_ref, final, landed, step_in, error_in, out_ref, step_ref, error_ref,
                  wide, stage, zeros, stage_sem, sem):
    owners, capacity, width = final.shape
    rows = width // 128
    step_ref[...] = step_in[0:1]
    error_ref[...] = error_in[0:1]
    star = lax.axis_index("own") // SLICES == layer
    batch = 4

    @pl.when(star)
    def _():
        copies = [pltpu.make_async_copy(final.at[pl.ds(i * batch, batch)], out_ref.at[pl.ds(i * batch, batch)], sem.at[i])
                  for i in range(owners // batch)]
        for cp in copies:
            cp.start()
        for cp in copies:
            cp.wait()

    @pl.when(jnp.logical_not(star))
    def _():
        zeros[...] = jnp.zeros_like(zeros)

        def empty(s, _):
            @pl.when(where_ref[s * capacity] < 0)
            def _():
                pltpu.make_async_copy(zeros, out_ref.at[s], sem.at[s]).start()
            return 0

        lax.fori_loop(0, owners, empty, 0)

        def fill(s, used):
            some = where_ref[s * capacity] >= 0
            slot = lax.rem(used, 2)

            @pl.when(some)
            def _():
                wide[...] = jnp.zeros_like(wide)

                def one(c, _):
                    at = where_ref[s * capacity + c]

                    @pl.when(at >= 0)
                    def _():
                        wide[pl.ds(c, rows, stride=capacity), :] = landed[at].astype(jnp.float32)
                    return 0

                lax.fori_loop(0, capacity, one, 0)

                @pl.when(used >= 2)
                def _():
                    pltpu.make_async_copy(stage.at[slot], out_ref.at[s], stage_sem.at[slot]).wait()
                for r in range(rows):
                    stage[slot, :, r * 128:(r + 1) * 128] = wide[r * capacity:(r + 1) * capacity, :].astype(jnp.bfloat16)
                pltpu.make_async_copy(stage.at[slot], out_ref.at[s], stage_sem.at[slot]).start()
            return used + some.astype(jnp.int32)

        used = lax.fori_loop(0, owners, fill, 0)
        for n in range(2):
            @pl.when(used > n)
            def _():
                pltpu.make_async_copy(stage.at[n], out_ref.at[n], stage_sem.at[n]).wait()

        def wait(s, _):
            @pl.when(where_ref[s * capacity] < 0)
            def _():
                pltpu.make_async_copy(zeros, out_ref.at[s], sem.at[s]).wait()
            return 0

        lax.fori_loop(0, owners, wait, 0)


def finish(layer, where_held, final, landed, step, error):
    owners, capacity, width = final.shape
    half = step.shape[1]
    vmem = pl.BlockSpec(memory_space=pltpu.VMEM)
    return pl.pallas_call(
        functools.partial(finish_kernel, layer),
        out_shape=(jax.ShapeDtypeStruct(final.shape, final.dtype),
                   jax.ShapeDtypeStruct((1, half), jnp.float32),
                   jax.ShapeDtypeStruct((1, half), jnp.float32)),
        in_specs=[pl.BlockSpec(memory_space=pltpu.SMEM), vmem, vmem, vmem, vmem],
        out_specs=(pl.BlockSpec(memory_space=pltpu.HBM), vmem, vmem),
        scratch_shapes=[
            pltpu.VMEM((width // 128 * capacity, 128), jnp.float32),
            pltpu.VMEM((2, capacity, width), final.dtype),
            pltpu.VMEM((capacity, width), final.dtype),
            pltpu.SemaphoreType.DMA((2,)),
            pltpu.SemaphoreType.DMA((owners,)),
        ],
        compiler_params=pltpu.CompilerParams(vmem_limit_bytes=VMEM_FINISH),
    )(where_held, final, landed, step, error)


def body(block_pool, sel_index, sel_layer, counts):
    own_count = lax.axis_size("own")
    rep_count = lax.axis_size("rep")
    layers = own_count // SLICES
    n_select = sel_index.shape[0]
    capacity = n_select // 4
    tokens = block_pool.shape[1]
    half = block_pool.shape[2] // SLICES
    period = 4 * half
    denominator = float(own_count * rep_count * capacity * tokens)
    hot, cold, table, tops = open_exchange(block_pool, sel_index, sel_layer, counts, capacity)
    fits, one, two, side, number, where_held = plan(sel_layer, table, capacity, n_select - capacity)

    def routed(layer):
        return finish(layer, where_held, *route(layer, denominator, one, two, side, number, hot, cold, tops))

    def sparse():
        return lax.switch(sel_layer[0], [functools.partial(routed, layer) for layer in range(layers)])

    def dense():
        parted = part(block_pool, sel_index, sel_layer, counts, layers, capacity)
        arrived = lax.all_to_all(parted, "own", split_axis=0, concat_axis=0, tiled=True)
        top = jnp.max(peaks(arrived, period)[0].reshape(4, half), axis=0)
        step = HEADROOM * jnp.maximum(top, 1.0) / 127.0
        codes, err = encode(arrived, jnp.tile(step, 4)[None, :], period)
        return codes, step[None, :], totals(err, step[None, :], denominator)

    codes, step, error = lax.cond(fits[0] == 1, sparse, dense)
    return codes[None, None], step, error


def solution(mesh):
    return jax.shard_map(
        body,
        mesh=mesh,
        in_specs=(
            P(("own", "rep"), None, None),
            P(("own", "rep")),
            P(("own", "rep")),
            P(("own", "rep")),
        ),
        out_specs=(P("own", "rep", None, None, None), P("own", None), P("own", None)),
        check_vma=False,
    )
```

```python
import functools

import jax
import jax.numpy as jnp
from jax import lax
from jax.experimental import pallas as pl
from jax.experimental.pallas import tpu as pltpu
from jax.sharding import PartitionSpec as P

SLICES = 2
HEADROOM = 0.5
MESH = pl.DeviceIdType.MESH


def part_kernel(layers, capacity, half, idx_ref, lay_ref, cnt_ref, pool_ref, out_ref,
                blocks, wide, stage, zeros, slot_of, in_sem, out_sem, zero_sem):
    n_select = idx_ref.shape[0]
    tokens = blocks.shape[1]
    latent = blocks.shape[2]
    for j in range(n_select):
        pltpu.make_async_copy(pool_ref.at[idx_ref[j]], blocks.at[j], in_sem).start()
    live = cnt_ref[0]

    def clear(i, _):
        slot_of[i] = -1
        return 0

    lax.fori_loop(0, layers * capacity + layers, clear, 0)

    def place(j, _):
        layer = lay_ref[j]

        @pl.when(j < live)
        def _():
            rank = slot_of[layers * capacity + layer] + 1
            slot_of[layers * capacity + layer] = rank
            slot_of[layer * capacity + rank] = j
        return 0

    lax.fori_loop(0, n_select, place, 0)
    zeros[...] = jnp.zeros_like(zeros)
    pltpu.make_async_copy(pool_ref.at[pl.ds(0, n_select)], blocks, in_sem).wait()

    def one_layer(layer, used):
        some = slot_of[layers * capacity + layer] >= 0

        @pl.when(jnp.logical_not(some))
        def _():
            cp = pltpu.make_async_copy(zeros, out_ref.at[pl.ds(layer * SLICES, SLICES)], zero_sem)
            cp.start()
            cp.wait()

        @pl.when(some)
        def _():
            @pl.when(used > 0)
            def _():
                pltpu.make_async_copy(stage.at[0], out_ref.at[pl.ds(0, SLICES)], out_sem).wait()
            for c in range(capacity):
                j = slot_of[layer * capacity + c]

                @pl.when(j >= 0)
                def _():
                    for k in range(wide.shape[0]):
                        cols = min(128, latent - k * 128)
                        wide[k, pl.ds(c * tokens, tokens), :cols] = blocks[j, :, k * 128:k * 128 + cols].astype(jnp.float32)

                @pl.when(j < 0)
                def _():
                    wide[:, pl.ds(c * tokens, tokens), :] = jnp.zeros((wide.shape[0], tokens, 128), jnp.float32)

            def four(q, _):
                rows = [jnp.concatenate([wide[k, pl.ds(4 * q + m, capacity, stride=tokens), :]
                                         for k in range(wide.shape[0])], axis=1) for m in range(4)]
                for h in range(SLICES):
                    flat = jnp.concatenate([r[:, h * half:(h + 1) * half] for r in rows], axis=1)
                    stage[0, h, :, pl.ds(pl.multiple_of(q * 4 * half, 128), 4 * half)] = flat.astype(jnp.bfloat16)
                return 0

            lax.fori_loop(0, tokens // 4, four, 0)
            pltpu.make_async_copy(stage.at[0], out_ref.at[pl.ds(layer * SLICES, SLICES)], out_sem).start()
        return used + some.astype(jnp.int32)

    used = lax.fori_loop(0, layers, one_layer, 0)

    @pl.when(used > 0)
    def _():
        pltpu.make_async_copy(stage.at[0], out_ref.at[pl.ds(0, SLICES)], out_sem).wait()


def part(block_pool, sel_index, sel_layer, counts, layers, capacity):
    rows, tokens, latent = block_pool.shape
    half = latent // SLICES
    n_select = sel_index.shape[0]
    groups = layers * SLICES
    smem = pl.BlockSpec(memory_space=pltpu.SMEM)
    return pl.pallas_call(
        functools.partial(part_kernel, layers, capacity, half),
        out_shape=jax.ShapeDtypeStruct((groups, capacity, tokens * half), jnp.bfloat16),
        in_specs=[smem, smem, smem, pl.BlockSpec(memory_space=pltpu.HBM)],
        out_specs=pl.BlockSpec(memory_space=pltpu.HBM),
        scratch_shapes=[
            pltpu.VMEM((n_select, tokens, latent), jnp.bfloat16),
            pltpu.VMEM((-(-latent // 128), capacity * tokens, 128), jnp.float32),
            pltpu.VMEM((1, SLICES, capacity, tokens * half), jnp.bfloat16),
            pltpu.VMEM((SLICES, capacity, tokens * half), jnp.bfloat16),
            pltpu.SMEM((layers * capacity + layers,), jnp.int32),
            pltpu.SemaphoreType.DMA,
            pltpu.SemaphoreType.DMA,
            pltpu.SemaphoreType.DMA,
        ],
    )(sel_index, sel_layer, counts, block_pool)


def rep_peers():
    me = lax.axis_index("rep")
    count = lax.axis_size("rep")
    return [lax.rem(me + d, count) for d in range(1, count)]


def greet():
    barrier = pltpu.get_barrier_semaphore()
    for peer in rep_peers():
        pl.semaphore_signal(barrier, inc=1, device_id={"rep": peer}, device_id_type=MESH)


def share(mine, theirs, send_sem, recv_sem):
    pl.semaphore_wait(pltpu.get_barrier_semaphore(), len(rep_peers()))
    copies = []
    for i, peer in enumerate(rep_peers()):
        cp = pltpu.make_async_remote_copy(
            src_ref=mine, dst_ref=theirs.at[i], send_sem=send_sem.at[i], recv_sem=recv_sem.at[i],
            device_id={"rep": peer}, device_id_type=MESH)
        cp.start()
        copies.append(cp)
    for cp in copies:
        cp.wait()


def peak_kernel(steps, period, x_ref, out_ref, acc, mine, theirs, send_sem, recv_sem):
    i = pl.program_id(0)

    @pl.when(i == 0)
    def _():
        greet()
        acc[...] = jnp.zeros_like(acc)

    def fold(g, top):
        chunk = x_ref[:, :, pl.ds(pl.multiple_of(g * period, 128), period)].astype(jnp.float32)
        return jnp.maximum(top, jnp.max(jnp.abs(chunk), axis=0))

    acc[...] = lax.fori_loop(0, x_ref.shape[2] // period, fold, acc[...])

    @pl.when(i == steps - 1)
    def _():
        mine[...] = jnp.broadcast_to(jnp.max(acc[...], axis=0, keepdims=True), mine.shape)
        share(mine, theirs, send_sem, recv_sem)
        out_ref[...] = jnp.maximum(jnp.max(theirs[...], axis=0), mine[...])


def peaks(arrived, period, per_step=4):
    sources, capacity, flat = arrived.shape
    steps = sources // per_step
    peers = lax.axis_size("rep") - 1
    return pl.pallas_call(
        functools.partial(peak_kernel, steps, period),
        grid=(steps,),
        out_shape=jax.ShapeDtypeStruct((8, period), jnp.float32),
        in_specs=[pl.BlockSpec((per_step, capacity, flat), lambda i: (i, 0, 0))],
        out_specs=pl.BlockSpec((8, period), lambda i: (0, 0)),
        scratch_shapes=[
            pltpu.VMEM((capacity, period), jnp.float32),
            pltpu.VMEM((8, period), jnp.float32),
            pltpu.VMEM((peers, 8, period), jnp.float32),
            pltpu.SemaphoreType.DMA((peers,)),
            pltpu.SemaphoreType.DMA((peers,)),
        ],
        compiler_params=pltpu.CompilerParams(collective_id=0, has_side_effects=True),
    )(arrived)


def code_kernel(period, x_ref, step_ref, out_ref, err_ref):
    @pl.when(pl.program_id(0) == 0)
    def _():
        err_ref[...] = jnp.zeros_like(err_ref)

    step = jnp.broadcast_to(step_ref[...], err_ref.shape)
    inverse = 1.0 / step

    def fold(g, total):
        at = pl.ds(pl.multiple_of(g * period, 128), period)
        for s in range(x_ref.shape[0]):
            values = x_ref[s, :, at].astype(jnp.float32)
            codes = jnp.clip(values * inverse, -127.0, 127.0).astype(jnp.bfloat16)
            out_ref[s, :, at] = codes
            miss = values - codes.astype(jnp.float32) * step
            total = total + miss * miss
        return total

    err_ref[...] = lax.fori_loop(0, x_ref.shape[2] // period, fold, err_ref[...])


def encode(arrived, step_row, period, per_step=4):
    sources, capacity, flat = arrived.shape
    return pl.pallas_call(
        functools.partial(code_kernel, period),
        grid=(sources // per_step,),
        out_shape=(jax.ShapeDtypeStruct(arrived.shape, jnp.bfloat16),
                   jax.ShapeDtypeStruct((capacity, period), jnp.float32)),
        in_specs=[pl.BlockSpec((per_step, capacity, flat), lambda i: (i, 0, 0)),
                  pl.BlockSpec((1, period), lambda i: (0, 0))],
        out_specs=(pl.BlockSpec((per_step, capacity, flat), lambda i: (i, 0, 0)),
                   pl.BlockSpec((capacity, period), lambda i: (0, 0))),
    )(arrived, step_row)


def total_kernel(denominator, err_ref, step_ref, out_ref, mine, theirs, send_sem, recv_sem):
    greet()
    half = step_ref.shape[1]
    row = jnp.sum(err_ref[...], axis=0, keepdims=True)
    parts = [row[:, m * half:(m + 1) * half] for m in range(4)]
    mine[...] = jnp.broadcast_to((parts[0] + parts[1]) + (parts[2] + parts[3]), mine.shape)
    share(mine, theirs, send_sem, recv_sem)
    total = (jnp.sum(theirs[...], axis=0) + mine[...])[0:1]
    step = step_ref[...]
    out_ref[...] = total / (step * step * denominator)


def totals(err, step, denominator):
    half = step.shape[1]
    peers = lax.axis_size("rep") - 1
    vmem = pl.BlockSpec(memory_space=pltpu.VMEM)
    return pl.pallas_call(
        functools.partial(total_kernel, denominator),
        out_shape=jax.ShapeDtypeStruct((1, half), jnp.float32),
        in_specs=[vmem, vmem],
        out_specs=vmem,
        scratch_shapes=[
            pltpu.VMEM((8, half), jnp.float32),
            pltpu.VMEM((peers, 8, half), jnp.float32),
            pltpu.SemaphoreType.DMA((peers,)),
            pltpu.SemaphoreType.DMA((peers,)),
        ],
        compiler_params=pltpu.CompilerParams(collective_id=1, has_side_effects=True),
    )(err, step)


SIDE = 4
CAP_ONE = 22
CAP_TWO = 18
CAP_SIDE = 8
BY_LAYER, BY_SIDE, LIVE = 32, 48, 56


def open_kernel(half, idx_ref, lay_ref, cnt_ref, pool_ref, hot_ref, cold_ref, table_ref, peaks_ref,
                pool, wide, flat, row_ref, pool_sem, own_send, own_recv, send_sem, recv_sem):
    n_select = idx_ref.shape[0]
    tokens, latent = pool.shape[1], pool.shape[2]
    capacity = hot_ref.shape[1]
    tiles = wide.shape[0]
    fetch = pltpu.make_async_copy(pool_ref, pool, pool_sem)
    fetch.start()
    me, mine = lax.axis_index("own"), lax.axis_index("rep")
    owners = lax.axis_size("own")
    barrier = pltpu.get_barrier_semaphore()

    def hello(i, _):
        pl.semaphore_signal(barrier, inc=1, device_id={"own": lax.rem(me + i, owners)}, device_id_type=MESH)
        return 0

    lax.fori_loop(1, owners, hello, 0)
    greet()

    lane = lax.broadcasted_iota(jnp.int32, (1, 128), 1)
    live = cnt_ref[0]
    row = jnp.where(lane == LIVE, live, jnp.where(lane < BY_LAYER, -1, 0))
    for j in range(n_select):
        layer = lay_ref[j]
        is_live = jnp.where(j < live, 1, 0)
        row = jnp.where(lane == j, jnp.where(j < live, layer, -1), row)
        if j >= capacity:
            spot = ((lane == BY_LAYER + layer) | (lane == BY_SIDE + lax.shift_right_logical(layer, 2))
                    | (lane == BY_SIDE + SIDE + (layer & (SIDE - 1))))
            row = row + jnp.where(spot, is_live, 0)
    row_ref[...] = row
    table_ref[mine, me] = row
    pl.semaphore_wait(barrier, owners - 1 + len(rep_peers()))

    def push(i, _):
        pltpu.make_async_remote_copy(
            src_ref=row_ref, dst_ref=table_ref.at[mine, me], send_sem=own_send, recv_sem=own_recv,
            device_id={"own": lax.rem(me + i, owners)}, device_id_type=MESH).start()
        return 0

    lax.fori_loop(1, owners, push, 0)
    fetch.wait()

    def widen(j, to):
        at = idx_ref[j]
        for k in range(tiles):
            cols = min(128, latent - k * 128)
            wide[k, pl.ds(to, tokens), :cols] = pool[at, :, k * 128:k * 128 + cols].astype(jnp.float32)

    def strided(start, count, stride):
        return jnp.concatenate([wide[k, pl.ds(start, count, stride=stride), :] for k in range(tiles)], axis=1)

    for c in range(capacity):
        widen(c, c * tokens)

    def four(q, top):
        rows = [strided(4 * q + m, capacity, tokens) for m in range(4)]
        for r in rows:
            top = jnp.maximum(top, jnp.abs(r))
        for h in range(SLICES):
            line = jnp.concatenate([r[:, h * half:(h + 1) * half] for r in rows], axis=1)
            hot_ref[h, :, pl.ds(pl.multiple_of(q * 4 * half, 128), 4 * half)] = line.astype(jnp.bfloat16)
        return top

    top = lax.fori_loop(0, tokens // 4, four, jnp.zeros((capacity, tiles * 128), jnp.float32))
    top = jnp.max(top, axis=0, keepdims=True)
    for h in range(SLICES):
        peaks_ref[h] = jnp.broadcast_to(top[:, h * half:(h + 1) * half], peaks_ref.shape[1:])

    rest = table_ref.at[mine, pl.ds(0, owners - 1)]
    pltpu.make_async_copy(rest, rest, own_recv).wait()
    pltpu.make_async_copy(rest, rest, own_send).wait()
    copies = []
    for i, peer in enumerate(rep_peers()):
        cp = pltpu.make_async_remote_copy(
            src_ref=table_ref.at[mine], dst_ref=table_ref.at[mine], send_sem=send_sem.at[i], recv_sem=recv_sem.at[i],
            device_id={"rep": peer}, device_id_type=MESH)
        cp.start()
        copies.append(cp)

    quads = tokens // 4
    lines = 4 * half // 128

    def one(j, _):
        widen(j, 0)
        rows = [strided(m, quads, 4) for m in range(4)]
        for h in range(SLICES):
            line = jnp.concatenate([r[:, h * half:(h + 1) * half] for r in rows], axis=1)
            for i in range(lines):
                flat[h, pl.ds(i, quads, stride=lines), :] = line[:, i * 128:(i + 1) * 128]
        for h in range(SLICES):
            cold_ref[h, j - capacity] = flat[h].astype(jnp.bfloat16)
        return 0

    lax.fori_loop(capacity, n_select, one, 0)
    for cp in copies:
        cp.wait()


def open_exchange(block_pool, sel_index, sel_layer, counts, capacity):
    _, tokens, latent = block_pool.shape
    half = latent // SLICES
    n_select = sel_index.shape[0]
    lines = tokens * half // 128
    owners, reps = lax.axis_size("own"), lax.axis_size("rep")
    smem = pl.BlockSpec(memory_space=pltpu.SMEM)
    vmem = pl.BlockSpec(memory_space=pltpu.VMEM)
    return pl.pallas_call(
        functools.partial(open_kernel, half),
        out_shape=(jax.ShapeDtypeStruct((SLICES, capacity, tokens * half), jnp.bfloat16),
                   jax.ShapeDtypeStruct((SLICES, n_select - capacity, lines, 128), jnp.bfloat16),
                   jax.ShapeDtypeStruct((reps, owners, 1, 128), jnp.int32),
                   jax.ShapeDtypeStruct((SLICES, 8, half), jnp.float32)),
        in_specs=[smem, smem, smem, pl.BlockSpec(memory_space=pltpu.HBM)],
        out_specs=(vmem, vmem, vmem, vmem),
        scratch_shapes=[
            pltpu.VMEM(block_pool.shape, jnp.bfloat16),
            pltpu.VMEM((-(-latent // 128), capacity * tokens, 128), jnp.float32),
            pltpu.VMEM((SLICES, lines, 128), jnp.float32),
            pltpu.VMEM((1, 128), jnp.int32),
            pltpu.SemaphoreType.DMA,
            pltpu.SemaphoreType.DMA,
            pltpu.SemaphoreType.DMA,
            pltpu.SemaphoreType.DMA((reps - 1,)),
            pltpu.SemaphoreType.DMA((reps - 1,)),
        ],
        compiler_params=pltpu.CompilerParams(collective_id=2, has_side_effects=True),
    )(sel_index, sel_layer, counts, block_pool)


def place():
    me = lax.axis_index("own")
    core = lax.rem(me, 2)
    x, z = me // (2 * SIDE), lax.rem(me // 2, SIDE)
    return core, jnp.where(core == 0, x, z), jnp.where(core == 0, z, x)


def index_of(core, a, b, slot):
    return jnp.where(core == 0, a * SIDE + b, b * SIDE + a) * 2 + slot


def chip_peer(core, a, b, slot):
    return {"own": index_of(core, lax.rem(a, SIDE), lax.rem(b, SIDE), slot)}


def plan_kernel(capacity, n_cold, lay_ref, table_ref, rows_ref, fits_ref, one_ref, two_ref, side_ref, number_ref, where_ref,
                near, rank_one, rank_two, rank_side, sem):
    core, a, b = place()
    me = lax.axis_index("own")
    cp = pltpu.make_async_copy(rows_ref.at[lax.axis_index("rep")], near, sem)
    cp.start()
    reps, owners = table_ref.shape[0], table_ref.shape[1]
    lane = lax.broadcasted_iota(jnp.int32, (1, 128), 1)
    one, two, side = (jnp.zeros((1, 128), jnp.int32) for _ in range(3))
    star_x, star_z = lax.shift_right_logical(lay_ref[0], 2), lay_ref[0] & (SIDE - 1)
    star_a, star_b = jnp.where(core == 0, star_x, star_z), jnp.where(core == 0, star_z, star_x)
    named = (lane >= BY_LAYER) & (lane < BY_SIDE)
    in_column = jnp.where(named & (lax.shift_right_logical(lane - BY_LAYER, 2) == star_x), 1, 0)
    in_row = jnp.where(named & (((lane - BY_LAYER) & (SIDE - 1)) == star_z), 1, 0)
    for r in range(reps):
        chips = [table_ref[r, 2 * c] + table_ref[r, 2 * c + 1] for c in range(SIDE * SIDE)]
        for c in chips:
            one = jnp.maximum(one, c)
        for i, c in enumerate(chips):
            x, z = i // SIDE, i % SIDE
            turns_x = jnp.where(jnp.logical_and(star_z == z, star_x != x), 1, 0)
            turns_z = jnp.where(jnp.logical_and(star_x == x, star_z != z), 1, 0)
            side = jnp.maximum(side, c * (in_column * turns_x + in_row * turns_z))
        for i in range(SIDE):
            for picked in (chips[i::SIDE], chips[SIDE * i:SIDE * i + SIDE]):
                two = jnp.maximum(two, (picked[0] + picked[1]) + (picked[2] + picked[3]))
    side = side.astype(jnp.float32)
    one = jnp.where((lane >= BY_SIDE) & (lane < LIVE), one, 0).astype(jnp.float32)
    two = jnp.where(named, two, 0).astype(jnp.float32)
    fits = jnp.logical_and(jnp.max(one) <= CAP_ONE, jnp.max(two) <= CAP_TWO)
    fits_ref[0] = jnp.where(jnp.logical_and(fits, jnp.max(side) <= CAP_SIDE), 1, 0)

    def clear(ref, value):
        def put(i, _):
            ref[i] = value
            return 0
        lax.fori_loop(0, ref.shape[0], put, 0, unroll=8 if ref.shape[0] % 8 == 0 else 1)

    clear(one_ref, 0)
    clear(two_ref, 0)
    clear(side_ref, 0)
    clear(number_ref, 0)
    clear(where_ref, -1)
    clear(rank_two, 0)
    clear(rank_side, 0)
    cp.wait()
    layer_here = me // 2

    def column(a_from, _):
        clear(rank_one, 0)
        turn = jnp.logical_and(b == star_b, a_from != star_a)
        for slot in range(2):
            device = index_of(core, a_from, b, slot)

            def entry(j, _):
                layer = near[device, 0, j]
                high, low = lax.shift_right_logical(layer, 2), layer & (SIDE - 1)
                to_a = jnp.where(core == 0, high, low)
                to_b = jnp.where(core == 0, low, high)
                aside = jnp.logical_and(turn, to_a == star_a)

                @pl.when(jnp.logical_and(aside, a_from == a))
                def _():
                    rank = rank_side[to_b]
                    rank_side[to_b] = rank + 1
                    side_ref[to_b * CAP_SIDE + jnp.minimum(rank, CAP_SIDE - 1)] = slot * n_cold + j - capacity

                @pl.when(jnp.logical_not(aside))
                def _():
                    first = rank_one[to_a]
                    rank_one[to_a] = first + 1
                    first = jnp.minimum(first, CAP_ONE - 1)

                    @pl.when(a_from == a)
                    def _():
                        one_ref[to_a * CAP_ONE + first] = slot * n_cold + j - capacity

                    @pl.when(to_a == a)
                    def _():
                        second = rank_two[to_b]
                        rank_two[to_b] = second + 1
                        two_ref[to_b * CAP_TWO + jnp.minimum(second, CAP_TWO - 1)] = a_from * CAP_ONE + first
                return 0

            lax.fori_loop(capacity, near[device, 0, LIVE], entry, 0)
        return 0

    lax.fori_loop(0, SIDE, column, 0)

    def arriving(n, _):
        b_from, a_from, slot = n // (2 * SIDE), lax.rem(n // 2, SIDE), lax.rem(n, 2)
        device = index_of(core, a_from, b_from, slot)
        aside = jnp.logical_and(jnp.logical_and(b_from == star_b, a == star_a), a_from != star_a)
        d = lax.rem(a + SIDE - a_from, SIDE) - 1
        bank = jnp.where(aside, SIDE + d, b_from)
        base = jnp.where(aside, SIDE * CAP_TWO + d * CAP_SIDE, b_from * CAP_TWO)

        @pl.when(near[device, 0, BY_LAYER + layer_here] > 0)
        def _():
            def entry(j, held):
                hit = near[device, 0, j] == layer_here

                @pl.when(hit)
                def _():
                    count = number_ref[bank]
                    number_ref[bank] = count + 1
                    where_ref[device * capacity + held] = base + count
                return held + jnp.where(hit, 1, 0)

            lax.fori_loop(capacity, near[device, 0, LIVE], entry, 0)
        return 0

    lax.fori_loop(0, owners, arriving, 0)


def plan(sel_layer, table, capacity, n_cold):
    reps, owners = table.shape[0], table.shape[1]
    smem = pl.BlockSpec(memory_space=pltpu.SMEM)
    sizes = (1, SIDE * CAP_ONE, SIDE * CAP_TWO, SIDE * CAP_SIDE, 2 * SIDE, owners * capacity)
    return pl.pallas_call(
        functools.partial(plan_kernel, capacity, n_cold),
        out_shape=tuple(jax.ShapeDtypeStruct((n,), jnp.int32) for n in sizes),
        in_specs=[smem, pl.BlockSpec(memory_space=pltpu.VMEM), pl.BlockSpec(memory_space=pl.ANY)],
        out_specs=tuple(smem for _ in sizes),
        scratch_shapes=[
            pltpu.SMEM((owners, 1, 128), jnp.int32),
            pltpu.SMEM((SIDE,), jnp.int32),
            pltpu.SMEM((SIDE,), jnp.int32),
            pltpu.SMEM((SIDE,), jnp.int32),
            pltpu.SemaphoreType.DMA,
        ],
    )(sel_layer, table, table)


def route_kernel(layer, denominator, one_ref, two_ref, side_ref, number_ref, hot_ref, cold_ref, peaks_ref,
                 final, landed, step_ref, error_ref,
                 held, first, passed, second, turned, turning, tops, wide_step, wide_inverse, acc, flat, flat_step, flat_inverse, mine, theirs, sums, their_sums,
                 sem_send, sem_block, sems_s, sems_r, side_s, side_r, side_f, local, top_send, top_recv, send_sem, recv_sem, sum_send, sum_recv):
    core, a, b = place()
    me = lax.axis_index("own")
    owners = final.shape[0]
    other = 1 - core
    beside = index_of(core, a, b, other)
    n_cold = cold_ref.shape[1]
    star_x, star_z = layer // SIDE, layer % SIDE
    star_a = jnp.where(core == 0, star_x, star_z)
    star_b = jnp.where(core == 0, star_z, star_x)
    da = lax.rem(a + SIDE - star_a, SIDE)
    db = lax.rem(b + SIDE - star_b, SIDE)
    relay = jnp.logical_and(da == 0, db != 0)
    star = jnp.logical_and(da == 0, db == 0)
    others = jnp.logical_not(star)
    beside_star = jnp.logical_and(da != 0, db == 0)
    corner = jnp.logical_and(da != 0, db != 0)
    barrier = pltpu.get_barrier_semaphore()
    partner = chip_peer(core, a, b, other)
    pl.semaphore_signal(barrier, inc=1, device_id=partner, device_id_type=MESH)
    for d in range(1, SIDE):
        pl.semaphore_signal(barrier, inc=1, device_id=chip_peer(core, a + d, b, core), device_id_type=MESH)
        pl.semaphore_signal(barrier, inc=1, device_id=chip_peer(core, a, b + d, core), device_id_type=MESH)
    greet()

    @pl.when(star)
    def _():
        def invite(i, _):
            pl.semaphore_signal(barrier, inc=1, device_id={"own": lax.rem(me + i, owners)}, device_id_type=MESH)
            return 0

        lax.fori_loop(1, owners, invite, 0)

    keep_hot = pltpu.make_async_copy(hot_ref.at[core], final.at[me], local.at[0])
    keep_hot.start()
    keep_cold = pltpu.make_async_copy(cold_ref.at[core], held.at[pl.ds(core * n_cold, n_cold)], local.at[1])
    keep_cold.start()
    pl.semaphore_wait(barrier, 2 * SIDE - 1 + len(rep_peers()) + jnp.where(star, 1, 2))

    def send(src, dst, send_at, recv_at, to):
        return pltpu.make_async_remote_copy(
            src_ref=src, dst_ref=dst, send_sem=send_at, recv_sem=recv_at, device_id=to, device_id_type=MESH)

    swap_hot = send(hot_ref.at[other], final.at[me], sem_send.at[0], sem_block.at[me], partner)
    swap_hot.start()
    swap_cold = send(cold_ref.at[other], held.at[pl.ds(core * n_cold, n_cold)], sems_s.at[0], sems_r.at[0], partner)
    swap_cold.start()
    report = [send(peaks_ref.at[h], tops.at[me], top_send.at[h], top_recv, {"own": SLICES * layer + h})
              for h in range(SLICES)]
    for h in range(SLICES):
        @pl.when(me != SLICES * layer + h)
        def _(h=h):
            report[h].start()
    keep_hot.wait()

    dist = jnp.where(da != 0, da, db)

    def onward(slot):
        step = jnp.where(dist == 2, jnp.where(slot == 0, 1, SIDE - 1), SIDE - dist)
        return chip_peer(core, a + jnp.where(da != 0, step, 0), b + jnp.where(da != 0, 0, step), core)

    def forward(s, n, slot):
        send(final.at[s], final.at[s], sem_send.at[n], sem_block.at[s], onward(slot)).start()

    def got(s):
        pltpu.make_async_copy(final.at[s], final.at[s], sem_block.at[s]).wait()

    @pl.when(others)
    def _():
        forward(me, 1, core)
        got(beside)
        forward(beside, 2, other)

    keep_cold.wait()
    swap_cold.wait()

    def pack(src, table, at, dst, start, count):
        def body(k, _):
            dst[start + k] = src[table[at + k]]
            return 0
        lax.fori_loop(0, count, body, 0)

    copies = []
    for d in (2, 1, 3):
        pack(held, one_ref, lax.rem(a + d, SIDE) * CAP_ONE, first, (d - 1) * CAP_ONE, CAP_ONE)
        cp = send(first.at[pl.ds((d - 1) * CAP_ONE, CAP_ONE)], passed.at[pl.ds(a * CAP_ONE, CAP_ONE)],
                  sems_s.at[d], sems_r.at[d], chip_peer(core, a + d, b, core))
        go = jnp.logical_not(jnp.logical_and(db == 0, da + d == SIDE))
        pl.when(go)(cp.start)
        copies.append((go, cp))

    for d in range(1, SIDE):
        @pl.when(beside_star)
        def _(d=d):
            at = (d - 1) * CAP_SIDE
            pack(held, side_ref, lax.rem(b + d, SIDE) * CAP_SIDE, turned, at, CAP_SIDE)
            send(turned.at[pl.ds(at, CAP_SIDE)], turning, side_s.at[d - 1], side_r, chip_peer(core, a, b + d, core)).start()
    pack(held, one_ref, a * CAP_ONE, passed, a * CAP_ONE, CAP_ONE)

    @pl.when(jnp.logical_or(da == 1, da == 3))
    def _():
        slot = jnp.where(da == 1, 1, 0)
        s = index_of(core, lax.rem(star_a + 2, SIDE), b, slot)
        got(s)
        forward(s, 3, slot)

    def of(a_from, b_from, slot):
        return index_of(core, lax.rem(star_a + a_from, SIDE), lax.rem(star_b + b_from, SIDE), slot)

    def row_order(p):
        return jnp.where(p < 2, p, 5 - p)

    def row_blocks(start, stop):
        def row_block(i, _):
            near = i < SIDE
            slot = jnp.where(near, i // 2, i - SIDE)
            s = of(jnp.where(near, 1 + 2 * lax.rem(i, 2), 2), db, slot)
            got(s)
            forward(s, 3 + i, slot)
            return 0

        lax.fori_loop(start, stop, row_block, 0)

    @pl.when(relay)
    def _():
        row_blocks(0, SIDE)

    period = acc.shape[1]
    lines = period // 128
    half = period // 4

    def trade(src, dst, send_at, recv_at):
        cps = []
        for i, peer in enumerate(rep_peers()):
            cp = send(src, dst.at[i], send_at.at[i], recv_at.at[i], {"rep": peer})
            cp.start()
            cps.append(cp)
        for cp in cps:
            cp.wait()

    def settle():
        trade(mine, theirs, send_sem, recv_sem)
        peak = jnp.maximum(jnp.max(theirs[...], axis=0), mine[...])
        step = HEADROOM * jnp.maximum(peak, 1.0) / 127.0
        step_ref[...] = step
        wide_step[...] = jnp.concatenate([step] * 4, axis=1)
        wide_inverse[...] = jnp.concatenate([1.0 / step] * 4, axis=1)

    @pl.when(star)
    def _():
        own_top = pltpu.make_async_copy(peaks_ref.at[core], tops.at[me], local.at[0])
        own_top.start()
        own_top.wait()
        rest = tops.at[pl.ds(0, owners - 1)]
        pltpu.make_async_copy(rest, rest, top_recv).wait()
        mine[...] = jnp.max(tops[...], axis=0)
        settle()

    def settled(copies):
        for go, cp in copies:
            pl.when(go)(cp.wait_send)
            pl.when(others)(cp.wait_recv)

    settled(copies)
    copies = []
    for d in (2, 1, 3):
        pack(passed, two_ref, lax.rem(b + d, SIDE) * CAP_TWO, second, (d - 1) * CAP_TWO, CAP_TWO)
        cp = send(second.at[pl.ds((d - 1) * CAP_TWO, CAP_TWO)], landed.at[pl.ds(b * CAP_TWO, CAP_TWO)],
                  sems_s.at[SIDE - 1 + d], sems_r.at[SIDE - 1 + d], chip_peer(core, a, b + d, core))
        go = jnp.logical_not(jnp.logical_and(da == 0, db + d == SIDE))
        pl.when(go)(cp.start)
        copies.append((go, cp))
    pack(passed, two_ref, b * CAP_TWO, landed, b * CAP_TWO, CAP_TWO)

    def side_slot(d):
        return landed.at[pl.ds(SIDE * CAP_TWO + d * CAP_SIDE, CAP_SIDE)]

    @pl.when(corner)
    def _():
        pltpu.make_async_copy(turning, turning, side_r).wait()
        d = SIDE - 1 - da
        cp = send(turning, side_slot(d), side_s.at[SIDE - 1], side_f.at[d], chip_peer(core, a + SIDE - da, b, core))
        cp.start()
        cp.wait_send()

    @pl.when(beside_star)
    def _():
        for d in range(SIDE - 1):
            pltpu.make_async_copy(turning, turning, side_s.at[d]).wait()

    @pl.when(relay)
    def _():
        row_blocks(SIDE, SIDE + 2)

        @pl.when(db != 2)
        def _():
            slot = jnp.where(db == 1, 1, 0)

            def far_block(p, _):
                s = of(row_order(p), 2, slot)
                got(s)
                forward(s, 2 * SIDE + 1 + p, slot)
                return 0

            lax.fori_loop(0, SIDE, far_block, 0)

    @pl.when(star)
    def _():
        acc[...] = jnp.zeros_like(acc)

        def encode_block(s):
            step = wide_step[...]
            inverse = wide_inverse[...]

            def fold(g, total):
                at = pl.ds(pl.multiple_of(g * period, 128), period)
                values = final[s, :, at].astype(jnp.float32)
                codes = jnp.clip(values * inverse, -127.0, 127.0).astype(jnp.bfloat16)
                final[s, :, at] = codes
                miss = values - codes.astype(jnp.float32) * step
                return total + miss * miss

            acc[...] = lax.fori_loop(0, final.shape[2] // period, fold, acc[...], unroll=2)

        swap_hot.wait_send()

        def arrive(n, _):
            i = n - 2
            step, which = i // 3, lax.rem(i, 3)
            early = i < 18
            row_a = jnp.where(step < 4, 1 + 2 * lax.rem(step, 2), 2)
            row_slot = jnp.where(step < 4, step // 2, step - 4)
            near_step = jnp.where(early, step, 6 + (i - 18) // 2)
            near_b = jnp.where(early, which * 2 - 1, 1 + 2 * lax.rem(i - 18, 2))
            is_row = jnp.logical_and(early, which == 0)
            is_far = i >= 22
            q = near_step - 2
            near_a = jnp.where(near_step < 2, 0, jnp.where(q < SIDE, 1 + 2 * lax.rem(q, 2), 2))
            near_slot = jnp.where(near_step < 2, near_step, jnp.where(q < SIDE, q // 2, q - SIDE))
            far_step = i - 22
            from_a = jnp.where(is_row, row_a, jnp.where(is_far, row_order(far_step // 2), near_a))
            from_b = jnp.where(is_row, 0, jnp.where(is_far, 2, near_b))
            slot = jnp.where(is_row, row_slot, jnp.where(is_far, lax.rem(far_step, 2), near_slot))
            s = jnp.where(n == 0, me, jnp.where(n == 1, beside, of(from_a, from_b, slot)))

            @pl.when(n > 0)
            def _():
                got(s)
            encode_block(s)
            return 0

        lax.fori_loop(0, owners, arrive, 0)
        row = jnp.sum(acc[...], axis=0, keepdims=True)
        parts = [row[:, m * half:(m + 1) * half] for m in range(4)]
        sums[...] = jnp.broadcast_to((parts[0] + parts[1]) + (parts[2] + parts[3]), sums.shape)

    settled(copies)

    @pl.when(relay)
    def _():
        for d in range(SIDE - 1):
            pltpu.make_async_copy(side_slot(d), side_slot(d), side_f.at[d]).wait()
    quads = flat.shape[0] // lines

    def gathered(op, join):
        row = [op(flat[pl.ds(i, quads, stride=lines), :], axis=0, keepdims=True) for i in range(lines)]
        row = jnp.concatenate(row, axis=1)
        parts = [row[:, m * half:(m + 1) * half] for m in range(4)]
        return join(join(parts[0], parts[1]), join(parts[2], parts[3]))

    @pl.when(others)
    def _():
        banks = [(q * CAP_TWO, CAP_TWO) for q in range(SIDE)]
        side_size = jnp.where(relay, CAP_SIDE, 0)
        banks += [(SIDE * CAP_TWO + d * CAP_SIDE, side_size) for d in range(SIDE - 1)]
        top = jnp.zeros(flat.shape, jnp.float32)
        for q, (start, size) in enumerate(banks):
            def cold_top(k, top):
                block = jnp.abs(landed[start + k].astype(jnp.float32))
                return jnp.maximum(top, jnp.where(k < number_ref[q], block, 0.0))

            top = lax.fori_loop(0, size, cold_top, top)
        flat[...] = top
        mine[...] = jnp.broadcast_to(gathered(jnp.max, jnp.maximum), mine.shape)
        settle()
        for i in range(lines):
            at = pl.ds(i, quads, stride=lines)
            flat_step[at, :] = jnp.broadcast_to(wide_step[0:1, i * 128:(i + 1) * 128], (quads, 128))
            flat_inverse[at, :] = jnp.broadcast_to(wide_inverse[0:1, i * 128:(i + 1) * 128], (quads, 128))
        total = jnp.zeros(flat.shape, jnp.float32)
        for q, (start, size) in enumerate(banks):
            def cold_code(k, total):
                values = landed[start + k].astype(jnp.float32)
                codes = jnp.clip(values * flat_inverse[...], -127.0, 127.0).astype(jnp.bfloat16)
                landed[start + k] = codes
                miss = values - codes.astype(jnp.float32) * flat_step[...]
                return total + jnp.where(k < number_ref[q], miss * miss, 0.0)

            total = lax.fori_loop(0, size, cold_code, total)
        flat[...] = total
        sums[...] = jnp.broadcast_to(gathered(jnp.sum, jnp.add), sums.shape)
        swap_hot.wait_send()

        def drained(n, _):
            pltpu.make_async_copy(final.at[0], final.at[0], sem_send.at[n]).wait()
            return 0

        sent = jnp.where(da != 0, jnp.where(da == 2, 2, 3), jnp.where(db == 2, 8, 12))
        lax.fori_loop(1, sent + 1, drained, 0)

    for h in range(SLICES):
        @pl.when(me != SLICES * layer + h)
        def _(h=h):
            report[h].wait_send()
    trade(sums, their_sums, sum_send, sum_recv)
    step = step_ref[...]
    error_ref[...] = (jnp.sum(their_sums[...], axis=0) + sums[...]) / (step * step * denominator)


def route(layer, denominator, one, two, side, number, hot, cold, peaks):
    _, capacity, flat = hot.shape
    owners = lax.axis_size("own")
    peers = lax.axis_size("rep") - 1
    _, n_cold, lines, width = cold.shape
    period = flat // 16
    half = period // 4
    smem = pl.BlockSpec(memory_space=pltpu.SMEM)
    vmem = pl.BlockSpec(memory_space=pltpu.VMEM)
    anywhere = pl.BlockSpec(memory_space=pl.ANY)
    block, small = (capacity, flat), (lines, width)
    stat = (8, half)
    dma = pltpu.SemaphoreType.DMA
    return pl.pallas_call(
        functools.partial(route_kernel, layer, denominator),
        out_shape=(jax.ShapeDtypeStruct((owners, *block), hot.dtype),
                   jax.ShapeDtypeStruct((SIDE * CAP_TWO + (SIDE - 1) * CAP_SIDE, *small), cold.dtype),
                   jax.ShapeDtypeStruct(stat, jnp.float32),
                   jax.ShapeDtypeStruct(stat, jnp.float32)),
        in_specs=[smem, smem, smem, smem, anywhere, anywhere, anywhere],
        out_specs=(vmem, vmem, vmem, vmem),
        scratch_shapes=[
            pltpu.VMEM((2 * n_cold, *small), cold.dtype),
            pltpu.VMEM(((SIDE - 1) * CAP_ONE, *small), cold.dtype),
            pltpu.VMEM((SIDE * CAP_ONE, *small), cold.dtype),
            pltpu.VMEM(((SIDE - 1) * CAP_TWO, *small), cold.dtype),
            pltpu.VMEM(((SIDE - 1) * CAP_SIDE, *small), cold.dtype),
            pltpu.VMEM((CAP_SIDE, *small), cold.dtype),
            pltpu.VMEM((owners, *stat), jnp.float32),
            pltpu.VMEM((8, period), jnp.float32),
            pltpu.VMEM((8, period), jnp.float32),
            pltpu.VMEM((capacity, period), jnp.float32),
            pltpu.VMEM(small, jnp.float32),
            pltpu.VMEM(small, jnp.float32),
            pltpu.VMEM(small, jnp.float32),
            pltpu.VMEM(stat, jnp.float32),
            pltpu.VMEM((peers, *stat), jnp.float32),
            pltpu.VMEM(stat, jnp.float32),
            pltpu.VMEM((peers, *stat), jnp.float32),
            dma((13,)), dma((owners,)), dma((2 * SIDE - 1,)), dma((2 * SIDE - 1,)),
            dma((SIDE,)), dma, dma((SIDE - 1,)), dma((2,)),
            dma((SLICES,)), dma, dma((peers,)), dma((peers,)), dma((peers,)), dma((peers,)),
        ],
        compiler_params=pltpu.CompilerParams(collective_id=4 + layer, has_side_effects=True,
                                             vmem_limit_bytes=VMEM_ROUTE),
    )(one, two, side, number, hot, cold, peaks)


VMEM_ROUTE = 40 * 1024 * 1024
VMEM_FINISH = 20 * 1024 * 1024


def finish_kernel(layer, where_ref, final, landed, step_in, error_in, out_ref, step_ref, error_ref,
                  wide, stage, zeros, stage_sem, sem):
    owners, capacity, width = final.shape
    rows = width // 128
    step_ref[...] = step_in[0:1]
    error_ref[...] = error_in[0:1]
    star = lax.axis_index("own") // SLICES == layer
    batch = 4

    @pl.when(star)
    def _():
        copies = [pltpu.make_async_copy(final.at[pl.ds(i * batch, batch)], out_ref.at[pl.ds(i * batch, batch)], sem.at[i])
                  for i in range(owners // batch)]
        for cp in copies:
            cp.start()
        for cp in copies:
            cp.wait()

    @pl.when(jnp.logical_not(star))
    def _():
        zeros[...] = jnp.zeros_like(zeros)

        def empty(s, _):
            @pl.when(where_ref[s * capacity] < 0)
            def _():
                pltpu.make_async_copy(zeros, out_ref.at[s], sem.at[s]).start()
            return 0

        lax.fori_loop(0, owners, empty, 0)

        def fill(s, used):
            some = where_ref[s * capacity] >= 0
            slot = lax.rem(used, 2)

            @pl.when(some)
            def _():
                wide[...] = jnp.zeros_like(wide)

                def one(c, _):
                    at = where_ref[s * capacity + c]

                    @pl.when(at >= 0)
                    def _():
                        wide[pl.ds(c, rows, stride=capacity), :] = landed[at].astype(jnp.float32)
                    return 0

                lax.fori_loop(0, capacity, one, 0)

                @pl.when(used >= 2)
                def _():
                    pltpu.make_async_copy(stage.at[slot], out_ref.at[s], stage_sem.at[slot]).wait()
                for r in range(rows):
                    stage[slot, :, r * 128:(r + 1) * 128] = wide[r * capacity:(r + 1) * capacity, :].astype(jnp.bfloat16)
                pltpu.make_async_copy(stage.at[slot], out_ref.at[s], stage_sem.at[slot]).start()
            return used + some.astype(jnp.int32)

        used = lax.fori_loop(0, owners, fill, 0)
        for n in range(2):
            @pl.when(used > n)
            def _():
                pltpu.make_async_copy(stage.at[n], out_ref.at[n], stage_sem.at[n]).wait()

        def wait(s, _):
            @pl.when(where_ref[s * capacity] < 0)
            def _():
                pltpu.make_async_copy(zeros, out_ref.at[s], sem.at[s]).wait()
            return 0

        lax.fori_loop(0, owners, wait, 0)


def finish(layer, where_held, final, landed, step, error):
    owners, capacity, width = final.shape
    half = step.shape[1]
    vmem = pl.BlockSpec(memory_space=pltpu.VMEM)
    return pl.pallas_call(
        functools.partial(finish_kernel, layer),
        out_shape=(jax.ShapeDtypeStruct(final.shape, final.dtype),
                   jax.ShapeDtypeStruct((1, half), jnp.float32),
                   jax.ShapeDtypeStruct((1, half), jnp.float32)),
        in_specs=[pl.BlockSpec(memory_space=pltpu.SMEM), vmem, vmem, vmem, vmem],
        out_specs=(pl.BlockSpec(memory_space=pltpu.HBM), vmem, vmem),
        scratch_shapes=[
            pltpu.VMEM((width // 128 * capacity, 128), jnp.float32),
            pltpu.VMEM((2, capacity, width), final.dtype),
            pltpu.VMEM((capacity, width), final.dtype),
            pltpu.SemaphoreType.DMA((2,)),
            pltpu.SemaphoreType.DMA((owners,)),
        ],
        compiler_params=pltpu.CompilerParams(vmem_limit_bytes=VMEM_FINISH),
    )(where_held, final, landed, step, error)


def body(block_pool, sel_index, sel_layer, counts):
    own_count = lax.axis_size("own")
    rep_count = lax.axis_size("rep")
    layers = own_count // SLICES
    n_select = sel_index.shape[0]
    capacity = n_select // 4
    tokens = block_pool.shape[1]
    half = block_pool.shape[2] // SLICES
    period = 4 * half
    denominator = float(own_count * rep_count * capacity * tokens)
    hot, cold, table, tops = open_exchange(block_pool, sel_index, sel_layer, counts, capacity)
    fits, one, two, side, number, where_held = plan(sel_layer, table, capacity, n_select - capacity)

    def routed(layer):
        return finish(layer, where_held, *route(layer, denominator, one, two, side, number, hot, cold, tops))

    def sparse():
        return lax.switch(sel_layer[0], [functools.partial(routed, layer) for layer in range(layers)])

    def dense():
        parted = part(block_pool, sel_index, sel_layer, counts, layers, capacity)
        arrived = lax.all_to_all(parted, "own", split_axis=0, concat_axis=0, tiled=True)
        top = jnp.max(peaks(arrived, period)[0].reshape(4, half), axis=0)
        step = HEADROOM * jnp.maximum(top, 1.0) / 127.0
        codes, err = encode(arrived, jnp.tile(step, 4)[None, :], period)
        return codes, step[None, :], totals(err, step[None, :], denominator)

    codes, step, error = lax.cond(fits[0] == 1, sparse, dense)
    return codes[None, None], step, error


def solution(mesh):
    return jax.shard_map(
        body,
        mesh=mesh,
        in_specs=(
            P(("own", "rep"), None, None),
            P(("own", "rep")),
            P(("own", "rep")),
            P(("own", "rep")),
        ),
        out_specs=(P("own", "rep", None, None, None), P("own", None), P("own", None)),
        check_vma=False,
    )
```
